128 devices in a mesh: tm: 16 (over y, x), batch: 8 (over z, core).
Axes of the slice: x: 4, y: 4, z: 4, core: 2. Of those that a mesh axis runs over, the one named last changes fastest.
Arguments:
- obs_feats: bfloat16 [32, 1024, 2048], P('batch', 'tm'), may hold values from -6 to 6
- next_feats: bfloat16 [32, 1024, 2048], P('batch', 'tm'), may hold values from -6 to 6
- online_w: float32 [2048, 2048], P(('tm', 'batch')), may hold values from -6 to 6
- target_w: float32 [2048, 2048], P(('tm', 'batch')), may hold values from -6 to 6
- log_decay: float32 [2048], replicated, may hold values from -1 to 0, as said below
- step_scale: float32 [32, 1024], P('batch', 'tm'), may hold values from 0.5 to 2
- online_heads: float32 [2, 2048], replicated, may hold values from -6 to 6
- target_heads: float32 [2, 2048], replicated, may hold values from -6 to 6
- reward: float32 [32, 1024], P('batch', 'tm'), may hold values from -6 to 6
- next_action_log_prob: float32 [32, 1024], P('batch', 'tm'), may hold values from -3 to 1
- resets: int32 [32, 1024], P('batch', 'tm'), may hold values 0 or 1
- horizon: int32 [32], P('batch'), may hold values from 1 to 8
- burn_in: int32 [32], P('batch'), may hold values from 0 to 64
Outputs:
- grad_w: float32 [2048, 2048], P(('tm', 'batch'))
- new_target: float32 [2048, 2048], P(('tm', 'batch'))
- returns: float32 [32, 1024], P('batch', 'tm')
The draws below stay inside these ranges and needn't reach their ends.
Inputs may be any that keep to these rules, and one draw needn't show every extreme that they name: `log_decay`: every entry is negative.
All inputs are finite; a program needn't handle non-finite values. No bound on the sum of `resets` on one device may be relied on, other than what follows from the above.
Results may differ from the reference program's by a relative error of at most 0.0059.
Values may be sent and summed in bfloat16 or wider, within the bound.
A program may use at most 128 MiB of HBM per device.

```python
import math
import jax
import jax.numpy as jnp
from jax import lax

D = 2048
H = 2048
T_DEV = 64
NMAX = 8
BURN_MAX = 64
B = 32
L = 1024


def draw_log_decay(key, part):
    first, second, third = jax.random.split(key, 3)
    keep_share = 0.5
    fast_rate = jax.random.uniform(third, (H,), minval=0.67, maxval=0.96) / T_DEV
    slow = jax.random.uniform(first, (H,)) < keep_share
    slow_rate = jnp.log(10.0) / (2.0 * L) * jax.random.uniform(second, (H,), minval=0.05, maxval=1.0)
    return (-jnp.where(slow, slow_rate, fast_rate)).astype(jnp.float32)


def touch_ends(result, stream_key, smallest, high):
    shape = result.shape
    place = [jax.random.randint(jax.random.fold_in(stream_key, axis), (), 0, shape[axis]) for axis in range(len(shape))]
    result = result.at[tuple(place)].set(smallest)
    longest = shape.index(max(shape))
    place[longest] = (place[longest] + 1) % shape[longest]
    return result.at[tuple(place)].set(high)


def with_spikes(result, stream_key, source, target, shards_of, factor):
    owner, partner = [(jnp.arange(result.shape[dim]) // (result.shape[dim] // shards_of)).reshape([-1 if axis == dim else 1 for axis in range(result.ndim)]) for dim in (source, target)]
    chosen = jax.random.permutation(stream_key, shards_of)[partner]
    strong = (owner == chosen) | (owner == (partner + shards_of // 2) % shards_of)
    return jnp.where(strong, factor * result, result)


def levels(rng, dims, cuts, smallest, largest):
    gain, own = 1.0, jax.random.fold_in(rng, 6)
    for position, shards_of in cuts:
        heights = jnp.exp(jax.random.uniform(jax.random.fold_in(own, position), (shards_of,), jnp.float32, smallest / len(cuts), largest / len(cuts)))
        gain = gain * jnp.repeat(heights, dims[position] // shards_of).reshape([-1 if axis == position else 1 for axis in range(len(dims))])
    return gain


def scatter_about(stream_key, extent, width, most, cuts=(), kind=jnp.bfloat16):
    result = jax.random.normal(stream_key, extent, jnp.float32) * width
    if len(cuts) > 0:
        result = levels(stream_key, extent, cuts, -0.22, 0.18) * result
    return jnp.clip(result, min=-most, max=most).astype(kind)


def heavy_noise(stream_key, extent, deviation, most, shards, heavy, dtype=jnp.bfloat16):
    values = deviation * jax.random.normal(stream_key, extent, jnp.float32)
    if shards:
        values = values * levels(stream_key, extent, shards, -0.22, 0.18)
    return jnp.clip(with_spikes(values, jax.random.fold_in(stream_key, 3), *heavy), -most, most).astype(dtype)


def setup_inputs(seed: int = 0) -> dict:
    keys = jax.random.split(jax.random.key(seed), 14)
    obs_feats = heavy_noise(keys[0], (B, L, D), 1.0, 6.0, ((0, 8), (1, 16)), (0, 2, 8, 2.0))
    next_feats = scatter_about(keys[1], (B, L, D), 1.0, 6.0, ((0, 8), (1, 16)))
    online_w = scatter_about(keys[2], (D, H), 1.0, 6.0, ((0, 128),), jnp.float32)
    target_w = scatter_about(keys[3], (D, H), 1.0, 6.0, ((0, 128),), jnp.float32)
    log_decay = draw_log_decay(jax.random.fold_in(keys[13], 71), 0)
    step_scale = jnp.clip(jnp.exp(math.log(2.0) - 1.3862944 * jax.random.uniform(keys[5], (B, L), jnp.float32) ** levels(keys[5], (B, L), ((0, 8), (1, 16)), -0.2, 0.2)), 0.5, 2.0)
    online_heads = scatter_about(keys[6], (2, H), 1.0, 6.0, (), jnp.float32)
    target_heads = scatter_about(keys[7], (2, H), 1.0, 6.0, (), jnp.float32)
    reward = scatter_about(keys[8], (B, L), 1.0, 6.0, ((0, 8), (1, 16)), jnp.float32)
    next_action_log_prob = jnp.clip(-3.0 + 4.0 * jax.random.uniform(keys[9], (B, L), jnp.float32) ** levels(keys[9], (B, L), ((0, 8), (1, 16)), -0.2, 0.2), -3.0, 1.0)
    resets = touch_ends((jax.random.randint(keys[10], (B, L), 0, 256) < 1).astype(jnp.int32), jax.random.fold_in(keys[10], 1), 0, 1)
    horizon = touch_ends(jax.random.randint(keys[11], (B,), 1, NMAX + 1), jax.random.fold_in(keys[11], 1), 1, NMAX).astype(jnp.int32)
    burn_in = touch_ends(jax.random.randint(keys[12], (B,), 0, BURN_MAX + 1), jax.random.fold_in(keys[12], 1), 0, BURN_MAX).astype(jnp.int32)
    return {"obs_feats": obs_feats, "next_feats": next_feats, "online_w": online_w, "target_w": target_w, "log_decay": log_decay, "step_scale": step_scale, "online_heads": online_heads, "target_heads": target_heads, "reward": reward, "next_action_log_prob": next_action_log_prob, "resets": resets, "horizon": horizon, "burn_in": burn_in}


DISCOUNT = 0.99
ENTROPY_COEFF = 0.2
POLYAK_RATE = 0.005
STEP_SIZE = 0.1

def affine(earlier, later):
    return (later[0] * earlier[0], later[0] * earlier[1] + later[1])

def silu_slope(values):
    sigma = jax.nn.sigmoid(values)
    return sigma * (1.0 + values * (1.0 - sigma))

def returns_from(ext_reward, ext_value, ext_keep, row_horizon, span):
    total = jnp.zeros((ext_reward.shape[0], span), jnp.float32)
    alive = jnp.ones((ext_reward.shape[0], span), jnp.float32)
    for offset in range(NMAX):
        inside = (row_horizon > offset)[:, None]
        total = total + jnp.where(inside, DISCOUNT ** offset * alive * ext_reward[:, offset:offset + span], 0.0)
        alive = alive * ext_keep[:, offset + 1:offset + 1 + span]
        finish = (row_horizon == offset + 1)[:, None]
        total = total + jnp.where(finish, DISCOUNT ** (offset + 1) * alive * ext_value[:, offset + 1:offset + 1 + span], 0.0)
    return total

def reference(obs_feats, next_feats, online_w, target_w, log_decay, step_scale, online_heads, target_heads, reward, next_action_log_prob, resets, horizon, burn_in):
    w_online = online_w.astype(jnp.bfloat16)
    w_target = target_w.astype(jnp.bfloat16)
    input_scale = D ** (-0.5)
    scale_head = H ** (-0.5)
    padding = jnp.zeros((NMAX,), jnp.float32)
    times = jnp.arange(L).astype(jnp.int32)

    def per_row(total_grad, row):
        inputs, inputs_next, stride, gains, action_log_prob, flags, row_horizon, row_burn = row
        decay = jnp.exp(stride[:, None] * log_decay[None, :])
        keeping = 1.0 - flags.astype(jnp.float32)
        factor = decay * keeping[:, None]
        spread = jnp.sqrt(1.0 - decay * decay)
        proj_on = jnp.dot(inputs, w_online, preferred_element_type=jnp.float32) * input_scale
        proj_tg = jnp.dot(inputs_next, w_target, preferred_element_type=jnp.float32) * input_scale
        state_on = lax.associative_scan(affine, (factor, spread * proj_on), axis=0)[1]
        state_tg = lax.associative_scan(affine, (factor, spread * proj_tg), axis=0)[1]
        q_on = jnp.dot(jax.nn.silu(state_on), online_heads.T, precision=lax.Precision.HIGHEST) * scale_head
        target_quality = jnp.dot(jax.nn.silu(state_tg), target_heads.T, precision=lax.Precision.HIGHEST) * scale_head
        soft_value = lax.optimization_barrier(jnp.min(target_quality, axis=1)) - ENTROPY_COEFF * action_log_prob
        row_returns = returns_from(jnp.concatenate([gains, padding])[None], jnp.concatenate([soft_value, padding])[None], jnp.concatenate([keeping, padding])[None], row_horizon[None], L)[0]
        weight_mask = (times >= row_burn).astype(jnp.float32)
        slope = weight_mask[:, None] * (q_on - row_returns[:, None])
        grad_y = jnp.dot(slope, online_heads, precision=lax.Precision.HIGHEST) * scale_head
        grad_h = grad_y * silu_slope(state_on)
        shifted = jnp.concatenate([factor[1:], jnp.ones((1, H), jnp.float32)], axis=0)
        adjoint = lax.associative_scan(affine, (shifted, grad_h), reverse=True, axis=0)[1]
        grad_u = (spread * adjoint).astype(jnp.bfloat16)
        term = lax.dot_general(inputs, grad_u, (((0,), (0,)), ((), ())), preferred_element_type=jnp.float32) * input_scale
        return (total_grad + term, row_returns)
    grad_w, returns = lax.scan(per_row, jnp.zeros((D, H), jnp.float32), (obs_feats, next_feats, step_scale, reward, next_action_log_prob, resets, horizon, burn_in))
    new_target = (1.0 - POLYAK_RATE) * target_w + POLYAK_RATE * (online_w - STEP_SIZE * grad_w)
    return (grad_w, new_target, returns)
```

```python
import jax
import jax.numpy as jnp
from jax import lax
from jax.experimental import pallas as pl
from jax.experimental.pallas import tpu as pltpu
from jax.sharding import PartitionSpec as P

NMAX = 8
DISCOUNT = 0.99
ENTROPY_COEFF = 0.2
POLYAK_RATE = 0.005
STEP_SIZE = 0.1

F32 = jnp.float32
BF16 = jnp.bfloat16
MESH = pl.DeviceIdType.MESH

D = 2048
H = 2048
HALF = H // 2
T = 64
PAIR = 8
ROWS = T * PAIR
TM = 16
SCALE = D ** (-0.5)

WIDTHS = (384, 384, 256)
OFFSETS = (0, 384, 768)
ORDERS = (("z", "x", "y"), ("y", "z", "x"), ("x", "y", "z"))
HALVED = ((None, "z", "x"), (None, "y", "y"), (None, "x", "y"))
AG_MESSAGES = 6


def half_shape(k, w):
    return ((16, w), (2, 32, w), (2, 4, 32, w))[k]


def kernel(
    obs, nxt, onw, tgw, ld, step, onh, tgh, rew, logp, rst, hor, burn,
    gw, nt, ret,
    xr_o, xr_n, xp_o, xp_n, xt, wst,
    wt0, wt1, wt2, wo0, wo1, wo2,
    pk_m, pk_i, bc0, bc1, cc, ss, pf, tp, vt, vo,
    sf, dall, ends_t, ends_o, lv, carry,
    q_s, q_r, nb_s, nb_r, du,
    g0, g1, g2,
    s00, s01, s02, s10, s11, s12, s20, s21, s22,
    r00, r01, r02, r10, r11, r12, r20, r21, r22,
    gx_s, gx_r,
    ag_ss, ag_rs, rs_ss, rs_rs, pre_ss, pre_rs, loc_sem, d2d_ss, d2d_rs, nb_sem,
):
    tm = lax.axis_index("tm")
    batch = lax.axis_index("batch")
    y, x = tm // 4, tm % 4
    z, c = batch // 2, batch % 2
    at = {"y": y, "x": x, "z": z}
    other = 1 - c
    wb = ((wt0, wt1, wt2), (wo0, wo1, wo2))
    gg = (g0, g1, g2)
    snd = ((s00, s01, s02), (s10, s11, s12), (s20, s21, s22))
    rcv = ((r00, r01, r02), (r10, r11, r12), (r20, r21, r22))
    pending = []

    def device(**moved):
        here = {**at, **moved}
        return {"tm": here["y"] * 4 + here["x"], "batch": here["z"] * 2 + c}

    partner = {"tm": tm, "batch": z * 2 + other}

    def remote(src, dst, ss_, rs_, dev):
        return pltpu.make_async_remote_copy(
            src_ref=src, dst_ref=dst, send_sem=ss_, recv_sem=rs_, device_id=dev,
            device_id_type=MESH,
        )

    def send(src, dst, ss_, rs_, dev):
        copy = remote(src, dst, ss_, rs_, dev)
        copy.start()
        pending.append(copy)

    mine = pl.ds(pl.multiple_of(c * HALF, HALF), HALF)
    theirs = pl.ds(pl.multiple_of(other * HALF, HALF), HALF)
    own_rows = pl.ds(pl.multiple_of(c * 16, 16), 16)
    for m, w in enumerate((tgw, onw)):
        wst[m] = w[:, theirs].astype(BF16)
        for p in range(3):
            cols = pl.ds(pl.multiple_of(c * HALF + OFFSETS[p], 128), WIDTHS[p])
            wb[m][p][y, x, z, own_rows, :] = w[:, cols].astype(BF16)

    row8 = lax.broadcasted_iota(jnp.int32, (PAIR, 128), 0)
    lane8 = lax.broadcasted_iota(jnp.int32, (PAIR, 128), 1)
    row_own = (row8[:, :T] // 4) == c

    def twice(v):
        return jnp.where(row_own, jnp.concatenate([v, v], axis=0), 0.0)

    pk_m[...] = jnp.zeros_like(pk_m)
    for slot, r in enumerate((step, rew, logp)):
        pk_m[slot, :, :T] = twice(r[...])
    pk_m[3, :, :T] = twice(rst[...].astype(F32))
    hz = jnp.zeros((PAIR, 128), F32)
    bz = jnp.zeros((PAIR, 128), F32)
    for i in range(4):
        sel = row8 == c * 4 + i
        hz = jnp.where(sel, hor[i].astype(F32), hz)
        bz = jnp.where(sel, burn[i].astype(F32), bz)
    pk_m[4] = hz
    pk_m[5] = bz

    own_half = pl.ds(pl.multiple_of(c * 256, 256), 256)
    local = [
        pltpu.make_async_copy(nxt, xr_n.at[own_half, :], loc_sem.at[0]),
        pltpu.make_async_copy(obs, xr_o.at[own_half, :], loc_sem.at[1]),
    ]
    for copy in local:
        copy.start()

    barrier = pltpu.get_barrier_semaphore()
    peers = [partner, device(z=lax.rem(z + 1, 4)), device(z=lax.rem(z + 3, 4))]
    peers += [{"tm": lax.rem(tm + d, TM), "batch": batch} for d in range(1, TM)]
    for dev in peers:
        pl.semaphore_signal(barrier, inc=1, device_id=dev, device_id_type=MESH)
    pl.semaphore_wait(barrier, len(peers))

    def w_half(m, p):
        cols = pl.ds(OFFSETS[p], WIDTHS[p])
        return wst.at[m, :, cols], wb[m][p].at[y, x, z, own_rows, :]

    def w_half_in(m, p):
        rows = pl.ds(pl.multiple_of(other * 16, 16), 16)
        dst = wb[m][p].at[y, x, z, rows, :]
        remote(dst, dst, d2d_ss.at[m * 3 + p], d2d_rs.at[m * 3 + p], partner).wait_recv()

    for m in range(2):
        for p in range(3):
            src, dst = w_half(m, p)
            send(src, dst, d2d_ss.at[m * 3 + p], d2d_rs.at[m * 3 + p], partner)
    send(pk_m, pk_i, d2d_ss.at[6], d2d_rs.at[6], partner)
    send(nxt, xr_n.at[own_half, :], d2d_ss.at[7], d2d_rs.at[7], partner)
    send(obs, xr_o.at[own_half, :], d2d_ss.at[8], d2d_rs.at[8], partner)

    def block(p, k, q, h):
        order = ORDERS[p]
        idx = {}
        for a in "yxz":
            if a in order[:k]:
                idx[a] = pl.ds(0, 4)
            elif a == order[k]:
                idx[a] = q
            else:
                idx[a] = at[a]
        rows = pl.ds(0, 32)
        if h is not None:
            if k == 0:
                rows = pl.ds(16 * h, 16)
            else:
                idx[HALVED[p][k]] = pl.ds(2 * h, 2)
        return (idx["y"], idx["x"], idx["z"], rows, pl.ds(0, WIDTHS[p]))

    def around(p, k):
        axis = ORDERS[p][k]
        q = at[axis]
        return (
            axis, q, lax.rem(q + 1, 4), lax.rem(q + 3, 4), lax.rem(q + 2, 4),
            device(**{axis: lax.rem(q + 1, 4)}), device(**{axis: lax.rem(q + 3, 4)}),
        )

    def ag_sem(m, p, k, j):
        n = ((m * 3 + p) * 3 + k) * AG_MESSAGES + j
        return ag_ss.at[n], ag_rs.at[n]

    def ag_send(m, p, k, q, h, j, dev):
        ref = wb[m][p].at[block(p, k, q, h)]
        send(ref, ref, *ag_sem(m, p, k, j), dev)

    def ag_wait(m, p, k, q, h, j, dev):
        ref = wb[m][p].at[block(p, k, q, h)]
        remote(ref, ref, *ag_sem(m, p, k, j), dev).wait_recv()

    def ag_first(m, p, k):
        _, q, _, _, _, plus, minus = around(p, k)
        if k == 2:
            ag_send(m, p, k, q, 0, 0, plus)
            ag_send(m, p, k, q, 1, 2, minus)
            ag_send(m, p, k, q, 1, 1, plus)
            ag_send(m, p, k, q, 0, 3, minus)
        else:
            ag_send(m, p, k, q, None, 0, plus)
            ag_send(m, p, k, q, None, 2, minus)

    def ag_forward(m, p, k):
        _, q, qp, qm, _, plus, minus = around(p, k)
        h0, h1 = (0, 1) if k == 2 else (None, None)
        ag_wait(m, p, k, qm, h0, 0, minus)
        ag_send(m, p, k, qm, 0, 4, plus)
        ag_wait(m, p, k, qp, h1, 2, plus)
        ag_send(m, p, k, qp, 1, 5, minus)

    def ag_last(m, p, k):
        _, q, qp, qm, opp, plus, minus = around(p, k)
        if k == 2:
            ag_wait(m, p, k, qm, 1, 1, minus)
            ag_wait(m, p, k, qp, 0, 3, plus)
        ag_wait(m, p, k, opp, 0, 4, minus)
        ag_wait(m, p, k, opp, 1, 5, plus)

    for m in range(2):
        for p in range(3):
            w_half_in(m, p)
            ag_first(m, p, 0)
    for m in range(2):
        for p in range(3):
            ag_forward(m, p, 0)
    for m in range(2):
        for p in range(3):
            ag_last(m, p, 0)
            ag_first(m, p, 1)
    for m in range(2):
        for p in range(3):
            ag_forward(m, p, 1)
    for p in range(3):
        ag_last(0, p, 1)
        ag_first(0, p, 2)

    remote(pk_m, pk_i, d2d_ss.at[6], d2d_rs.at[6], partner).wait_recv()
    step8 = pk_m[0] + pk_i[0]
    rew8 = pk_m[1] + pk_i[1]
    logp8 = pk_m[2] + pk_i[2]
    rst8 = pk_m[3] + pk_i[3]
    keep8 = 1.0 - rst8
    hor8 = pk_m[4] + pk_i[4]
    burn8 = pk_m[5] + pk_i[5]

    sf[tm, 0] = jnp.broadcast_to(jnp.sum(step8, axis=1, keepdims=True), (PAIR, 128))
    sf[tm, 1] = jnp.broadcast_to(1.0 - jnp.max(rst8, axis=1, keepdims=True), (PAIR, 128))
    for d in range(1, TM):
        dev = {"tm": lax.rem(tm + d, TM), "batch": batch}
        send(sf.at[tm], sf.at[tm], pre_ss.at[0, d], pre_rs.at[0, tm], dev)

    def spread_lanes(dst, v):
        for t in range(T):
            dst[pl.ds(t * PAIR, PAIR), :] = jnp.broadcast_to(v[:, t : t + 1], (PAIR, 128))

    spread_lanes(bc0, step8)
    spread_lanes(bc1, keep8)
    ld8 = jnp.broadcast_to(ld[:, mine], (PAIR, HALF))

    def wide(v):
        return jnp.concatenate([v] * (HALF // 128), axis=1)

    def at_t(t):
        return pl.ds(pl.multiple_of(t * PAIR, PAIR), PAIR)

    def factors(t, prod):
        e = jnp.exp(wide(bc0[at_t(t), :]) * ld8)
        f = e * wide(bc1[at_t(t), :])
        cc[at_t(t), :] = f
        ss[at_t(t), :] = jnp.sqrt(1.0 - e * e)
        prod = prod * f
        pf[at_t(t), :] = prod
        return prod

    lax.fori_loop(0, T, factors, jnp.ones((PAIR, HALF), F32))

    def tails(i, prod):
        t = T - 1 - i
        tp[at_t(t), :] = prod
        return prod * cc[at_t(t), :]

    lax.fori_loop(0, T, tails, jnp.ones((PAIR, HALF), F32))

    r_out = lax.broadcasted_iota(jnp.int32, (ROWS, ROWS), 0)
    r_in = lax.broadcasted_iota(jnp.int32, (ROWS, ROWS), 1)

    def permutation():
        return jnp.where(r_out == (r_in % T) * PAIR + r_in // T, 1.0, 0.0).astype(BF16)

    for p in range(3):
        ag_forward(0, p, 2)
    for p in range(3):
        ag_last(1, p, 1)
        ag_first(1, p, 2)

    other_half = pl.ds(pl.multiple_of(other * 256, 256), 256)
    local[0].wait()
    remote(nxt, xr_n.at[other_half, :], d2d_ss.at[7], d2d_rs.at[7], partner).wait_recv()
    local[1].wait()
    remote(obs, xr_o.at[other_half, :], d2d_ss.at[8], d2d_rs.at[8], partner).wait_recv()
    perm = permutation()

    def permute(i, _):
        cols = pl.ds(pl.multiple_of(i * 256, 256), 256)
        xp_n[:, cols] = jnp.dot(perm, xr_n[:, cols], preferred_element_type=F32).astype(BF16)
        v = jnp.dot(perm, xr_o[:, cols], preferred_element_type=F32)
        xp_o[:, cols] = v.astype(BF16)
        xt[cols, :] = v.T.astype(BF16)
        return 0

    lax.fori_loop(0, D // 256, permute, 0)

    for d in range(1, TM):
        j = lax.rem(tm + d, TM)
        dev = {"tm": j, "batch": batch}
        remote(sf.at[j], sf.at[j], pre_ss.at[0, d], pre_rs.at[0, j], dev).wait_recv()

    def block_decay(j, _):
        dall[j] = jnp.exp(wide(sf[j, 0]) * ld8) * wide(sf[j, 1])
        return 0

    lax.fori_loop(0, TM, block_decay, 0)

    def project(m, p, xp, v):
        def tile(i, _):
            rows = pl.ds(pl.multiple_of(i * 256, 256), 256)
            w = wb[m][p][...].reshape(D, WIDTHS[p])
            acc = jnp.dot(xp[rows, :], w, preferred_element_type=F32)
            v[rows, pl.ds(OFFSETS[p], WIDTHS[p])] = acc * SCALE
            return 0

        lax.fori_loop(0, ROWS // 256, tile, 0)

    def scan(v):
        def body(t, st):
            st = cc[at_t(t), :] * st + ss[at_t(t), :] * v[at_t(t), :]
            v[at_t(t), :] = st
            return st

        return lax.fori_loop(0, T, body, jnp.zeros((PAIR, HALF), F32))

    def prefix_send(n, ends, forward):
        for d in range(TM - 1, 0, -1):
            to = tm + d if forward else tm - d

            @pl.when(to < TM if forward else to >= 0)
            def _(d=d, to=to):
                dev = {"tm": to, "batch": batch}
                remote(ends.at[tm], ends.at[tm], pre_ss.at[n, d], pre_rs.at[n, tm], dev).start()

    def prefix_take(n, ends, forward):
        carry[...] = jnp.zeros_like(carry)
        for j in range(TM) if forward else range(TM - 1, -1, -1):

            @pl.when(j < tm if forward else j > tm)
            def _(j=j):
                dev = {"tm": j, "batch": batch}
                remote(ends.at[j], ends.at[j], pre_ss.at[n, 0], pre_rs.at[n, j], dev).wait_recv()
                carry[...] = dall[j] * carry[...] + ends[j]

    def prefix_drain(n, ends, forward):
        for d in range(1, TM):
            to = tm + d if forward else tm - d

            @pl.when(to < TM if forward else to >= 0)
            def _(d=d, to=to):
                dev = {"tm": to, "batch": batch}
                remote(ends.at[tm], ends.at[tm], pre_ss.at[n, d], pre_rs.at[n, tm], dev).wait_send()

    def lane_fold(v):
        out = v[:, :128]
        for i in range(1, HALF // 128):
            out = out + v[:, i * 128 : (i + 1) * 128]
        return jnp.sum(out, axis=1, keepdims=True)

    def quality(v, heads, slot):
        h0 = jnp.broadcast_to(heads[0:1, mine], (PAIR, HALF))
        h1 = jnp.broadcast_to(heads[1:2, mine], (PAIR, HALF))
        start = carry[...]

        def body(t, acc):
            st = v[at_t(t), :] + pf[at_t(t), :] * start
            v[at_t(t), :] = st
            act = st / (1.0 + jnp.exp(-st))
            here = lane8 == t
            return (
                jnp.where(here, lane_fold(act * h0), acc[0]),
                jnp.where(here, lane_fold(act * h1), acc[1]),
            )

        zero = jnp.zeros((PAIR, 128), F32)
        a0, a1 = lax.fori_loop(0, T, body, (zero, zero))
        q_s[slot, 0] = a0
        q_s[slot, 1] = a1
        send(q_s.at[slot], q_r.at[slot], d2d_ss.at[9 + slot], d2d_rs.at[9 + slot], partner)

    def quality_sum(slot):
        remote(
            q_s.at[slot], q_r.at[slot], d2d_ss.at[9 + slot], d2d_rs.at[9 + slot], partner
        ).wait_recv()
        return [(q_s[slot, k] + q_r[slot, k]) * (H ** (-0.5)) for k in range(2)]

    for p in range(3):
        ag_last(0, p, 2)
        project(0, p, xp_n, vt)
    for p in range(3):
        ag_forward(1, p, 2)
    ends_t[tm] = scan(vt)
    prefix_send(1, ends_t, True)
    prefix_take(1, ends_t, True)
    quality(vt, tgh, 0)
    tq = quality_sum(0)
    value8 = jnp.minimum(tq[0], tq[1]) - ENTROPY_COEFF * logp8

    nb_s[0] = rew8
    nb_s[1] = value8
    nb_s[2] = keep8
    before = {"tm": lax.rem(tm + TM - 1, TM), "batch": batch}
    send(nb_s, nb_r, nb_sem.at[0], nb_sem.at[1], before)
    remote(nb_s, nb_r, nb_sem.at[0], nb_sem.at[1], before).wait_recv()
    inside = (lane8 >= T) & (lane8 < T + NMAX) & (tm < TM - 1)

    def extended(own, slot):
        later = jnp.where(inside, pltpu.roll(nb_r[slot], T, 1), 0.0)
        return jnp.where(lane8 < T, own, later)

    ext_r, ext_v, ext_k = extended(rew8, 0), extended(value8, 1), extended(keep8, 2)

    def shifted(v, n):
        return v if n == 0 else pltpu.roll(v, 128 - n, 1)

    total = jnp.zeros((PAIR, 128), F32)
    alive = jnp.ones((PAIR, 128), F32)
    for n in range(NMAX):
        total = total + jnp.where(hor8 > n, DISCOUNT**n * alive * shifted(ext_r, n), 0.0)
        alive = alive * shifted(ext_k, n + 1)
        total = total + jnp.where(
            hor8 == n + 1, DISCOUNT ** (n + 1) * alive * shifted(ext_v, n + 1), 0.0
        )
    ret[...] = jnp.where(c == 0, total[:4, :T], total[4:, :T])
    weight = jnp.where((lane8 + tm * T).astype(F32) >= burn8, 1.0, 0.0)

    for p in range(3):
        ag_last(1, p, 2)
        project(1, p, xp_o, vo)
    ends_o[tm] = scan(vo)
    prefix_send(2, ends_o, True)
    prefix_take(2, ends_o, True)
    quality(vo, onh, 1)

    def slopes(t, _):
        v = vo[at_t(t), :]
        sig = 1.0 / (1.0 + jnp.exp(-v))
        vo[at_t(t), :] = sig * (1.0 + v * (1.0 - sig)) * (H ** (-0.5))
        return 0

    lax.fori_loop(0, T, slopes, 0)
    oq = quality_sum(1)
    spread_lanes(bc0, weight * (oq[0] - total))
    spread_lanes(bc1, weight * (oq[1] - total))
    h0 = jnp.broadcast_to(onh[0:1, mine], (PAIR, HALF))
    h1 = jnp.broadcast_to(onh[1:2, mine], (PAIR, HALF))

    def back(i, adj):
        t = T - 1 - i
        dh = (wide(bc0[at_t(t), :]) * h0 + wide(bc1[at_t(t), :]) * h1) * vo[at_t(t), :]
        adj = dh + adj
        vo[at_t(t), :] = adj
        return cc[at_t(t), :] * adj

    lv[tm] = lax.fori_loop(0, T, back, jnp.zeros((PAIR, HALF), F32))
    prefix_send(3, lv, False)
    prefix_take(3, lv, False)
    incoming = carry[...]
    both = jnp.concatenate([incoming, incoming], axis=0)

    def finish(i, _):
        rows = pl.ds(pl.multiple_of(i * 16, 16), 16)
        adj = vo[rows, :] + tp[rows, :] * both
        du[rows, :] = (ss[rows, :] * adj).astype(BF16)
        return 0

    lax.fori_loop(0, ROWS // 16, finish, 0)

    def gradient(p):
        def tile(i, _):
            rows = pl.ds(pl.multiple_of(i * 512, 512), 512)
            v = jnp.dot(
                xt[rows, :], du[:, pl.ds(OFFSETS[p], WIDTHS[p])], preferred_element_type=F32
            )
            gg[p][i] = (v * SCALE).reshape(4, 4, 32, WIDTHS[p])
            return 0

        lax.fori_loop(0, 4, tile, 0)

    def pieces(p, k, q, h, fn):
        order = ORDERS[p]
        if k == 0:
            fn(block(p, k, q, h), ())
            return
        free = [a for a in "yxz" if a in order[:k]]

        def at_piece(ids):
            idx = dict(at)
            idx[order[k]] = q
            for a, i in zip(free, ids):
                idx[a] = i + 2 * h if a == HALVED[p][k] else i
            return (idx["y"], idx["x"], idx["z"], pl.ds(0, 32), pl.ds(0, WIDTHS[p]))

        if k == 1:
            for i in range(2):
                fn(at_piece((i,)), (i,))
            return

        def body(n, _):
            i, j = n // 4, n % 4
            fn(at_piece((i, j)), (i, j))
            return 0

        lax.fori_loop(0, 8, body, 0)

    def rs_sem(p, k, j):
        n = (p * 3 + k) * 6 + j
        return rs_ss.at[n], rs_rs.at[n]

    def rs_send(p, k, j, dev):
        send(snd[p][k].at[j], rcv[p][k].at[j], *rs_sem(p, k, j), dev)

    def rs_wait(p, k, j):
        _, _, _, _, _, plus, minus = around(p, k)
        dev = plus if j % 2 == 0 else minus
        remote(snd[p][k].at[j], rcv[p][k].at[j], *rs_sem(p, k, j), dev).wait_recv()

    def rs_fill(p, k, j, q, h, add):
        def fn(idx, at_):
            v = gg[p][idx]
            if add:
                v = v + rcv[p][k][(j - 4,) + at_].astype(F32)
            snd[p][k][(j,) + at_] = v.astype(BF16)

        pieces(p, k, q, h, fn)

    def rs_first(p, k):
        _, q, qp, qm, opp, plus, minus = around(p, k)
        for j, (who, h, dev) in enumerate(
            ((opp, 0, minus), (opp, 1, plus), (qm, 1, minus), (qp, 0, plus))
        ):
            rs_fill(p, k, j, who, h, False)
            rs_send(p, k, j, dev)

    def rs_middle(p, k):
        _, q, qp, qm, opp, plus, minus = around(p, k)
        for j, (who, h, dev) in ((4, (qm, 0, minus)), (5, (qp, 1, plus))):
            rs_wait(p, k, j - 4)
            rs_fill(p, k, j, who, h, True)
            rs_send(p, k, j, dev)

    def rs_last(p, k):
        q = at[ORDERS[p][k]]
        for h, pair in ((0, (3, 4)), (1, (2, 5))):
            for j in pair:
                rs_wait(p, k, j)

            def fn(idx, at_, pair=pair):
                v = gg[p][idx]
                for j in pair:
                    v = v + rcv[p][k][(j,) + at_].astype(F32)
                gg[p][idx] = v

            pieces(p, k, q, h, fn)

    for p in range(3):
        gradient(p)
        rs_first(p, 2)
    for p in range(3):
        rs_middle(p, 2)
    for k in (1, 0):
        for p in range(3):
            rs_last(p, k + 1)
            rs_first(p, k)
        for p in range(3):
            rs_middle(p, k)
    for p in range(3):
        rs_last(p, 0)

    other_rows = pl.ds(pl.multiple_of(other * 16, 16), 16)
    for p in range(3):
        gx_s[:, pl.ds(OFFSETS[p], WIDTHS[p])] = gg[p][y, x, z, other_rows, :]
    send(gx_s, gx_r, d2d_ss.at[11], d2d_rs.at[11], partner)
    for p in range(3):
        cols = pl.ds(pl.multiple_of(c * HALF + OFFSETS[p], 128), WIDTHS[p])
        gw[:, cols] = gg[p][y, x, z, own_rows, :]
    remote(gx_s, gx_r, d2d_ss.at[11], d2d_rs.at[11], partner).wait_recv()
    gw[:, theirs] = gx_r[...]
    nt[...] = (1.0 - POLYAK_RATE) * tgw[...] + POLYAK_RATE * (onw[...] - STEP_SIZE * gw[...])

    prefix_drain(1, ends_t, True)
    prefix_drain(2, ends_o, True)
    prefix_drain(3, lv, False)
    for copy in pending:
        copy.wait_send()


def shards(
    obs_feats, next_feats, online_w, target_w, log_decay, step_scale, online_heads, target_heads,
    reward, next_action_log_prob, resets, horizon, burn_in,
):
    vmem = pl.BlockSpec(memory_space=pltpu.VMEM)
    smem = pl.BlockSpec(memory_space=pltpu.SMEM)
    hbm = pl.BlockSpec(memory_space=pl.ANY)
    weights = [pltpu.VMEM((4, 4, 4, 32, w), BF16) for w in WIDTHS]
    staged = [pltpu.VMEM((6, *half_shape(k, w)), BF16) for w in WIDTHS for k in range(3)]
    big = pltpu.VMEM((ROWS, HALF), F32)
    ends = pltpu.VMEM((TM, PAIR, HALF), F32)
    narrow = pltpu.VMEM((ROWS, 128), F32)
    scratch = [
        pltpu.VMEM((ROWS, D), BF16), pltpu.VMEM((ROWS, D), BF16),
        pltpu.VMEM((ROWS, D), BF16), pltpu.VMEM((ROWS, D), BF16),
        pltpu.VMEM((D, ROWS), BF16), pltpu.VMEM((2, 16, HALF), BF16),
        *weights, *weights,
        pltpu.VMEM((6, PAIR, 128), F32), pltpu.VMEM((6, PAIR, 128), F32), narrow, narrow,
        big, big, big, big, big, big,
        pltpu.VMEM((TM, 2, PAIR, 128), F32), ends, ends, ends, ends,
        pltpu.VMEM((PAIR, HALF), F32),
        pltpu.VMEM((2, 2, PAIR, 128), F32), pltpu.VMEM((2, 2, PAIR, 128), F32),
        pltpu.VMEM((3, PAIR, 128), F32), pltpu.VMEM((3, PAIR, 128), F32),
        pltpu.VMEM((ROWS, HALF), BF16),
        *[pltpu.VMEM((4, 4, 4, 32, w), F32) for w in WIDTHS],
        *staged, *staged,
        pltpu.VMEM((16, HALF), F32), pltpu.VMEM((16, HALF), F32),
        pltpu.SemaphoreType.DMA((18 * AG_MESSAGES,)), pltpu.SemaphoreType.DMA((18 * AG_MESSAGES,)),
        pltpu.SemaphoreType.DMA((54,)), pltpu.SemaphoreType.DMA((54,)),
        pltpu.SemaphoreType.DMA((4, TM)), pltpu.SemaphoreType.DMA((4, TM)),
        pltpu.SemaphoreType.DMA((2,)),
        pltpu.SemaphoreType.DMA((12,)), pltpu.SemaphoreType.DMA((12,)),
        pltpu.SemaphoreType.DMA((2,)),
    ]
    rows_b, span, width = obs_feats.shape
    return pl.pallas_call(
        kernel,
        name="critic_step",
        out_shape=(
            jax.ShapeDtypeStruct(online_w.shape, F32),
            jax.ShapeDtypeStruct(target_w.shape, F32),
            jax.ShapeDtypeStruct(reward.shape, F32),
        ),
        in_specs=[hbm, hbm] + [vmem] * 9 + [smem] * 2,
        out_specs=(vmem, vmem, vmem),
        scratch_shapes=scratch,
        compiler_params=pltpu.CompilerParams(
            collective_id=0, has_side_effects=True, vmem_limit_bytes=62 * 1024 * 1024
        ),
    )(
        obs_feats.reshape(rows_b * span, width), next_feats.reshape(rows_b * span, width),
        online_w, target_w, log_decay[None], step_scale, online_heads, target_heads,
        reward, next_action_log_prob, resets, horizon, burn_in,
    )


def solution(mesh):
    return jax.shard_map(
        shards,
        mesh=mesh,
        in_specs=(
            P("batch", "tm", None), P("batch", "tm", None),
            P(("tm", "batch"), None), P(("tm", "batch"), None),
            P(), P("batch", "tm"), P(), P(),
            P("batch", "tm"), P("batch", "tm"), P("batch", "tm"), P("batch"), P("batch"),
        ),
        out_specs=(P(("tm", "batch"), None), P(("tm", "batch"), None), P("batch", "tm")),
        check_vma=False,
    )
```

```python
import jax
import jax.numpy as jnp
from jax import lax
from jax.experimental import pallas as pl
from jax.experimental.pallas import tpu as pltpu
from jax.sharding import PartitionSpec as P

NMAX = 8
DISCOUNT = 0.99
ENTROPY_COEFF = 0.2
POLYAK_RATE = 0.005
STEP_SIZE = 0.1

F32 = jnp.float32
BF16 = jnp.bfloat16
MESH = pl.DeviceIdType.MESH

D = 2048
H = 2048
HALF = H // 2
T = 64
PAIR = 8
ROWS = T * PAIR
TM = 16
SCALE = D ** (-0.5)

WIDTHS = (384, 384, 256)
OFFSETS = (0, 384, 768)
ORDERS = (("z", "x", "y"), ("y", "z", "x"), ("x", "y", "z"))
PARTS = (2, 0, 1)
AG_SEMS = 23
RS_SEMS = 23
LINES = (2, 3, 1, 0)


def kernel(
    obs, nxt, onw, tgw, ld, step, onh, tgh, rew, logp, rst, hor, burn,
    gw, ret,
    xr_o, xr_n, xp_o, xp_n, xt, wst,
    wt0, wt1, wt2, wo0, wo1, wo2,
    pk_m, pk_i, bc0, bc1, qa0, qa1, cc, ss, pf, tp, vt, vo,
    sf, dall, ends_t, ends_o, lv, carry,
    q_s, q_r, nb_s, nb_r, du,
    g0, g1, g2,
    sh0, sh1, sh2, sw0, sw1, sw2, sb0, sb1, sb2,
    rh0, rh1, rh2, rw0, rw1, rw2, rb0, rb1, rb2,
    gx_s, gx_r,
    ag_ss, ag_rs, rs_ss, rs_rs, pre_ss, pre_rs, loc_sem, d2d_ss, d2d_rs, nb_sem,
):
    tm = lax.axis_index("tm")
    batch = lax.axis_index("batch")
    y, x = tm // 4, tm % 4
    z, c = batch // 2, batch % 2
    at = {"y": y, "x": x, "z": z}
    other = 1 - c
    wb = ((wt0, wt1, wt2), (wo0, wo1, wo2))
    gg = (g0, g1, g2)
    snd_h, snd_w, snd_b = (sh0, sh1, sh2), (sw0, sw1, sw2), (sb0, sb1, sb2)
    rcv_h, rcv_w, rcv_b = (rh0, rh1, rh2), (rw0, rw1, rw2), (rb0, rb1, rb2)
    pending = []

    def device(**moved):
        here = {**at, **moved}
        return {"tm": here["y"] * 4 + here["x"], "batch": here["z"] * 2 + c}

    partner = {"tm": tm, "batch": z * 2 + other}

    def remote(src, dst, ss_, rs_, dev):
        return pltpu.make_async_remote_copy(
            src_ref=src, dst_ref=dst, send_sem=ss_, recv_sem=rs_, device_id=dev,
            device_id_type=MESH,
        )

    def send(src, dst, ss_, rs_, dev):
        copy = remote(src, dst, ss_, rs_, dev)
        copy.start()
        pending.append(copy)

    mine = pl.ds(pl.multiple_of(c * HALF, HALF), HALF)
    theirs = pl.ds(pl.multiple_of(other * HALF, HALF), HALF)
    own_rows = pl.ds(pl.multiple_of(c * 16, 16), 16)
    other_rows = pl.ds(pl.multiple_of(other * 16, 16), 16)
    for m, w in enumerate((tgw, onw)):
        wst[m] = w[:, theirs].astype(BF16)
        for p in range(3):
            cols = pl.ds(pl.multiple_of(c * HALF + OFFSETS[p], 128), WIDTHS[p])
            wb[m][p][y, x, z, own_rows, :] = w[:, cols].astype(BF16)

    row8 = lax.broadcasted_iota(jnp.int32, (PAIR, 128), 0)
    lane8 = lax.broadcasted_iota(jnp.int32, (PAIR, 128), 1)
    row_own = (row8[:, :T] // 4) == c

    def twice(v):
        return jnp.where(row_own, jnp.concatenate([v, v], axis=0), 0.0)

    pk_m[...] = jnp.zeros_like(pk_m)
    for slot, r in enumerate((step, rew, logp)):
        pk_m[slot, :, :T] = twice(r[...])
    pk_m[3, :, :T] = twice(rst[...].astype(F32))
    hz = jnp.zeros((PAIR, 128), F32)
    bz = jnp.zeros((PAIR, 128), F32)
    for i in range(4):
        sel = row8 == c * 4 + i
        hz = jnp.where(sel, hor[i].astype(F32), hz)
        bz = jnp.where(sel, burn[i].astype(F32), bz)
    pk_m[4] = hz
    pk_m[5] = bz

    own_half = pl.ds(pl.multiple_of(c * 256, 256), 256)
    other_half = pl.ds(pl.multiple_of(other * 256, 256), 256)
    local = [
        pltpu.make_async_copy(nxt, xr_n.at[own_half, :], loc_sem.at[0]),
        pltpu.make_async_copy(obs, xr_o.at[own_half, :], loc_sem.at[1]),
    ]
    for copy in local:
        copy.start()

    barrier = pltpu.get_barrier_semaphore()
    peers = [partner] + [device(z=lax.rem(z + d, 4)) for d in range(1, 4)]
    peers += [{"tm": lax.rem(tm + d, TM), "batch": batch} for d in range(1, TM)]
    for dev in peers:
        pl.semaphore_signal(barrier, inc=1, device_id=dev, device_id_type=MESH)
    pl.semaphore_wait(barrier, len(peers))

    def w_half(m, p):
        cols = pl.ds(OFFSETS[p], WIDTHS[p])
        return wst.at[m, :, cols], wb[m][p].at[y, x, z, own_rows, :]

    def w_half_in(m, p):
        dst = wb[m][p].at[y, x, z, other_rows, :]
        remote(dst, dst, d2d_ss.at[m * 3 + p], d2d_rs.at[m * 3 + p], partner).wait_recv()

    for m in range(2):
        for p in range(3):
            src, dst = w_half(m, p)
            send(src, dst, d2d_ss.at[m * 3 + p], d2d_rs.at[m * 3 + p], partner)
    send(pk_m, pk_i, d2d_ss.at[6], d2d_rs.at[6], partner)
    send(nxt, xr_n.at[own_half, :], d2d_ss.at[7], d2d_rs.at[7], partner)
    send(obs, xr_o.at[own_half, :], d2d_ss.at[8], d2d_rs.at[8], partner)

    def place(p, first, second, last):
        idx = dict(zip(ORDERS[p], (first, second, last)))
        return idx["y"], idx["x"], idx["z"]

    def turned(p, i, d):
        return lax.rem(at[ORDERS[p][i]] + d, 4)

    def toward(p, i, d):
        return device(**{ORDERS[p][i]: turned(p, i, d)})

    FULL = pl.ds(0, 4)

    def half_of(h):
        return FULL if h is None else pl.ds(2 * h, 2)

    def ag_copy(m, p, j, where, dev):
        ref = wb[m][p].at[where]
        n = (m * 3 + p) * AG_SEMS + j
        return remote(ref, ref, ag_ss.at[n], ag_rs.at[n], dev)

    def ag_send(m, p, j, where, dev):
        copy = ag_copy(m, p, j, where, dev)
        copy.start()
        pending.append(copy)

    def ag_wait(m, p, j, where, dev):
        ag_copy(m, p, j, where, dev).wait_recv()

    def line(p, second, last, h=None):
        return place(p, half_of(h), second, last)

    def ag_one(m, p):
        for d in (2, 1, 3):
            ag_send(m, p, d - 1, (y, x, z), toward(p, 0, d))

    def ag_one_in(m, p):
        for d in (1, 3, 2):
            where = place(p, turned(p, 0, 4 - d), turned(p, 1, 0), turned(p, 2, 0))
            ag_wait(m, p, d - 1, where, toward(p, 0, 4 - d))

    def ag_two(m, p):
        own = line(p, turned(p, 1, 0), turned(p, 2, 0))
        ag_send(m, p, 3, own, toward(p, 1, 1))
        ag_send(m, p, 4, own, toward(p, 1, 3))

    def ag_two_forward(m, p):
        q3 = turned(p, 2, 0)
        ag_wait(m, p, 3, line(p, turned(p, 1, 3), q3), toward(p, 1, 3))
        ag_send(m, p, 5, line(p, turned(p, 1, 3), q3, 0), toward(p, 1, 1))
        ag_wait(m, p, 4, line(p, turned(p, 1, 1), q3), toward(p, 1, 1))
        ag_send(m, p, 6, line(p, turned(p, 1, 1), q3, 1), toward(p, 1, 3))

    def ag_two_last(m, p):
        q3 = turned(p, 2, 0)
        ag_wait(m, p, 5, line(p, turned(p, 1, 2), q3, 0), toward(p, 1, 3))
        ag_wait(m, p, 6, line(p, turned(p, 1, 2), q3, 1), toward(p, 1, 1))

    def ag_three(m, p, l):
        own = line(p, turned(p, 1, l), turned(p, 2, 0))
        ag_send(m, p, 7 + 4 * l, own, toward(p, 2, 1))
        ag_send(m, p, 8 + 4 * l, own, toward(p, 2, 3))

    def ag_three_forward(m, p, l):
        second = turned(p, 1, l)
        ag_wait(m, p, 7 + 4 * l, line(p, second, turned(p, 2, 3)), toward(p, 2, 3))
        ag_send(m, p, 9 + 4 * l, line(p, second, turned(p, 2, 3), 0), toward(p, 2, 1))
        ag_wait(m, p, 8 + 4 * l, line(p, second, turned(p, 2, 1)), toward(p, 2, 1))
        ag_send(m, p, 10 + 4 * l, line(p, second, turned(p, 2, 1), 1), toward(p, 2, 3))

    def ag_three_last(m, p):
        for l in range(4):
            second = turned(p, 1, l)
            ag_wait(m, p, 9 + 4 * l, line(p, second, turned(p, 2, 2), 0), toward(p, 2, 3))
            ag_wait(m, p, 10 + 4 * l, line(p, second, turned(p, 2, 2), 1), toward(p, 2, 1))

    def cols_of(p):
        return pl.ds(OFFSETS[p], WIDTHS[p])

    def wide(v, w=HALF):
        return jnp.concatenate([v] * (w // 128), axis=1)

    def at_t(t):
        return pl.ds(pl.multiple_of(t * PAIR, PAIR), PAIR)

    def spread_lanes(dst, v):
        for t in range(T):
            dst[pl.ds(t * PAIR, PAIR), :] = jnp.broadcast_to(v[:, t : t + 1], (PAIR, 128))

    r_out = lax.broadcasted_iota(jnp.int32, (ROWS, ROWS), 0)
    r_in = lax.broadcasted_iota(jnp.int32, (ROWS, ROWS), 1)

    def permutation():
        return jnp.where(r_out == (r_in % T) * PAIR + r_in // T, 1.0, 0.0).astype(BF16)

    def permute_next():
        perm = permutation()

        def body(i, _):
            cols = pl.ds(pl.multiple_of(i * 256, 256), 256)
            xp_n[:, cols] = jnp.dot(perm, xr_n[:, cols], preferred_element_type=F32).astype(BF16)
            return 0

        lax.fori_loop(0, D // 256, body, 0)

    def permute_obs(lo, hi):
        perm = permutation()

        def body(i, _):
            cols = pl.ds(pl.multiple_of(i * 256, 256), 256)
            v = jnp.dot(perm, xr_o[:, cols], preferred_element_type=F32)
            xp_o[:, cols] = v.astype(BF16)
            xt[i // 2, pl.ds(2 * (i % 2), 2)] = v.T.astype(BF16).reshape(2, 4, 32, ROWS)
            return 0

        lax.fori_loop(lo, hi, body, 0)

    def project(m, p, xp, v):
        def tile(i, _):
            rows = pl.ds(pl.multiple_of(i * 256, 256), 256)
            w = wb[m][p][...].reshape(D, WIDTHS[p])
            acc = jnp.dot(xp[rows, :], w, preferred_element_type=F32)
            v[rows, cols_of(p)] = acc * SCALE
            return 0

        lax.fori_loop(0, ROWS // 256, tile, 0)

    def scan(v, p, ends):
        cols = cols_of(p)

        def body(i, st):
            for k in range(4):
                rows = at_t(i * 4 + k)
                st = cc[rows, cols] * st + ss[rows, cols] * v[rows, cols]
                v[rows, cols] = st
            return st

        ends[tm, :, cols] = lax.fori_loop(0, T // 4, body, jnp.zeros((PAIR, WIDTHS[p]), F32))

    def ends_copy(n, ends, p, slot, d, dev):
        cols = pl.ds(0, HALF) if p is None else cols_of(p)
        ref = ends.at[slot, :, cols]
        return remote(ref, ref, pre_ss.at[n, d], pre_rs.at[n, slot], dev)

    def prefix_send(n, ends, p, forward):
        for d in range(TM - 1, 0, -1):
            to = tm + d if forward else tm - d

            @pl.when(to < TM if forward else to >= 0)
            def _(d=d, to=to):
                ends_copy(n, ends, p, tm, d, {"tm": to, "batch": batch}).start()

    def prefix_take(n, ends, p, forward):
        cols = pl.ds(0, HALF) if p is None else cols_of(p)
        carry[:, cols] = jnp.zeros_like(carry[:, cols])
        for j in range(TM - 1) if forward else range(TM - 1, 0, -1):

            @pl.when(j < tm if forward else j > tm)
            def _(j=j):
                ends_copy(n, ends, p, j, 0, {"tm": j, "batch": batch}).wait_recv()
                carry[:, cols] = dall[j, :, cols] * carry[:, cols] + ends[j, :, cols]

    def prefix_drain(n, ends, p, forward):
        for d in range(1, TM):
            to = tm + d if forward else tm - d

            @pl.when(to < TM if forward else to >= 0)
            def _(d=d, to=to):
                ends_copy(n, ends, p, tm, d, {"tm": to, "batch": batch}).wait_send()

    def quality(v, heads, p, fresh, slope):
        cols, w = cols_of(p), WIDTHS[p]
        hcols = pl.ds(pl.multiple_of(c * HALF + OFFSETS[p], 128), w)
        h0 = jnp.broadcast_to(heads[0:1, hcols], (PAIR, w))
        h1 = jnp.broadcast_to(heads[1:2, hcols], (PAIR, w))
        start = carry[:, cols]

        def fold(u):
            out = u[:, :128]
            for i in range(1, w // 128):
                out = out + u[:, i * 128 : (i + 1) * 128]
            return out

        def body(i, _):
            for k in range(4):
                rows = at_t(i * 4 + k)
                st = v[rows, cols] + pf[rows, cols] * start
                sig = 1.0 / (1.0 + jnp.exp(-st))
                act = st * sig
                if slope:
                    v[rows, cols] = (sig + act * (1.0 - sig)) * (H ** (-0.5))
                f0, f1 = fold(act * h0), fold(act * h1)
                qa0[rows, :] = f0 if fresh else qa0[rows, :] + f0
                qa1[rows, :] = f1 if fresh else qa1[rows, :] + f1
            return 0

        lax.fori_loop(0, T // 4, body, 0)

    def quality_send(slot):
        def body(i, acc):
            a0, a1 = acc
            for k in range(8):
                rows = at_t(i * 8 + k)
                here = lane8 == i * 8 + k
                a0 = jnp.where(here, jnp.sum(qa0[rows, :], axis=1, keepdims=True), a0)
                a1 = jnp.where(here, jnp.sum(qa1[rows, :], axis=1, keepdims=True), a1)
            return a0, a1

        zero = jnp.zeros((PAIR, 128), F32)
        a0, a1 = lax.fori_loop(0, T // 8, body, (zero, zero))
        q_s[slot, 0] = a0
        q_s[slot, 1] = a1
        send(q_s.at[slot], q_r.at[slot], d2d_ss.at[9 + slot], d2d_rs.at[9 + slot], partner)

    def quality_sum(slot):
        remote(
            q_s.at[slot], q_r.at[slot], d2d_ss.at[9 + slot], d2d_rs.at[9 + slot], partner
        ).wait_recv()
        return [(q_s[slot, k] + q_r[slot, k]) * (H ** (-0.5)) for k in range(2)]

    for m in range(2):
        for p in range(3):
            w_half_in(m, p)
            ag_one(m, p)
    for p in range(3):
        ag_one_in(0, p)
        ag_two(0, p)
        ag_three(0, p, 0)
    for p in range(3):
        ag_one_in(1, p)
        ag_two(1, p)
    remote(pk_m, pk_i, d2d_ss.at[6], d2d_rs.at[6], partner).wait_recv()
    step8 = pk_m[0] + pk_i[0]
    rew8 = pk_m[1] + pk_i[1]
    logp8 = pk_m[2] + pk_i[2]
    rst8 = pk_m[3] + pk_i[3]
    keep8 = 1.0 - rst8
    hor8 = pk_m[4] + pk_i[4]
    burn8 = pk_m[5] + pk_i[5]

    sf[tm, 0] = jnp.broadcast_to(jnp.sum(step8, axis=1, keepdims=True), (PAIR, 128))
    sf[tm, 1] = jnp.broadcast_to(1.0 - jnp.max(rst8, axis=1, keepdims=True), (PAIR, 128))
    for d in range(1, TM):
        dev = {"tm": lax.rem(tm + d, TM), "batch": batch}
        send(sf.at[tm], sf.at[tm], pre_ss.at[0, d], pre_rs.at[0, tm], dev)

    spread_lanes(bc0, step8)
    spread_lanes(bc1, keep8)
    ld8 = jnp.broadcast_to(ld[:, mine], (PAIR, HALF))

    def factors(t, prod):
        e = jnp.exp(wide(bc0[at_t(t), :]) * ld8)
        f = e * wide(bc1[at_t(t), :])
        cc[at_t(t), :] = f
        ss[at_t(t), :] = jnp.sqrt(1.0 - e * e)
        prod = prod * f
        pf[at_t(t), :] = prod
        return prod

    lax.fori_loop(0, T, factors, jnp.ones((PAIR, HALF), F32))
    for p in range(3):
        ag_two_forward(0, p)
        ag_three(0, p, 3)
        ag_three(0, p, 1)
    for p in range(3):
        ag_three_forward(0, p, 0)
    local[0].wait()
    remote(nxt, xr_n.at[other_half, :], d2d_ss.at[7], d2d_rs.at[7], partner).wait_recv()
    permute_next()
    for p in range(3):
        ag_two_forward(1, p)
        ag_three(1, p, 0)
    for p in range(3):
        ag_two_last(0, p)
        ag_three(0, p, 2)
    def tails(i, prod):
        t = T - 1 - i
        tp[at_t(t), :] = prod
        return prod * cc[at_t(t), :]

    lax.fori_loop(0, T, tails, jnp.ones((PAIR, HALF), F32))
    local[1].wait()
    remote(obs, xr_o.at[other_half, :], d2d_ss.at[8], d2d_rs.at[8], partner).wait_recv()
    for l in (3, 1):
        for p in range(3):
            ag_three_forward(0, p, l)
    for p in range(3):
        ag_three(1, p, 3)
        ag_three(1, p, 1)
        ag_two_last(1, p)
    permute_obs(0, 4)
    for p in range(3):
        ag_three_forward(0, p, 2)
        ag_three(1, p, 2)
    permute_obs(4, 8)

    for d in range(1, TM):
        j = lax.rem(tm + d, TM)
        dev = {"tm": j, "batch": batch}
        remote(sf.at[j], sf.at[j], pre_ss.at[0, d], pre_rs.at[0, j], dev).wait_recv()

    def block_decay(j, _):
        dall[j] = jnp.exp(wide(sf[j, 0]) * ld8) * wide(sf[j, 1])
        return 0

    lax.fori_loop(0, TM, block_decay, 0)

    for p in range(3):
        ag_three_forward(1, p, 0)
    for p in PARTS[:2]:
        ag_three_last(0, p)
        project(0, p, xp_n, vt)
        scan(vt, p, ends_t)
    for p in range(3):
        ag_three_forward(1, p, 3)
    for p in PARTS[2:]:
        ag_three_last(0, p)
        project(0, p, xp_n, vt)
        scan(vt, p, ends_t)
    prefix_send(1, ends_t, None, True)
    for l in (1, 2):
        for p in range(3):
            ag_three_forward(1, p, l)
    ag_three_last(1, PARTS[0])
    project(1, PARTS[0], xp_o, vo)
    scan(vo, PARTS[0], ends_o)
    prefix_send(2 + PARTS[0], ends_o, PARTS[0], True)
    prefix_take(1, ends_t, None, True)
    for p in PARTS:
        quality(vt, tgh, p, p == PARTS[0], False)
    quality_send(0)
    for p in PARTS[1:]:
        ag_three_last(1, p)
    for p in PARTS[1:]:
        project(1, p, xp_o, vo)
        scan(vo, p, ends_o)
        prefix_send(2 + p, ends_o, p, True)
    tq = quality_sum(0)
    value8 = jnp.minimum(tq[0], tq[1]) - ENTROPY_COEFF * logp8
    nb_s[0] = rew8
    nb_s[1] = value8
    nb_s[2] = keep8
    before = {"tm": lax.rem(tm + TM - 1, TM), "batch": batch}
    send(nb_s, nb_r, nb_sem.at[0], nb_sem.at[1], before)
    prefix_take(2 + PARTS[0], ends_o, PARTS[0], True)
    quality(vo, onh, PARTS[0], True, True)

    remote(nb_s, nb_r, nb_sem.at[0], nb_sem.at[1], before).wait_recv()
    inside = (lane8 >= T) & (lane8 < T + NMAX) & (tm < TM - 1)

    def extended(own, slot):
        later = jnp.where(inside, pltpu.roll(nb_r[slot], T, 1), 0.0)
        return jnp.where(lane8 < T, own, later)

    ext_r, ext_v, ext_k = extended(rew8, 0), extended(value8, 1), extended(keep8, 2)

    def shifted(v, n):
        return v if n == 0 else pltpu.roll(v, 128 - n, 1)

    total = jnp.zeros((PAIR, 128), F32)
    alive = jnp.ones((PAIR, 128), F32)
    for n in range(NMAX):
        total = total + jnp.where(hor8 > n, DISCOUNT**n * alive * shifted(ext_r, n), 0.0)
        alive = alive * shifted(ext_k, n + 1)
        total = total + jnp.where(
            hor8 == n + 1, DISCOUNT ** (n + 1) * alive * shifted(ext_v, n + 1), 0.0
        )
    ret[...] = jnp.where(c == 0, total[:4, :T], total[4:, :T])
    weight = jnp.where((lane8 + tm * T).astype(F32) >= burn8, 1.0, 0.0)

    for p in PARTS[1:]:
        prefix_take(2 + p, ends_o, p, True)
        quality(vo, onh, p, False, True)
    quality_send(1)
    oq = quality_sum(1)
    spread_lanes(bc0, weight * (oq[0] - total))
    spread_lanes(bc1, weight * (oq[1] - total))

    for p in PARTS:
        cols, w = cols_of(p), WIDTHS[p]
        hcols = pl.ds(pl.multiple_of(c * HALF + OFFSETS[p], 128), w)
        h0 = jnp.broadcast_to(onh[0:1, hcols], (PAIR, w))
        h1 = jnp.broadcast_to(onh[1:2, hcols], (PAIR, w))

        def back(i, adj, cols=cols, w=w, h0=h0, h1=h1):
            for k in range(4):
                rows = at_t(T - 1 - (i * 4 + k))
                dh = wide(bc0[rows, :], w) * h0 + wide(bc1[rows, :], w) * h1
                adj = dh * vo[rows, cols] + adj
                vo[rows, cols] = adj
                adj = cc[rows, cols] * adj
            return adj

        lv[tm, :, cols] = lax.fori_loop(0, T // 4, back, jnp.zeros((PAIR, w), F32))
        prefix_send(5 + p, lv, p, False)

    def finish(p):
        prefix_take(5 + p, lv, p, False)
        cols = cols_of(p)
        incoming = carry[:, cols]
        both = jnp.concatenate([incoming, incoming], axis=0)

        def body(i, _):
            for k in range(2):
                rows = pl.ds(pl.multiple_of(i * 32 + k * 16, 16), 16)
                adj = vo[rows, cols] + tp[rows, cols] * both
                du[rows, cols] = (ss[rows, cols] * adj).astype(BF16)
            return 0

        lax.fori_loop(0, ROWS // 32, body, 0)

    def gradient(p, l):
        where = place(p, FULL, turned(p, 1, l), FULL)
        lhs = xt[where].reshape(512, ROWS)
        v = jnp.dot(lhs, du[:, cols_of(p)], preferred_element_type=F32)
        gg[p][where] = v.reshape(4, 4, 32, WIDTHS[p])

    def rs_copy(p, j, src, dst, dev):
        n = p * RS_SEMS + j
        return remote(src, dst, rs_ss.at[n], rs_rs.at[n], dev)

    def rs_send(p, j, src, dst, dev):
        copy = rs_copy(p, j, src, dst, dev)
        copy.start()
        pending.append(copy)

    def rs_ref(p, s, d, h=None):
        if s < 4:
            return line(p, turned(p, 1, s), turned(p, 2, d), h)
        return line(p, turned(p, 1, d), turned(p, 2, 0), h)

    def rs_axis(s):
        return 2 if s < 4 else 1

    def rs_opposite(p, s):
        for h, d in ((0, 3), (1, 1)):
            snd_h[p][s, h] = gg[p][rs_ref(p, s, 2, h)].astype(BF16)
            rs_send(
                p, 4 * s + h, snd_h[p].at[s, h], rcv_h[p].at[s, h], toward(p, rs_axis(s), d)
            )

    def rs_neighbour(p, s, h):
        d = (3, 1)[h]
        rs_copy(
            p, 4 * s + h, snd_h[p].at[s, h], rcv_h[p].at[s, h], toward(p, rs_axis(s), 4 - d)
        ).wait_recv()
        with_recv = gg[p][rs_ref(p, s, d, h)] + rcv_h[p][s, h].astype(F32)
        snd_w[p][s, h, pl.ds(2 * h, 2)] = with_recv.astype(BF16)
        snd_w[p][s, h, pl.ds(2 - 2 * h, 2)] = gg[p][rs_ref(p, s, d, 1 - h)].astype(BF16)
        rs_send(
            p, 4 * s + 2 + h, snd_w[p].at[s, h], rcv_w[p].at[s, h], toward(p, rs_axis(s), d)
        )

    def rs_sum(p, s):
        for h, d in ((0, 1), (1, 3)):
            rs_copy(
                p, 4 * s + 2 + h, snd_w[p].at[s, h], rcv_w[p].at[s, h], toward(p, rs_axis(s), d)
            ).wait_recv()
        own = rs_ref(p, s, 0)
        both = rcv_w[p][s, 0].astype(F32) + rcv_w[p][s, 1].astype(F32)
        gg[p][own] = gg[p][own] + both

    def rs_one(p):
        for d in (2, 1, 3):
            block = gg[p][place(p, turned(p, 0, d), turned(p, 1, 0), turned(p, 2, 0))]
            snd_b[p][d - 1] = block.astype(BF16)
            rs_send(p, 19 + d, snd_b[p].at[d - 1], rcv_b[p].at[d - 1], toward(p, 0, d))

    def rs_one_sum(p):
        v = gg[p][y, x, z]
        for d in (1, 3, 2):
            rs_copy(
                p, 19 + d, snd_b[p].at[d - 1], rcv_b[p].at[d - 1], toward(p, 0, 4 - d)
            ).wait_recv()
            v = v + rcv_b[p][d - 1].astype(F32)
        gg[p][y, x, z] = v * SCALE

    for p in PARTS:
        finish(p)
        gradient(p, LINES[0])
        rs_opposite(p, LINES[0])
    for p in PARTS:
        gradient(p, LINES[1])
        rs_opposite(p, LINES[1])
    for i in range(4):
        if i < 2:
            for p in PARTS:
                gradient(p, LINES[i + 2])
                rs_opposite(p, LINES[i + 2])
        for p in PARTS:
            rs_neighbour(p, LINES[i], 0)
            rs_neighbour(p, LINES[i], 1)
    for p in PARTS:
        rs_sum(p, LINES[0])
        rs_opposite(p, 4)
    for p in PARTS:
        rs_sum(p, LINES[1])
        rs_neighbour(p, 4, 0)
        rs_sum(p, LINES[2])
        rs_neighbour(p, 4, 1)
    for p in PARTS:
        rs_sum(p, LINES[3])
    for p in PARTS:
        rs_sum(p, 4)
        rs_one(p)
    for p in PARTS:
        rs_one_sum(p)

    for p in range(3):
        gx_s[:, cols_of(p)] = gg[p][y, x, z, other_rows, :]
    send(gx_s, gx_r, d2d_ss.at[11], d2d_rs.at[11], partner)
    for p in range(3):
        cols = pl.ds(pl.multiple_of(c * HALF + OFFSETS[p], 128), WIDTHS[p])
        gw[:, cols] = gg[p][y, x, z, own_rows, :]
    remote(gx_s, gx_r, d2d_ss.at[11], d2d_rs.at[11], partner).wait_recv()
    gw[:, theirs] = gx_r[...]

    prefix_drain(1, ends_t, None, True)
    for p in range(3):
        prefix_drain(2 + p, ends_o, p, True)
        prefix_drain(5 + p, lv, p, False)
    for copy in pending:
        copy.wait_send()


def shards(
    obs_feats, next_feats, online_w, target_w, log_decay, step_scale, online_heads, target_heads,
    reward, next_action_log_prob, resets, horizon, burn_in,
):
    vmem = pl.BlockSpec(memory_space=pltpu.VMEM)
    smem = pl.BlockSpec(memory_space=pltpu.SMEM)
    hbm = pl.BlockSpec(memory_space=pl.ANY)
    weights = [pltpu.VMEM((4, 4, 4, 32, w), BF16) for w in WIDTHS]
    staged = [
        *[pltpu.VMEM((5, 2, 2, 32, w), BF16) for w in WIDTHS],
        *[pltpu.VMEM((5, 2, 4, 32, w), BF16) for w in WIDTHS],
        *[pltpu.VMEM((3, 32, w), BF16) for w in WIDTHS],
    ]
    big = pltpu.VMEM((ROWS, HALF), F32)
    ends = pltpu.VMEM((TM, PAIR, HALF), F32)
    narrow = pltpu.VMEM((ROWS, 128), F32)
    scratch = [
        pltpu.VMEM((ROWS, D), BF16), pltpu.VMEM((ROWS, D), BF16),
        pltpu.VMEM((ROWS, D), BF16), pltpu.VMEM((ROWS, D), BF16),
        pltpu.VMEM((4, 4, 4, 32, ROWS), BF16), pltpu.VMEM((2, 16, HALF), BF16),
        *weights, *weights,
        pltpu.VMEM((6, PAIR, 128), F32), pltpu.VMEM((6, PAIR, 128), F32),
        narrow, narrow, narrow, narrow,
        big, big, big, big, big, big,
        pltpu.VMEM((TM, 2, PAIR, 128), F32), ends, ends, ends, ends,
        pltpu.VMEM((PAIR, HALF), F32),
        pltpu.VMEM((2, 2, PAIR, 128), F32), pltpu.VMEM((2, 2, PAIR, 128), F32),
        pltpu.VMEM((3, PAIR, 128), F32), pltpu.VMEM((3, PAIR, 128), F32),
        pltpu.VMEM((ROWS, HALF), BF16),
        *[pltpu.VMEM((4, 4, 4, 32, w), F32) for w in WIDTHS],
        *staged, *staged,
        pltpu.VMEM((16, HALF), F32), pltpu.VMEM((16, HALF), F32),
        pltpu.SemaphoreType.DMA((6 * AG_SEMS,)), pltpu.SemaphoreType.DMA((6 * AG_SEMS,)),
        pltpu.SemaphoreType.DMA((3 * RS_SEMS,)), pltpu.SemaphoreType.DMA((3 * RS_SEMS,)),
        pltpu.SemaphoreType.DMA((8, TM)), pltpu.SemaphoreType.DMA((8, TM)),
        pltpu.SemaphoreType.DMA((2,)),
        pltpu.SemaphoreType.DMA((12,)), pltpu.SemaphoreType.DMA((12,)),
        pltpu.SemaphoreType.DMA((2,)),
    ]
    rows_b, span, width = obs_feats.shape
    grad_w, returns = pl.pallas_call(
        kernel,
        name="critic_step",
        out_shape=(
            jax.ShapeDtypeStruct(online_w.shape, F32),
            jax.ShapeDtypeStruct(reward.shape, F32),
        ),
        in_specs=[hbm, hbm] + [vmem] * 9 + [smem] * 2,
        out_specs=(vmem, vmem),
        scratch_shapes=scratch,
        compiler_params=pltpu.CompilerParams(
            collective_id=0, has_side_effects=True, vmem_limit_bytes=62 * 1024 * 1024
        ),
    )(
        obs_feats.reshape(rows_b * span, width), next_feats.reshape(rows_b * span, width),
        online_w, target_w, log_decay[None], step_scale, online_heads, target_heads,
        reward, next_action_log_prob, resets, horizon, burn_in,
    )
    new_target = (1.0 - POLYAK_RATE) * target_w + POLYAK_RATE * (online_w - STEP_SIZE * grad_w)
    return grad_w, new_target, returns


def solution(mesh):
    return jax.shard_map(
        shards,
        mesh=mesh,
        in_specs=(
            P("batch", "tm", None), P("batch", "tm", None),
            P(("tm", "batch"), None), P(("tm", "batch"), None),
            P(), P("batch", "tm"), P(), P(),
            P("batch", "tm"), P("batch", "tm"), P("batch", "tm"), P("batch"), P("batch"),
        ),
        out_specs=(P(("tm", "batch"), None), P(("tm", "batch"), None), P("batch", "tm")),
        check_vma=False,
    )
```

```python
import jax
import jax.numpy as jnp
from jax import lax
from jax.experimental import pallas as pl
from jax.experimental.pallas import tpu as pltpu
from jax.sharding import PartitionSpec as P

NMAX = 8
DISCOUNT = 0.99
ENTROPY_COEFF = 0.2
POLYAK_RATE = 0.005
STEP_SIZE = 0.1

F32 = jnp.float32
BF16 = jnp.bfloat16
MESH = pl.DeviceIdType.MESH

D = 2048
H = 2048
HALF = H // 2
T = 64
PAIR = 8
ROWS = T * PAIR
TM = 16
SCALE = D ** (-0.5)

WIDTHS = (384, 384, 256)
OFFSETS = (0, 384, 768)
ORDERS = (("z", "x", "y"), ("y", "z", "x"), ("x", "y", "z"))
PARTS = (2, 0, 1)
AG_SEMS = 13
RS_SEMS = 16
LINES = (2, 3, 1, 0)


def kernel(
    obs, nxt, onw, tgw, ld, step, onh, tgh, rew, logp, rst, hor, burn,
    gw, ret,
    xr_o, xr_n, xp_o, xp_n, xt, wst,
    wt0, wt1, wt2, wo0, wo1, wo2,
    pk_m, pk_i, bc0, bc1, qa0, qa1, cc, ss, pf, tp, vt, vo,
    sf, dall, ends_t, ends_o, lv, carry,
    q_s, q_r, nb_s, nb_r, du,
    g0, g1, g2,
    sh0, sh1, sh2, sw0, sw1, sw2, sb0, sb1, sb2,
    rh0, rh1, rh2, rw0, rw1, rw2, rb0, rb1, rb2,
    gx_s, gx_r,
    ag_ss, ag_rs, rs_ss, rs_rs, pre_ss, pre_rs, loc_sem, d2d_ss, d2d_rs, nb_sem,
):
    tm = lax.axis_index("tm")
    batch = lax.axis_index("batch")
    y, x = tm // 4, tm % 4
    z, c = batch // 2, batch % 2
    at = {"y": y, "x": x, "z": z}
    other = 1 - c
    wb = ((wt0, wt1, wt2), (wo0, wo1, wo2))
    gg = (g0, g1, g2)
    snd_h, snd_w, snd_b = (sh0, sh1, sh2), (sw0, sw1, sw2), (sb0, sb1, sb2)
    rcv_h, rcv_w, rcv_b = (rh0, rh1, rh2), (rw0, rw1, rw2), (rb0, rb1, rb2)
    pending = []

    def device(**moved):
        here = {**at, **moved}
        return {"tm": here["y"] * 4 + here["x"], "batch": here["z"] * 2 + c}

    partner = {"tm": tm, "batch": z * 2 + other}

    def remote(src, dst, ss_, rs_, dev):
        return pltpu.make_async_remote_copy(
            src_ref=src, dst_ref=dst, send_sem=ss_, recv_sem=rs_, device_id=dev,
            device_id_type=MESH,
        )

    def send(src, dst, ss_, rs_, dev):
        copy = remote(src, dst, ss_, rs_, dev)
        copy.start()
        pending.append(copy)

    mine = pl.ds(pl.multiple_of(c * HALF, HALF), HALF)
    theirs = pl.ds(pl.multiple_of(other * HALF, HALF), HALF)
    own_rows = pl.ds(pl.multiple_of(c * 16, 16), 16)
    other_rows = pl.ds(pl.multiple_of(other * 16, 16), 16)
    for m, w in enumerate((tgw, onw)):
        wst[m] = w[:, theirs].astype(BF16)
        for p in range(3):
            cols = pl.ds(pl.multiple_of(c * HALF + OFFSETS[p], 128), WIDTHS[p])
            wb[m][p][y, x, z, own_rows, :] = w[:, cols].astype(BF16)

    row8 = lax.broadcasted_iota(jnp.int32, (PAIR, 128), 0)
    lane8 = lax.broadcasted_iota(jnp.int32, (PAIR, 128), 1)
    row_own = (row8[:, :T] // 4) == c

    def twice(v):
        return jnp.where(row_own, jnp.concatenate([v, v], axis=0), 0.0)

    pk_m[...] = jnp.zeros_like(pk_m)
    for slot, r in enumerate((step, rew, logp)):
        pk_m[slot, :, :T] = twice(r[...])
    pk_m[3, :, :T] = twice(rst[...].astype(F32))
    hz = jnp.zeros((PAIR, 128), F32)
    bz = jnp.zeros((PAIR, 128), F32)
    for i in range(4):
        sel = row8 == c * 4 + i
        hz = jnp.where(sel, hor[i].astype(F32), hz)
        bz = jnp.where(sel, burn[i].astype(F32), bz)
    pk_m[4] = hz
    pk_m[5] = bz

    own_half = pl.ds(pl.multiple_of(c * 256, 256), 256)
    other_half = pl.ds(pl.multiple_of(other * 256, 256), 256)
    local = [
        pltpu.make_async_copy(nxt, xr_n.at[own_half, :], loc_sem.at[0]),
        pltpu.make_async_copy(obs, xr_o.at[own_half, :], loc_sem.at[1]),
    ]
    for copy in local:
        copy.start()

    barrier = pltpu.get_barrier_semaphore()
    peers = [partner] + [device(z=lax.rem(z + d, 4)) for d in range(1, 4)]
    peers += [{"tm": lax.rem(tm + d, TM), "batch": batch} for d in range(1, TM)]
    for dev in peers:
        pl.semaphore_signal(barrier, inc=1, device_id=dev, device_id_type=MESH)
    pl.semaphore_wait(barrier, len(peers))

    def w_half(m, p):
        src, dst = wst.at[m, :, cols_of(p)], wb[m][p].at[y, x, z, own_rows, :]
        return remote(src, dst, d2d_ss.at[0], d2d_rs.at[m], partner)

    def w_half_in(m):
        remote(wst.at[m], wst.at[m], d2d_ss.at[0], d2d_rs.at[m], partner).wait_recv()

    def cols_of(p):
        return pl.ds(OFFSETS[p], WIDTHS[p])

    for m in range(2):
        for p in range(3):
            w_half(m, p).start()
    send(pk_m, pk_i, d2d_ss.at[2], d2d_rs.at[2], partner)
    send(nxt, xr_n.at[own_half, :], d2d_ss.at[3], d2d_rs.at[3], partner)
    send(obs, xr_o.at[own_half, :], d2d_ss.at[4], d2d_rs.at[4], partner)

    def place(p, first, second, last):
        idx = dict(zip(ORDERS[p], (first, second, last)))
        return idx["y"], idx["x"], idx["z"]

    def turned(p, i, d):
        return lax.rem(at[ORDERS[p][i]] + d, 4)

    def toward(p, i, d):
        return device(**{ORDERS[p][i]: turned(p, i, d)})

    FULL = pl.ds(0, 4)

    def half_of(h):
        return FULL if h is None else pl.ds(2 * h, 2)

    def ag_copy(m, p, k, j, where, dev):
        ref = wb[m][p].at[where]
        n = m * 3 + p
        return remote(ref, ref, ag_ss.at[n * 3 + k], ag_rs.at[n * AG_SEMS + j], dev)

    def ag_send(m, p, k, j, where, dev):
        ag_copy(m, p, k, j, where, dev).start()

    def ag_wait(m, p, j, where):
        ag_copy(m, p, 0, j, where, partner).wait_recv()

    def ag_drain(m, p):
        for k, where in enumerate(((0, 0, pl.ds(0, 3)), (0, pl.ds(0, 3)), (pl.ds(0, 3),))):
            ag_copy(m, p, k, 0, where, partner).wait_send()

    def line(p, second, last, h=None):
        return place(p, half_of(h), second, last)

    def ag_one(m, p):
        for d in (2, 1, 3):
            ag_send(m, p, 0, 0, (y, x, z), toward(p, 0, d))

    def ag_one_in(m, p):
        ag_wait(m, p, 0, (0, 0, pl.ds(0, 3)))

    def ag_two(m, p):
        own = line(p, turned(p, 1, 0), turned(p, 2, 0))
        ag_send(m, p, 1, 1, own, toward(p, 1, 1))
        ag_send(m, p, 1, 2, own, toward(p, 1, 3))

    def ag_two_forward(m, p):
        q3 = turned(p, 2, 0)
        ag_wait(m, p, 1, line(p, turned(p, 1, 3), q3))
        ag_send(m, p, 1, 3, line(p, turned(p, 1, 3), q3, 0), toward(p, 1, 1))
        ag_wait(m, p, 2, line(p, turned(p, 1, 1), q3))
        ag_send(m, p, 1, 3, line(p, turned(p, 1, 1), q3, 1), toward(p, 1, 3))

    def ag_two_last(m, p):
        ag_wait(m, p, 3, line(p, turned(p, 1, 2), turned(p, 2, 0)))

    def ag_three(m, p, l):
        own = line(p, turned(p, 1, l), turned(p, 2, 0))
        ag_send(m, p, 2, 4 + 2 * l, own, toward(p, 2, 1))
        ag_send(m, p, 2, 5 + 2 * l, own, toward(p, 2, 3))

    def ag_three_forward(m, p, l):
        second = turned(p, 1, l)
        ag_wait(m, p, 4 + 2 * l, line(p, second, turned(p, 2, 3)))
        ag_send(m, p, 2, 12, line(p, second, turned(p, 2, 3), 0), toward(p, 2, 1))
        ag_wait(m, p, 5 + 2 * l, line(p, second, turned(p, 2, 1)))
        ag_send(m, p, 2, 12, line(p, second, turned(p, 2, 1), 1), toward(p, 2, 3))

    def ag_three_last(m, p):
        ag_wait(m, p, 12, place(p, FULL, FULL, turned(p, 2, 2)))

    def wide(v, w=HALF):
        return jnp.concatenate([v] * (w // 128), axis=1)

    def at_t(t):
        return pl.ds(pl.multiple_of(t * PAIR, PAIR), PAIR)

    def spread_lanes(dst, v):
        for t in range(T):
            dst[pl.ds(t * PAIR, PAIR), :] = jnp.broadcast_to(v[:, t : t + 1], (PAIR, 128))

    r_out = lax.broadcasted_iota(jnp.int32, (ROWS, ROWS), 0)
    r_in = lax.broadcasted_iota(jnp.int32, (ROWS, ROWS), 1)

    def permutation():
        return jnp.where(r_out == (r_in % T) * PAIR + r_in // T, 1.0, 0.0).astype(BF16)

    def permute_next():
        perm = permutation()

        def body(i, _):
            cols = pl.ds(pl.multiple_of(i * 256, 256), 256)
            xp_n[:, cols] = jnp.dot(perm, xr_n[:, cols], preferred_element_type=F32).astype(BF16)
            return 0

        lax.fori_loop(0, D // 256, body, 0)

    def permute_obs(lo, hi):
        perm = permutation()

        def body(i, _):
            cols = pl.ds(pl.multiple_of(i * 256, 256), 256)
            v = jnp.dot(perm, xr_o[:, cols], preferred_element_type=F32)
            xp_o[:, cols] = v.astype(BF16)
            xt[i // 2, pl.ds(2 * (i % 2), 2)] = v.T.astype(BF16).reshape(2, 4, 32, ROWS)
            return 0

        lax.fori_loop(lo, hi, body, 0)

    def project(m, p, xp, v):
        def tile(i, _):
            rows = pl.ds(pl.multiple_of(i * 256, 256), 256)
            w = wb[m][p][...].reshape(D, WIDTHS[p])
            acc = jnp.dot(xp[rows, :], w, preferred_element_type=F32)
            v[rows, cols_of(p)] = acc * SCALE
            return 0

        lax.fori_loop(0, ROWS // 256, tile, 0)

    def scan(v, p, ends):
        cols = cols_of(p)

        def body(i, st):
            for k in range(4):
                rows = at_t(i * 4 + k)
                st = cc[rows, cols] * st + ss[rows, cols] * v[rows, cols]
                v[rows, cols] = st
            return st

        last = lax.fori_loop(0, T // 4, body, jnp.zeros((PAIR, WIDTHS[p]), F32))
        ends[tm, :, cols] = last.astype(BF16)

    def ends_copy(n, ends, p, slots, dev):
        cols = pl.ds(0, HALF) if p is None else cols_of(p)
        ref = ends.at[slots, :, cols]
        return remote(ref, ref, pre_ss.at[n], pre_rs.at[n], dev)

    def prefix_send(n, ends, p, forward):
        for d in range(TM - 1, 0, -1):
            to = tm + d if forward else tm - d

            @pl.when(to < TM if forward else to >= 0)
            def _(to=to):
                ends_copy(n, ends, p, tm, {"tm": to, "batch": batch}).start()

    def prefix_wait(n, ends, p, count, arrived):
        for k in range(1, TM):

            @pl.when(count == k)
            def _(k=k):
                copies = ends_copy(n, ends, p, pl.ds(0, k), partner)
                copies.wait_recv() if arrived else copies.wait_send()

    def prefix_take(n, ends, p, forward):
        cols, w = (pl.ds(0, HALF), HALF) if p is None else (cols_of(p), WIDTHS[p])
        count = tm if forward else TM - 1 - tm
        prefix_wait(n, ends, p, count, True)

        def body(i, v):
            j = i if forward else TM - 1 - i
            return dall[j, :, cols] * v + ends[j, :, cols].astype(F32)

        carry[:, cols] = lax.fori_loop(0, count, body, jnp.zeros((PAIR, w), F32))

    def prefix_drain(n, ends, p, forward):
        prefix_wait(n, ends, p, TM - 1 - tm if forward else tm, False)

    def quality(v, heads, p, fresh, slope):
        cols, w = cols_of(p), WIDTHS[p]
        hcols = pl.ds(pl.multiple_of(c * HALF + OFFSETS[p], 128), w)
        h0 = jnp.broadcast_to(heads[0:1, hcols], (PAIR, w))
        h1 = jnp.broadcast_to(heads[1:2, hcols], (PAIR, w))
        start = carry[:, cols]

        def fold(u):
            out = u[:, :128]
            for i in range(1, w // 128):
                out = out + u[:, i * 128 : (i + 1) * 128]
            return out

        def body(i, _):
            for k in range(4):
                rows = at_t(i * 4 + k)
                st = v[rows, cols] + pf[rows, cols] * start
                sig = 1.0 / (1.0 + jnp.exp(-st))
                act = st * sig
                if slope:
                    v[rows, cols] = (sig + act * (1.0 - sig)) * (H ** (-0.5))
                f0, f1 = fold(act * h0), fold(act * h1)
                qa0[rows, :] = f0 if fresh else qa0[rows, :] + f0
                qa1[rows, :] = f1 if fresh else qa1[rows, :] + f1
            return 0

        lax.fori_loop(0, T // 4, body, 0)

    def quality_send(slot):
        def body(i, acc):
            a0, a1 = acc
            for k in range(8):
                rows = at_t(i * 8 + k)
                here = lane8 == i * 8 + k
                a0 = jnp.where(here, jnp.sum(qa0[rows, :], axis=1, keepdims=True), a0)
                a1 = jnp.where(here, jnp.sum(qa1[rows, :], axis=1, keepdims=True), a1)
            return a0, a1

        zero = jnp.zeros((PAIR, 128), F32)
        a0, a1 = lax.fori_loop(0, T // 8, body, (zero, zero))
        q_s[slot, 0] = a0
        q_s[slot, 1] = a1
        send(q_s.at[slot], q_r.at[slot], d2d_ss.at[5 + slot], d2d_rs.at[5 + slot], partner)

    def quality_sum(slot):
        remote(
            q_s.at[slot], q_r.at[slot], d2d_ss.at[5 + slot], d2d_rs.at[5 + slot], partner
        ).wait_recv()
        return [(q_s[slot, k] + q_r[slot, k]) * (H ** (-0.5)) for k in range(2)]

    for m in range(2):
        w_half_in(m)
        for p in range(3):
            ag_one(m, p)
    for p in range(3):
        ag_one_in(0, p)
        ag_two(0, p)
        ag_three(0, p, 0)
    remote(pk_m, pk_i, d2d_ss.at[2], d2d_rs.at[2], partner).wait_recv()
    step8 = pk_m[0] + pk_i[0]
    rew8 = pk_m[1] + pk_i[1]
    logp8 = pk_m[2] + pk_i[2]
    rst8 = pk_m[3] + pk_i[3]
    keep8 = 1.0 - rst8
    hor8 = pk_m[4] + pk_i[4]
    burn8 = pk_m[5] + pk_i[5]

    sf[tm, 0] = jnp.broadcast_to(jnp.sum(step8, axis=1, keepdims=True), (PAIR, 128))
    sf[tm, 1] = jnp.broadcast_to(1.0 - jnp.max(rst8, axis=1, keepdims=True), (PAIR, 128))
    for d in range(1, TM):
        dev = {"tm": lax.rem(tm + d, TM), "batch": batch}
        remote(sf.at[tm], sf.at[tm], pre_ss.at[0], pre_rs.at[0], dev).start()

    spread_lanes(bc0, step8)
    spread_lanes(bc1, keep8)
    ld8 = jnp.broadcast_to(ld[:, mine], (PAIR, HALF))

    def factors(t, prod):
        e = jnp.exp(wide(bc0[at_t(t), :]) * ld8)
        f = e * wide(bc1[at_t(t), :])
        cc[at_t(t), :] = f
        ss[at_t(t), :] = jnp.sqrt(1.0 - e * e)
        prod = prod * f
        pf[at_t(t), :] = prod
        return prod

    lax.fori_loop(0, T, factors, jnp.ones((PAIR, HALF), F32))
    for p in range(3):
        ag_two_forward(0, p)
        ag_three(0, p, 3)
        ag_three(0, p, 1)
    for p in range(3):
        ag_one_in(1, p)
        ag_two(1, p)
    local[0].wait()
    remote(nxt, xr_n.at[other_half, :], d2d_ss.at[3], d2d_rs.at[3], partner).wait_recv()
    permute_next()
    for p in range(3):
        ag_three_forward(0, p, 0)
    for p in range(3):
        ag_two_last(0, p)
        ag_three(0, p, 2)
    for l in (3, 1):
        for p in range(3):
            ag_three_forward(0, p, l)
    for p in range(3):
        ag_two_forward(1, p)
        ag_three(1, p, 0)
    def tails(i, prod):
        t = T - 1 - i
        tp[at_t(t), :] = prod
        return prod * cc[at_t(t), :]

    lax.fori_loop(0, T, tails, jnp.ones((PAIR, HALF), F32))
    for p in range(3):
        ag_three_forward(0, p, 2)
        ag_three(1, p, 3)
        ag_three(1, p, 1)
    local[1].wait()
    remote(obs, xr_o.at[other_half, :], d2d_ss.at[4], d2d_rs.at[4], partner).wait_recv()
    permute_obs(0, 4)
    for p in range(3):
        ag_two_last(1, p)
        ag_three(1, p, 2)
    sums = remote(
        sf.at[pl.ds(0, TM - 1)], sf.at[pl.ds(0, TM - 1)], pre_ss.at[0], pre_rs.at[0], partner
    )
    sums.wait_recv()

    def block_decay(j, _):
        dall[j] = jnp.exp(wide(sf[j, 0]) * ld8) * wide(sf[j, 1])
        return 0

    lax.fori_loop(0, TM, block_decay, 0)
    for p in range(3):
        ag_three_forward(1, p, 0)
    for p in PARTS[:2]:
        ag_three_last(0, p)
        project(0, p, xp_n, vt)
        scan(vt, p, ends_t)
    for p in range(3):
        ag_three_forward(1, p, 3)
    for p in PARTS[2:]:
        ag_three_last(0, p)
        project(0, p, xp_n, vt)
        scan(vt, p, ends_t)
    prefix_send(1, ends_t, None, True)
    for p in range(3):
        ag_three_forward(1, p, 1)
    permute_obs(4, 8)
    for p in range(3):
        ag_three_forward(1, p, 2)
    prefix_take(1, ends_t, None, True)
    for p in PARTS:
        quality(vt, tgh, p, p == PARTS[0], False)
    quality_send(0)
    ag_three_last(1, PARTS[0])
    project(1, PARTS[0], xp_o, vo)
    scan(vo, PARTS[0], ends_o)
    prefix_send(2 + PARTS[0], ends_o, PARTS[0], True)
    tq = quality_sum(0)
    value8 = jnp.minimum(tq[0], tq[1]) - ENTROPY_COEFF * logp8
    nb_s[0] = rew8
    nb_s[1] = value8
    nb_s[2] = keep8
    before = {"tm": lax.rem(tm + TM - 1, TM), "batch": batch}
    send(nb_s, nb_r, nb_sem.at[0], nb_sem.at[1], before)
    ag_three_last(1, PARTS[1])
    project(1, PARTS[1], xp_o, vo)
    scan(vo, PARTS[1], ends_o)
    prefix_send(2 + PARTS[1], ends_o, PARTS[1], True)
    ag_three_last(1, PARTS[2])
    project(1, PARTS[2], xp_o, vo)
    scan(vo, PARTS[2], ends_o)
    prefix_send(2 + PARTS[2], ends_o, PARTS[2], True)
    prefix_take(2 + PARTS[0], ends_o, PARTS[0], True)
    quality(vo, onh, PARTS[0], True, True)

    remote(nb_s, nb_r, nb_sem.at[0], nb_sem.at[1], before).wait_recv()
    inside = (lane8 >= T) & (lane8 < T + NMAX) & (tm < TM - 1)

    def extended(own, slot):
        later = jnp.where(inside, pltpu.roll(nb_r[slot], T, 1), 0.0)
        return jnp.where(lane8 < T, own, later)

    ext_r, ext_v, ext_k = extended(rew8, 0), extended(value8, 1), extended(keep8, 2)

    def shifted(v, n):
        return v if n == 0 else pltpu.roll(v, 128 - n, 1)

    total = jnp.zeros((PAIR, 128), F32)
    alive = jnp.ones((PAIR, 128), F32)
    for n in range(NMAX):
        total = total + jnp.where(hor8 > n, DISCOUNT**n * alive * shifted(ext_r, n), 0.0)
        alive = alive * shifted(ext_k, n + 1)
        total = total + jnp.where(
            hor8 == n + 1, DISCOUNT ** (n + 1) * alive * shifted(ext_v, n + 1), 0.0
        )
    ret[...] = jnp.where(c == 0, total[:4, :T], total[4:, :T])
    weight = jnp.where((lane8 + tm * T).astype(F32) >= burn8, 1.0, 0.0)

    for p in PARTS[1:]:
        prefix_take(2 + p, ends_o, p, True)
        quality(vo, onh, p, False, True)
    quality_send(1)
    oq = quality_sum(1)
    spread_lanes(bc0, weight * (oq[0] - total))
    spread_lanes(bc1, weight * (oq[1] - total))

    for p in PARTS:
        cols, w = cols_of(p), WIDTHS[p]
        hcols = pl.ds(pl.multiple_of(c * HALF + OFFSETS[p], 128), w)
        h0 = jnp.broadcast_to(onh[0:1, hcols], (PAIR, w))
        h1 = jnp.broadcast_to(onh[1:2, hcols], (PAIR, w))

        def back(i, adj, cols=cols, w=w, h0=h0, h1=h1):
            for k in range(4):
                rows = at_t(T - 1 - (i * 4 + k))
                dh = wide(bc0[rows, :], w) * h0 + wide(bc1[rows, :], w) * h1
                adj = dh * vo[rows, cols] + adj
                vo[rows, cols] = adj
                adj = cc[rows, cols] * adj
            return adj

        leaving = lax.fori_loop(0, T // 4, back, jnp.zeros((PAIR, w), F32))
        lv[tm, :, cols] = leaving.astype(BF16)
        prefix_send(5 + p, lv, p, False)

    def finish(p):
        prefix_take(5 + p, lv, p, False)
        cols = cols_of(p)
        incoming = carry[:, cols]
        both = jnp.concatenate([incoming, incoming], axis=0)

        def body(i, _):
            for k in range(2):
                rows = pl.ds(pl.multiple_of(i * 32 + k * 16, 16), 16)
                adj = vo[rows, cols] + tp[rows, cols] * both
                du[rows, cols] = (ss[rows, cols] * adj).astype(BF16)
            return 0

        lax.fori_loop(0, ROWS // 32, body, 0)

    def gradient(p, l):
        where = place(p, FULL, turned(p, 1, l), FULL)
        lhs = xt[where].reshape(512, ROWS)
        v = jnp.dot(lhs, du[:, cols_of(p)], preferred_element_type=F32)
        gg[p][where] = v.reshape(4, 4, 32, WIDTHS[p])

    def rs_copy(p, k, j, src, dst, dev):
        return remote(src, dst, rs_ss.at[p * 3 + k], rs_rs.at[p * RS_SEMS + j], dev)

    def rs_half(p, s, h, dev):
        return rs_copy(p, 0, 2 * s + h, snd_h[p].at[s, h], rcv_h[p].at[s, h], dev)

    def rs_whole(p, s, h, dev):
        return rs_copy(p, 1, 10 + s, snd_w[p].at[s, h], rcv_w[p].at[s, h], dev)

    def rs_drain(p):
        for k, (src, dst) in enumerate(
            ((snd_h[p], rcv_h[p]), (snd_w[p], rcv_w[p]), (snd_b[p], rcv_b[p]))
        ):
            rs_copy(p, k, 0, src, dst, partner).wait_send()

    def rs_ref(p, s, d, h=None):
        if s < 4:
            return line(p, turned(p, 1, s), turned(p, 2, d), h)
        return line(p, turned(p, 1, d), turned(p, 2, 0), h)

    def rs_axis(s):
        return 2 if s < 4 else 1

    def rs_opposite(p, s):
        for h, d in ((0, 3), (1, 1)):
            snd_h[p][s, h] = gg[p][rs_ref(p, s, 2, h)].astype(BF16)
            rs_half(p, s, h, toward(p, rs_axis(s), d)).start()

    def rs_neighbour(p, s, h):
        d = (3, 1)[h]
        rs_half(p, s, h, partner).wait_recv()
        with_recv = gg[p][rs_ref(p, s, d, h)] + rcv_h[p][s, h].astype(F32)
        snd_w[p][s, h, pl.ds(2 * h, 2)] = with_recv.astype(BF16)
        snd_w[p][s, h, pl.ds(2 - 2 * h, 2)] = gg[p][rs_ref(p, s, d, 1 - h)].astype(BF16)
        rs_whole(p, s, h, toward(p, rs_axis(s), d)).start()

    def rs_sum(p, s):
        rs_copy(p, 1, 10 + s, snd_w[p].at[s], rcv_w[p].at[s], partner).wait_recv()
        own = rs_ref(p, s, 0)
        both = rcv_w[p][s, 0].astype(F32) + rcv_w[p][s, 1].astype(F32)
        gg[p][own] = gg[p][own] + both

    def rs_one(p):
        for d in (2, 1, 3):
            block = gg[p][place(p, turned(p, 0, d), turned(p, 1, 0), turned(p, 2, 0))]
            snd_b[p][d - 1] = block.astype(BF16)
            rs_copy(p, 2, 15, snd_b[p].at[d - 1], rcv_b[p].at[d - 1], toward(p, 0, d)).start()

    def rs_one_sum(p):
        rs_copy(p, 2, 15, snd_b[p], rcv_b[p], partner).wait_recv()
        v = gg[p][y, x, z]
        for d in range(3):
            v = v + rcv_b[p][d].astype(F32)
        gg[p][y, x, z] = v

    for p in PARTS:
        finish(p)
        gradient(p, LINES[0])
        rs_opposite(p, LINES[0])
    for p in PARTS:
        gradient(p, LINES[1])
        rs_opposite(p, LINES[1])
    for i in range(4):
        if i < 2:
            for p in PARTS:
                gradient(p, LINES[i + 2])
                rs_opposite(p, LINES[i + 2])
        for p in PARTS:
            rs_neighbour(p, LINES[i], 0)
            rs_neighbour(p, LINES[i], 1)
    for p in PARTS:
        rs_sum(p, LINES[0])
        rs_opposite(p, 4)
    for p in PARTS:
        rs_sum(p, LINES[1])
        rs_neighbour(p, 4, 0)
        rs_sum(p, LINES[2])
        rs_neighbour(p, 4, 1)
    for p in PARTS:
        rs_sum(p, LINES[3])
    for p in PARTS:
        rs_sum(p, 4)
        rs_one(p)
    for p in PARTS:
        rs_one_sum(p)

    for p in range(3):
        gx_s[:, cols_of(p)] = gg[p][y, x, z, other_rows, :]
    send(gx_s, gx_r, d2d_ss.at[7], d2d_rs.at[7], partner)
    for p in range(3):
        cols = pl.ds(pl.multiple_of(c * HALF + OFFSETS[p], 128), WIDTHS[p])
        gw[:, cols] = gg[p][y, x, z, own_rows, :]
    remote(gx_s, gx_r, d2d_ss.at[7], d2d_rs.at[7], partner).wait_recv()
    gw[:, theirs] = gx_r[...]

    prefix_drain(1, ends_t, None, True)
    for p in range(3):
        prefix_drain(2 + p, ends_o, p, True)
        prefix_drain(5 + p, lv, p, False)
    for p in range(3):
        ag_drain(0, p)
        ag_drain(1, p)
        rs_drain(p)
    remote(wst, wst, d2d_ss.at[0], d2d_rs.at[0], partner).wait_send()
    sums.wait_send()
    for copy in pending:
        copy.wait_send()


def shards(
    obs_feats, next_feats, online_w, target_w, log_decay, step_scale, online_heads, target_heads,
    reward, next_action_log_prob, resets, horizon, burn_in,
):
    vmem = pl.BlockSpec(memory_space=pltpu.VMEM)
    smem = pl.BlockSpec(memory_space=pltpu.SMEM)
    hbm = pl.BlockSpec(memory_space=pl.ANY)
    weights = [pltpu.VMEM((4, 4, 4, 32, w), BF16) for w in WIDTHS]
    staged = [
        *[pltpu.VMEM((5, 2, 2, 32, w), BF16) for w in WIDTHS],
        *[pltpu.VMEM((5, 2, 4, 32, w), BF16) for w in WIDTHS],
        *[pltpu.VMEM((3, 32, w), BF16) for w in WIDTHS],
    ]
    big = pltpu.VMEM((ROWS, HALF), F32)
    ends = pltpu.VMEM((TM, PAIR, HALF), BF16)
    narrow = pltpu.VMEM((ROWS, 128), F32)
    scratch = [
        pltpu.VMEM((ROWS, D), BF16), pltpu.VMEM((ROWS, D), BF16),
        pltpu.VMEM((ROWS, D), BF16), pltpu.VMEM((ROWS, D), BF16),
        pltpu.VMEM((4, 4, 4, 32, ROWS), BF16), pltpu.VMEM((2, 16, HALF), BF16),
        *weights, *weights,
        pltpu.VMEM((6, PAIR, 128), F32), pltpu.VMEM((6, PAIR, 128), F32),
        narrow, narrow, narrow, narrow,
        big, big, big, big, big, big,
        pltpu.VMEM((TM, 2, PAIR, 128), F32), pltpu.VMEM((TM, PAIR, HALF), F32), ends, ends, ends,
        pltpu.VMEM((PAIR, HALF), F32),
        pltpu.VMEM((2, 2, PAIR, 128), F32), pltpu.VMEM((2, 2, PAIR, 128), F32),
        pltpu.VMEM((3, PAIR, 128), F32), pltpu.VMEM((3, PAIR, 128), F32),
        pltpu.VMEM((ROWS, HALF), BF16),
        *[pltpu.VMEM((4, 4, 4, 32, w), F32) for w in WIDTHS],
        *staged, *staged,
        pltpu.VMEM((16, HALF), F32), pltpu.VMEM((16, HALF), F32),
        pltpu.SemaphoreType.DMA((18,)), pltpu.SemaphoreType.DMA((6 * AG_SEMS,)),
        pltpu.SemaphoreType.DMA((9,)), pltpu.SemaphoreType.DMA((3 * RS_SEMS,)),
        pltpu.SemaphoreType.DMA((8,)), pltpu.SemaphoreType.DMA((8,)),
        pltpu.SemaphoreType.DMA((2,)),
        pltpu.SemaphoreType.DMA((8,)), pltpu.SemaphoreType.DMA((8,)),
        pltpu.SemaphoreType.DMA((2,)),
    ]
    rows_b, span, width = obs_feats.shape
    grad, returns = pl.pallas_call(
        kernel,
        name="critic_step",
        out_shape=(
            jax.ShapeDtypeStruct(online_w.shape, F32),
            jax.ShapeDtypeStruct(reward.shape, F32),
        ),
        in_specs=[hbm, hbm] + [vmem] * 9 + [smem] * 2,
        out_specs=(vmem, vmem),
        scratch_shapes=scratch,
        compiler_params=pltpu.CompilerParams(
            collective_id=0, has_side_effects=True, vmem_limit_bytes=62 * 1024 * 1024
        ),
    )(
        obs_feats.reshape(rows_b * span, width), next_feats.reshape(rows_b * span, width),
        online_w, target_w, log_decay[None], step_scale, online_heads, target_heads,
        reward, next_action_log_prob, resets, horizon, burn_in,
    )
    grad_w = grad * SCALE
    new_target = (1.0 - POLYAK_RATE) * target_w + POLYAK_RATE * (online_w - STEP_SIZE * grad_w)
    return grad_w, new_target, returns


def solution(mesh):
    return jax.shard_map(
        shards,
        mesh=mesh,
        in_specs=(
            P("batch", "tm", None), P("batch", "tm", None),
            P(("tm", "batch"), None), P(("tm", "batch"), None),
            P(), P("batch", "tm"), P(), P(),
            P("batch", "tm"), P("batch", "tm"), P("batch", "tm"), P("batch"), P("batch"),
        ),
        out_specs=(P(("tm", "batch"), None), P(("tm", "batch"), None), P("batch", "tm")),
        check_vma=False,
    )
```

```python
import jax
import jax.numpy as jnp
from jax import lax
from jax.experimental import pallas as pl
from jax.experimental.pallas import tpu as pltpu
from jax.sharding import PartitionSpec as P

NMAX = 8
DISCOUNT = 0.99
ENTROPY_COEFF = 0.2
POLYAK_RATE = 0.005
STEP_SIZE = 0.1

F32 = jnp.float32
BF16 = jnp.bfloat16
MESH = pl.DeviceIdType.MESH

D = 2048
H = 2048
HALF = H // 2
T = 64
PAIR = 8
ROWS = T * PAIR
TM = 16
VMEM_LIMIT = 56
SCALE = D ** (-0.5)

WIDTHS_T = (384, 256, 384)
OFFSETS_T = (0, 384, 640)
WIDTHS = (256, 384, 384)
OFFSETS = (0, 256, 640)
ORDERS = (("z", "x", "y"), ("y", "z", "x"), ("x", "y", "z"))
PARTS = (0, 2, 1)
AG_SEMS = 13
RS_SEMS = 16
LINES = (2, 3, 1, 0)


def kernel(
    obs, nxt, onw_in, tgw_in, ld_in, step_in, onh_in, tgh_in, rew_in, logp_in, rst_in, hor, burn,
    gw, ret,
    onw, tgw, ld, step, onh, tgh, rew, logp, rst,
    xr_o, xr_n, xp_o, xp_n, xt, wst,
    wt0, wt1, wt2, wo0, wo1, wo2,
    pk_m, pk_i, bc0, bc1, qa0, qa1, cc, ss, pf, tp, vt, vo,
    sf, dfor, dback, ends_t, ends_o, lv, carry,
    q_s, q_r, nb_s, nb_r, du,
    g0, g1, g2,
    sh0, sh1, sh2, sw0, sw1, sw2, sb0, sb1, sb2,
    rh0, rh1, rh2, rw0, rw1, rw2, rb0, rb1, rb2,
    gx_s, gx_r,
    ag_ss, ag_rs, rs_ss, rs_rs, pre_ss, pre_rs, loc_sem, in_sem, d2d_ss, d2d_rs, nb_sem,
):
    tm = lax.axis_index("tm")
    batch = lax.axis_index("batch")
    y, x = tm // 4, tm % 4
    z, c = batch // 2, batch % 2
    at = {"y": y, "x": x, "z": z}
    other = 1 - c
    wb = ((wt0, wt1, wt2), (wo0, wo1, wo2))
    gg = (g0, g1, g2)
    snd_h, snd_w, snd_b = (sh0, sh1, sh2), (sw0, sw1, sw2), (sb0, sb1, sb2)
    rcv_h, rcv_w, rcv_b = (rh0, rh1, rh2), (rw0, rw1, rw2), (rb0, rb1, rb2)
    pending = []

    def device(**moved):
        here = {**at, **moved}
        return {"tm": here["y"] * 4 + here["x"], "batch": here["z"] * 2 + c}

    partner = {"tm": tm, "batch": z * 2 + other}

    def remote(src, dst, ss_, rs_, dev):
        return pltpu.make_async_remote_copy(
            src_ref=src, dst_ref=dst, send_sem=ss_, recv_sem=rs_, device_id=dev,
            device_id_type=MESH,
        )

    def send(src, dst, ss_, rs_, dev):
        copy = remote(src, dst, ss_, rs_, dev)
        copy.start()
        pending.append(copy)

    barrier = pltpu.get_barrier_semaphore()
    peers = [partner] + [device(z=lax.rem(z + d, 4)) for d in range(1, 4)]
    peers += [{"tm": lax.rem(tm + d, TM), "batch": batch} for d in range(1, TM)]
    for dev in peers:
        pl.semaphore_signal(barrier, inc=1, device_id=dev, device_id_type=MESH)

    own_half = pl.ds(pl.multiple_of(c * 256, 256), 256)
    other_half = pl.ds(pl.multiple_of(other * 256, 256), 256)
    loads = [
        pltpu.make_async_copy(src, dst, in_sem.at[i])
        for i, (src, dst) in enumerate((
            (tgw_in, tgw), (onw_in, onw), (step_in, step), (rew_in, rew), (logp_in, logp),
            (rst_in, rst), (ld_in, ld), (onh_in, onh), (tgh_in, tgh),
        ))
    ]
    local = [
        pltpu.make_async_copy(nxt, xr_n.at[own_half, :], loc_sem.at[0]),
        pltpu.make_async_copy(obs, xr_o.at[own_half, :], loc_sem.at[1]),
    ]
    for copy in loads + local:
        copy.start()
    for copy in loads:
        copy.wait()

    mine = pl.ds(pl.multiple_of(c * HALF, HALF), HALF)
    theirs = pl.ds(pl.multiple_of(other * HALF, HALF), HALF)
    own_rows = pl.ds(pl.multiple_of(c * 16, 16), 16)
    other_rows = pl.ds(pl.multiple_of(other * 16, 16), 16)
    for m, w in enumerate((tgw, onw)):
        wst[m] = w[:, theirs].astype(BF16)
        for p in range(3):
            off = (OFFSETS_T, OFFSETS)[m][p]
            cols = pl.ds(pl.multiple_of(c * HALF + off, 128), (WIDTHS_T, WIDTHS)[m][p])
            wb[m][p][y, x, z, own_rows, :] = w[:, cols].astype(BF16)

    row8 = lax.broadcasted_iota(jnp.int32, (PAIR, 128), 0)
    lane8 = lax.broadcasted_iota(jnp.int32, (PAIR, 128), 1)
    row_own = (row8[:, :T] // 4) == c

    def twice(v):
        return jnp.where(row_own, jnp.concatenate([v, v], axis=0), 0.0)

    pk_m[...] = jnp.zeros_like(pk_m)
    for slot, r in enumerate((step, rew, logp)):
        pk_m[slot, :, :T] = twice(r[...])
    pk_m[3, :, :T] = twice(rst[...].astype(F32))
    hz = jnp.zeros((PAIR, 128), F32)
    bz = jnp.zeros((PAIR, 128), F32)
    for i in range(4):
        sel = row8 == c * 4 + i
        hz = jnp.where(sel, hor[i].astype(F32), hz)
        bz = jnp.where(sel, burn[i].astype(F32), bz)
    pk_m[4] = hz
    pk_m[5] = bz

    pl.semaphore_wait(barrier, len(peers))

    def w_half(m, p):
        src, dst = wst.at[m, :, cols_of(p, m)], wb[m][p].at[y, x, z, own_rows, :]
        return remote(src, dst, d2d_ss.at[0], d2d_rs.at[m], partner)

    def w_half_in(m):
        remote(wst.at[m], wst.at[m], d2d_ss.at[0], d2d_rs.at[m], partner).wait_recv()

    def width(m, p):
        return (WIDTHS_T, WIDTHS)[m][p]

    def cols_of(p, m=1):
        return pl.ds((OFFSETS_T, OFFSETS)[m][p], width(m, p))

    for m in range(2):
        for p in range(3):
            w_half(m, p).start()
    send(pk_m, pk_i, d2d_ss.at[2], d2d_rs.at[2], partner)
    send(nxt, xr_n.at[own_half, :], d2d_ss.at[3], d2d_rs.at[3], partner)
    send(obs, xr_o.at[own_half, :], d2d_ss.at[4], d2d_rs.at[4], partner)

    def place(p, first, second, last):
        idx = dict(zip(ORDERS[p], (first, second, last)))
        return idx["y"], idx["x"], idx["z"]

    def turned(p, i, d):
        return lax.rem(at[ORDERS[p][i]] + d, 4)

    def toward(p, i, d):
        return device(**{ORDERS[p][i]: turned(p, i, d)})

    FULL = pl.ds(0, 4)

    def half_of(h):
        return FULL if h is None else pl.ds(2 * h, 2)

    def ag_copy(m, p, k, j, where, dev):
        ref = wb[m][p].at[where]
        n = m * 3 + p
        return remote(ref, ref, ag_ss.at[n * 3 + k], ag_rs.at[n * AG_SEMS + j], dev)

    def ag_end(m, p, l):
        return 12 + l if (m, p) == (1, 2) else 12

    def ag_send(m, p, k, j, where, dev):
        ag_copy(m, p, k, j, where, dev).start()

    def ag_wait(m, p, j, where):
        ag_copy(m, p, 0, j, where, partner).wait_recv()

    def ag_drain(m, p):
        for k, where in enumerate(((0, 0, pl.ds(0, 3)), (0, pl.ds(0, 3)), (pl.ds(0, 3),))):
            ag_copy(m, p, k, 0, where, partner).wait_send()

    def line(p, second, last, h=None):
        return place(p, half_of(h), second, last)

    def ag_one(m, p):
        for d in (2, 1, 3):
            ag_send(m, p, 0, 0, (y, x, z), toward(p, 0, d))

    def ag_one_in(m, p):
        ag_wait(m, p, 0, (0, 0, pl.ds(0, 3)))

    def ag_two(m, p):
        for d in (1, 3, 2):
            where = place(p, turned(p, 0, d), turned(p, 1, 0), turned(p, 2, 0))
            ag_send(m, p, 1, 1, where, toward(p, 1, 1))
            ag_send(m, p, 1, 2, where, toward(p, 1, 3))

    def ag_three_own(m, p):
        for d in (1, 3, 2):
            where = place(p, turned(p, 0, d), turned(p, 1, 0), turned(p, 2, 0))
            ag_send(m, p, 2, 4, where, toward(p, 2, 1))
            ag_send(m, p, 2, 5, where, toward(p, 2, 3))

    def ag_early(m, p):
        for k in (1, 2):
            ag_send(m, p, k, 3 * k - 2, (y, x, z), toward(p, k, 1))
            ag_send(m, p, k, 3 * k - 1, (y, x, z), toward(p, k, 3))

    def ag_two_forward(m, p):
        q3 = turned(p, 2, 0)
        ag_wait(m, p, 1, line(p, turned(p, 1, 3), q3))
        ag_send(m, p, 1, 3, line(p, turned(p, 1, 3), q3, 0), toward(p, 1, 1))
        ag_wait(m, p, 2, line(p, turned(p, 1, 1), q3))
        ag_send(m, p, 1, 3, line(p, turned(p, 1, 1), q3, 1), toward(p, 1, 3))

    def ag_two_last(m, p):
        ag_wait(m, p, 3, line(p, turned(p, 1, 2), turned(p, 2, 0)))

    def ag_three(m, p, l):
        own = line(p, turned(p, 1, l), turned(p, 2, 0))
        ag_send(m, p, 2, 4 + 2 * l, own, toward(p, 2, 1))
        ag_send(m, p, 2, 5 + 2 * l, own, toward(p, 2, 3))

    def ag_three_forward(m, p, l):
        second = turned(p, 1, l)
        ag_wait(m, p, 4 + 2 * l, line(p, second, turned(p, 2, 3)))
        ag_send(m, p, 2, ag_end(m, p, l), line(p, second, turned(p, 2, 3), 0), toward(p, 2, 1))
        ag_wait(m, p, 5 + 2 * l, line(p, second, turned(p, 2, 1)))
        ag_send(m, p, 2, ag_end(m, p, l), line(p, second, turned(p, 2, 1), 1), toward(p, 2, 3))

    def ag_three_last(m, p):
        ag_wait(m, p, 12, place(p, FULL, FULL, turned(p, 2, 2)))

    def ag_line_last(l):
        ag_wait(1, 2, 12 + l, line(2, turned(2, 1, l), turned(2, 2, 2)))

    def wide(v, w=HALF):
        return jnp.concatenate([v] * (w // 128), axis=1)

    def at_t(t):
        return pl.ds(pl.multiple_of(t * PAIR, PAIR), PAIR)

    def spread_lanes(dst, v):
        for t in range(T):
            dst[pl.ds(t * PAIR, PAIR), :] = jnp.broadcast_to(v[:, t : t + 1], (PAIR, 128))

    r_out = lax.broadcasted_iota(jnp.int32, (ROWS, ROWS), 0)
    r_in = lax.broadcasted_iota(jnp.int32, (ROWS, ROWS), 1)

    def permutation():
        return jnp.where(r_out == (r_in % T) * PAIR + r_in // T, 1.0, 0.0).astype(BF16)

    def permute_next():
        perm = permutation()

        def body(i, _):
            cols = pl.ds(pl.multiple_of(i * 256, 256), 256)
            xp_n[:, cols] = jnp.dot(perm, xr_n[:, cols], preferred_element_type=F32).astype(BF16)
            return 0

        lax.fori_loop(0, D // 256, body, 0)

    def permute_obs(lo, hi):
        perm = permutation()

        def body(i, _):
            cols = pl.ds(pl.multiple_of(i * 256, 256), 256)
            v = jnp.dot(perm, xr_o[:, cols], preferred_element_type=F32)
            xp_o[:, cols] = v.astype(BF16)
            xt[i // 2, pl.ds(2 * (i % 2), 2)] = v.T.astype(BF16).reshape(2, 4, 32, ROWS)
            return 0

        lax.fori_loop(lo, hi, body, 0)

    def project(m, p, xp, v):
        def tile(i, _):
            rows = pl.ds(pl.multiple_of(i * 256, 256), 256)
            w = wb[m][p][...].reshape(D, width(m, p))
            acc = jnp.dot(xp[rows, :], w, preferred_element_type=F32)
            v[rows, cols_of(p, m)] = acc * SCALE
            return 0

        lax.fori_loop(0, ROWS // 256, tile, 0)

    def project_planes(p, planes, fresh):
        axis = 1 if p == 2 else 2
        qs = [turned(p, axis, d) for d in planes]

        def tile(i, _):
            rows = pl.ds(pl.multiple_of(i * 256, 256), 256)
            acc = None if fresh else vo[rows, cols_of(p)]
            for q in qs:
                where = place(p, FULL, q, FULL) if p == 2 else place(p, FULL, FULL, q)
                w = wb[1][p][where].reshape(512, WIDTHS[p])
                if p == 1:
                    starts = [pl.multiple_of((k * 4 + q) * 128, 128) for k in range(4)]
                    lhs = jnp.concatenate([xp_o[rows, pl.ds(k, 128)] for k in starts], axis=1)
                else:
                    lhs = xp_o[rows, pl.ds(pl.multiple_of(q * 512, 512), 512)]
                v = jnp.dot(lhs, w, preferred_element_type=F32) * SCALE
                acc = v if acc is None else acc + v
            vo[rows, cols_of(p)] = acc
            return 0

        lax.fori_loop(0, ROWS // 256, tile, 0)

    def scan(m, v, p, ends):
        cols = cols_of(p, m)

        def body(i, st):
            for k in range(4):
                rows = at_t(i * 4 + k)
                st = cc[rows, cols] * st + ss[rows, cols] * v[rows, cols]
                v[rows, cols] = st
            return st

        last = lax.fori_loop(0, T // 4, body, jnp.zeros((PAIR, width(m, p)), F32))
        ends[tm, :, cols] = last

    def ends_copy(n, ends, p, slots, dev):
        cols = pl.ds(0, HALF) if p is None else cols_of(p)
        ref = ends.at[slots, :, cols]
        return remote(ref, ref, pre_ss.at[n], pre_rs.at[n], dev)

    def prefix_send(n, ends, p, forward):
        for d in range(TM - 1, 0, -1):
            to = tm + d if forward else tm - d

            @pl.when(to < TM if forward else to >= 0)
            def _(to=to):
                ends_copy(n, ends, p, tm, {"tm": to, "batch": batch}).start()

    def prefix_wait(n, ends, p, count, arrived):
        for k in range(1, TM):

            @pl.when(count == k)
            def _(k=k):
                copies = ends_copy(n, ends, p, pl.ds(0, k), partner)
                copies.wait_recv() if arrived else copies.wait_send()

    def prefix_take(n, ends, p, forward):
        cols, w = (pl.ds(0, HALF), HALF) if p is None else (cols_of(p), WIDTHS[p])
        prefix_wait(n, ends, p, tm if forward else TM - 1 - tm, True)
        decay = dfor if forward else dback
        v = jnp.zeros((PAIR, w), F32)
        for j in range(TM - 1) if forward else range(TM - 1, 0, -1):
            counted = jnp.where(j < tm if forward else j > tm, 1.0, 0.0)
            v = decay[j, :, cols] * v + counted * ends[j, :, cols].astype(F32)
        carry[:, cols] = v

    def prefix_drain(n, ends, p, forward):
        prefix_wait(n, ends, p, TM - 1 - tm if forward else tm, False)

    def quality(m, v, heads, p, fresh, slope):
        cols, w = cols_of(p, m), width(m, p)
        hcols = pl.ds(pl.multiple_of(c * HALF + (OFFSETS_T, OFFSETS)[m][p], 128), w)
        h0 = jnp.broadcast_to(heads[0:1, hcols], (PAIR, w))
        h1 = jnp.broadcast_to(heads[1:2, hcols], (PAIR, w))
        start = carry[:, cols]

        def fold(u):
            out = u[:, :128]
            for i in range(1, w // 128):
                out = out + u[:, i * 128 : (i + 1) * 128]
            return out

        def body(i, _):
            for k in range(8):
                rows = at_t(i * 8 + k)
                st = v[rows, cols] + pf[rows, cols] * start
                sig = 1.0 / (1.0 + jnp.exp(-st))
                act = st * sig
                if slope:
                    v[rows, cols] = sig + act * (1.0 - sig)
                f0, f1 = fold(act * h0), fold(act * h1)
                qa0[rows, :] = f0 if fresh else qa0[rows, :] + f0
                qa1[rows, :] = f1 if fresh else qa1[rows, :] + f1
            return 0

        lax.fori_loop(0, T // 8, body, 0)

    def quality_send(slot):
        def body(i, acc):
            a0, a1 = acc
            for k in range(16):
                rows = at_t(i * 16 + k)
                here = lane8 == i * 16 + k
                a0 = jnp.where(here, jnp.sum(qa0[rows, :], axis=1, keepdims=True), a0)
                a1 = jnp.where(here, jnp.sum(qa1[rows, :], axis=1, keepdims=True), a1)
            return a0, a1

        zero = jnp.zeros((PAIR, 128), F32)
        a0, a1 = lax.fori_loop(0, T // 16, body, (zero, zero))
        q_s[slot, 0] = a0
        q_s[slot, 1] = a1
        send(q_s.at[slot], q_r.at[slot], d2d_ss.at[5 + slot], d2d_rs.at[5 + slot], partner)

    def quality_sum(slot):
        remote(
            q_s.at[slot], q_r.at[slot], d2d_ss.at[5 + slot], d2d_rs.at[5 + slot], partner
        ).wait_recv()
        return [(q_s[slot, k] + q_r[slot, k]) * (H ** (-0.5)) for k in range(2)]

    for m in range(2):
        w_half_in(m)
        for p in range(3):
            ag_one(m, p)
        for p in range(3):
            ag_early(m, p)
    for p in range(3):
        ag_one_in(0, p)
        ag_two(0, p)
    for p in range(3):
        ag_three_own(0, p)
    def clear(j, _):
        @pl.when(j > tm)
        def _():
            ends_t[j] = jnp.zeros((PAIR, HALF), F32)
            ends_o[j] = jnp.zeros((PAIR, HALF), F32)

        @pl.when(j < tm)
        def _():
            lv[j] = jnp.zeros((PAIR, HALF), BF16)

        return 0

    lax.fori_loop(0, TM, clear, 0)
    remote(pk_m, pk_i, d2d_ss.at[2], d2d_rs.at[2], partner).wait_recv()
    step8 = pk_m[0] + pk_i[0]
    rew8 = pk_m[1] + pk_i[1]
    logp8 = pk_m[2] + pk_i[2]
    rst8 = pk_m[3] + pk_i[3]
    keep8 = 1.0 - rst8
    hor8 = pk_m[4] + pk_i[4]
    burn8 = pk_m[5] + pk_i[5]

    sf[tm, 0] = jnp.broadcast_to(jnp.sum(step8, axis=1, keepdims=True), (PAIR, 128))
    sf[tm, 1] = jnp.broadcast_to(1.0 - jnp.max(rst8, axis=1, keepdims=True), (PAIR, 128))
    for d in range(1, TM):
        dev = {"tm": lax.rem(tm + d, TM), "batch": batch}
        remote(sf.at[tm], sf.at[tm], pre_ss.at[0], pre_rs.at[0], dev).start()

    spread_lanes(bc0, step8)
    spread_lanes(bc1, keep8)
    ld8 = jnp.broadcast_to(ld[:, mine], (PAIR, HALF))

    def factors(t, prod):
        e = jnp.exp(wide(bc0[at_t(t), :]) * ld8)
        f = e * wide(bc1[at_t(t), :])
        cc[at_t(t), :] = f
        ss[at_t(t), :] = jnp.sqrt(1.0 - e * e)
        prod = prod * f
        pf[at_t(t), :] = prod
        return prod

    lax.fori_loop(0, T, factors, jnp.ones((PAIR, HALF), F32))
    for p in range(3):
        ag_one_in(1, p)
        ag_two(1, p)
    for p in range(3):
        ag_two_forward(0, p)
        ag_three(0, p, 3)
        ag_three(0, p, 1)
    local[0].wait()
    remote(nxt, xr_n.at[other_half, :], d2d_ss.at[3], d2d_rs.at[3], partner).wait_recv()
    permute_next()
    for p in range(3):
        ag_three_forward(0, p, 0)
    local[1].wait()
    remote(obs, xr_o.at[other_half, :], d2d_ss.at[4], d2d_rs.at[4], partner).wait_recv()
    permute_obs(0, 8)
    for p in range(3):
        ag_two_last(0, p)
        ag_three(0, p, 2)
    for l in (3, 1):
        for p in range(3):
            ag_three_forward(0, p, l)
    for p in range(3):
        ag_two_forward(1, p)
        ag_three_own(1, p)
    def tails(i, prod):
        t = T - 1 - i
        tp[at_t(t), :] = prod
        return prod * cc[at_t(t), :]

    lax.fori_loop(0, T, tails, jnp.ones((PAIR, HALF), F32))
    for p in range(3):
        ag_three_forward(0, p, 2)
        ag_three(1, p, 3)
        ag_three(1, p, 1)
    for p in range(3):
        ag_two_last(1, p)
        ag_three(1, p, 2)
    sums = remote(
        sf.at[pl.ds(0, TM - 1)], sf.at[pl.ds(0, TM - 1)], pre_ss.at[0], pre_rs.at[0], partner
    )
    sums.wait_recv()

    def block_decay(j, _):
        v = jnp.exp(wide(sf[j, 0]) * ld8) * wide(sf[j, 1])
        dfor[j] = jnp.where(j < tm, v, 1.0)
        dback[j] = jnp.where(j > tm, v, 1.0)
        return 0

    lax.fori_loop(0, TM, block_decay, 0)
    for p in range(3):
        ag_three_forward(1, p, 0)
    for p in PARTS[:2]:
        ag_three_last(0, p)
        project(0, p, xp_n, vt)
        scan(0, vt, p, ends_t)
    for p in range(3):
        ag_three_forward(1, p, 3)
    for p in PARTS[2:]:
        ag_three_last(0, p)
        project(0, p, xp_n, vt)
        scan(0, vt, p, ends_t)
    prefix_send(1, ends_t, None, True)
    for p in range(3):
        ag_three_forward(1, p, 1)
    for p in range(3):
        ag_three_forward(1, p, 2)
    for p in (0, 1):
        project_planes(p, (0, 1, 3), True)
    for l in (0, 3, 1):
        ag_line_last(l)
    project_planes(2, (0, 1, 3), True)
    ag_three_last(1, 0)
    project_planes(0, (2,), False)
    scan(1, vo, PARTS[0], ends_o)
    prefix_send(2 + PARTS[0], ends_o, PARTS[0], True)
    ag_line_last(2)
    project_planes(2, (2,), False)
    scan(1, vo, PARTS[1], ends_o)
    prefix_send(2 + PARTS[1], ends_o, PARTS[1], True)
    ag_three_last(1, 1)
    project_planes(1, (2,), False)
    scan(1, vo, PARTS[2], ends_o)
    prefix_send(2 + PARTS[2], ends_o, PARTS[2], True)
    prefix_take(1, ends_t, None, True)
    for p in PARTS:
        quality(0, vt, tgh, p, p == PARTS[0], False)
    quality_send(0)
    prefix_take(2 + PARTS[0], ends_o, PARTS[0], True)
    quality(1, vo, onh, PARTS[0], True, True)

    tq = quality_sum(0)
    value8 = jnp.minimum(tq[0], tq[1]) - ENTROPY_COEFF * logp8
    nb_s[0] = rew8
    nb_s[1] = value8
    nb_s[2] = keep8
    before = {"tm": lax.rem(tm + TM - 1, TM), "batch": batch}
    send(nb_s, nb_r, nb_sem.at[0], nb_sem.at[1], before)
    for p in PARTS[1:]:
        prefix_take(2 + p, ends_o, p, True)
        quality(1, vo, onh, p, False, True)
    quality_send(1)
    remote(nb_s, nb_r, nb_sem.at[0], nb_sem.at[1], before).wait_recv()
    inside = (lane8 >= T) & (lane8 < T + NMAX) & (tm < TM - 1)

    def extended(own, slot):
        later = jnp.where(inside, pltpu.roll(nb_r[slot], T, 1), 0.0)
        return jnp.where(lane8 < T, own, later)

    ext_r, ext_v, ext_k = extended(rew8, 0), extended(value8, 1), extended(keep8, 2)

    def shifted(v, n):
        return v if n == 0 else pltpu.roll(v, 128 - n, 1)

    total = jnp.zeros((PAIR, 128), F32)
    alive = jnp.ones((PAIR, 128), F32)
    for n in range(NMAX):
        total = total + jnp.where(hor8 > n, DISCOUNT**n * alive * shifted(ext_r, n), 0.0)
        alive = alive * shifted(ext_k, n + 1)
        total = total + jnp.where(
            hor8 == n + 1, DISCOUNT ** (n + 1) * alive * shifted(ext_v, n + 1), 0.0
        )
    ret[...] = jnp.where(c == 0, total[:4, :T], total[4:, :T])
    weight = jnp.where((lane8 + tm * T).astype(F32) >= burn8, 1.0, 0.0)

    oq = quality_sum(1)
    spread_lanes(bc0, weight * (oq[0] - total) * (H ** (-0.5)))
    spread_lanes(bc1, weight * (oq[1] - total) * (H ** (-0.5)))

    for p in PARTS:
        cols, w = cols_of(p), WIDTHS[p]
        hcols = pl.ds(pl.multiple_of(c * HALF + OFFSETS[p], 128), w)
        h0 = jnp.broadcast_to(onh[0:1, hcols], (PAIR, w))
        h1 = jnp.broadcast_to(onh[1:2, hcols], (PAIR, w))

        def back(i, adj, cols=cols, w=w, h0=h0, h1=h1):
            for k in range(4):
                rows = at_t(T - 1 - (i * 4 + k))
                dh = wide(bc0[rows, :], w) * h0 + wide(bc1[rows, :], w) * h1
                adj = dh * vo[rows, cols] + adj
                vo[rows, cols] = adj
                adj = cc[rows, cols] * adj
            return adj

        leaving = lax.fori_loop(0, T // 4, back, jnp.zeros((PAIR, w), F32))
        lv[tm, :, cols] = leaving.astype(BF16)
        prefix_send(5 + p, lv, p, False)

    def finish(p):
        prefix_take(5 + p, lv, p, False)
        cols = cols_of(p)
        incoming = carry[:, cols]
        both = jnp.concatenate([incoming, incoming], axis=0)

        def body(i, _):
            for k in range(2):
                rows = pl.ds(pl.multiple_of(i * 32 + k * 16, 16), 16)
                adj = vo[rows, cols] + tp[rows, cols] * both
                du[rows, cols] = (ss[rows, cols] * adj).astype(BF16)
            return 0

        lax.fori_loop(0, ROWS // 32, body, 0)

    def gradient(p, l):
        where = place(p, FULL, turned(p, 1, l), FULL)
        lhs = xt[where].reshape(512, ROWS)
        v = jnp.dot(lhs, du[:, cols_of(p)], preferred_element_type=F32)
        gg[p][where] = v.reshape(4, 4, 32, WIDTHS[p])

    def rs_copy(p, k, j, src, dst, dev):
        return remote(src, dst, rs_ss.at[p * 3 + k], rs_rs.at[p * RS_SEMS + j], dev)

    def rs_half(p, s, h, dev):
        return rs_copy(p, 0, 2 * s + h, snd_h[p].at[s, h], rcv_h[p].at[s, h], dev)

    def rs_whole(p, s, h, dev):
        return rs_copy(p, 1, 10 + s, snd_w[p].at[s, h], rcv_w[p].at[s, h], dev)

    def rs_drain(p):
        for k, (src, dst) in enumerate(
            ((snd_h[p], rcv_h[p]), (snd_w[p], rcv_w[p]), (snd_b[p], rcv_b[p]))
        ):
            rs_copy(p, k, 0, src, dst, partner).wait_send()

    def rs_ref(p, s, d, h=None):
        if s < 4:
            return line(p, turned(p, 1, s), turned(p, 2, d), h)
        return line(p, turned(p, 1, d), turned(p, 2, 0), h)

    def rs_axis(s):
        return 2 if s < 4 else 1

    def rs_opposite(p, s):
        for h, d in ((0, 3), (1, 1)):
            snd_h[p][s, h] = gg[p][rs_ref(p, s, 2, h)].astype(BF16)
            rs_half(p, s, h, toward(p, rs_axis(s), d)).start()

    def rs_neighbour(p, s, h):
        d = (3, 1)[h]
        rs_half(p, s, h, partner).wait_recv()
        with_recv = gg[p][rs_ref(p, s, d, h)] + rcv_h[p][s, h].astype(F32)
        snd_w[p][s, h, pl.ds(2 * h, 2)] = with_recv.astype(BF16)
        snd_w[p][s, h, pl.ds(2 - 2 * h, 2)] = gg[p][rs_ref(p, s, d, 1 - h)].astype(BF16)
        rs_whole(p, s, h, toward(p, rs_axis(s), d)).start()

    def rs_sum(p, s):
        rs_copy(p, 1, 10 + s, snd_w[p].at[s], rcv_w[p].at[s], partner).wait_recv()
        own = rs_ref(p, s, 0)
        both = rcv_w[p][s, 0].astype(F32) + rcv_w[p][s, 1].astype(F32)
        gg[p][own] = gg[p][own] + both

    def rs_one(p):
        for d in (2, 1, 3):
            block = gg[p][place(p, turned(p, 0, d), turned(p, 1, 0), turned(p, 2, 0))]
            snd_b[p][d - 1] = block.astype(BF16)
            rs_copy(p, 2, 15, snd_b[p].at[d - 1], rcv_b[p].at[d - 1], toward(p, 0, d)).start()

    def rs_one_sum(p):
        rs_copy(p, 2, 15, snd_b[p], rcv_b[p], partner).wait_recv()
        v = gg[p][y, x, z]
        for d in range(3):
            v = v + rcv_b[p][d].astype(F32)
        gg[p][y, x, z] = v

    for p in PARTS:
        finish(p)
        gradient(p, LINES[0])
        rs_opposite(p, LINES[0])
    for p in PARTS:
        gradient(p, LINES[1])
        rs_opposite(p, LINES[1])
    for p in PARTS:
        rs_neighbour(p, LINES[0], 0)
        rs_neighbour(p, LINES[0], 1)
        gradient(p, LINES[2])
        rs_opposite(p, LINES[2])
    for p in PARTS:
        rs_neighbour(p, LINES[1], 0)
        rs_neighbour(p, LINES[1], 1)
        gradient(p, LINES[3])
        rs_opposite(p, LINES[3])
    for p in PARTS:
        rs_sum(p, LINES[0])
        rs_opposite(p, 4)
    for p in PARTS:
        rs_neighbour(p, LINES[2], 0)
        rs_neighbour(p, LINES[2], 1)
    for p in PARTS:
        rs_sum(p, LINES[1])
        rs_neighbour(p, 4, 0)
    for p in PARTS:
        rs_neighbour(p, LINES[3], 0)
        rs_neighbour(p, LINES[3], 1)
    for p in PARTS:
        rs_sum(p, LINES[2])
        rs_neighbour(p, 4, 1)
    for p in PARTS:
        rs_sum(p, LINES[3])
    for p in PARTS:
        rs_sum(p, 4)
        rs_one(p)
    for p in PARTS:
        rs_one_sum(p)

    for p in range(3):
        gx_s[:, cols_of(p)] = gg[p][y, x, z, other_rows, :]
    send(gx_s, gx_r, d2d_ss.at[7], d2d_rs.at[7], partner)
    for p in range(3):
        cols = pl.ds(pl.multiple_of(c * HALF + OFFSETS[p], 128), WIDTHS[p])
        gw[:, cols] = gg[p][y, x, z, own_rows, :]
    remote(gx_s, gx_r, d2d_ss.at[7], d2d_rs.at[7], partner).wait_recv()
    gw[:, theirs] = gx_r[...]

    prefix_drain(1, ends_t, None, True)
    for p in range(3):
        prefix_drain(2 + p, ends_o, p, True)
        prefix_drain(5 + p, lv, p, False)
    for p in range(3):
        ag_drain(0, p)
        ag_drain(1, p)
        rs_drain(p)
    remote(wst, wst, d2d_ss.at[0], d2d_rs.at[0], partner).wait_send()
    sums.wait_send()
    for copy in pending:
        copy.wait_send()


def update(grad, returns, onw, tgw, grad_w, new_target, returns_out):
    g = grad[...] * SCALE
    grad_w[...] = g
    new_target[...] = (1.0 - POLYAK_RATE) * tgw[...] + POLYAK_RATE * (onw[...] - STEP_SIZE * g)
    returns_out[...] = returns[...]


def shards(
    obs_feats, next_feats, online_w, target_w, log_decay, step_scale, online_heads, target_heads,
    reward, next_action_log_prob, resets, horizon, burn_in,
):
    vmem = pl.BlockSpec(memory_space=pltpu.VMEM)
    smem = pl.BlockSpec(memory_space=pltpu.SMEM)
    hbm = pl.BlockSpec(memory_space=pltpu.HBM)
    small = (
        online_w, target_w, log_decay[None], step_scale, online_heads, target_heads,
        reward, next_action_log_prob, resets,
    )
    weights = [pltpu.VMEM((4, 4, 4, 32, w), BF16) for w in WIDTHS_T + WIDTHS]
    staged = [
        *[pltpu.VMEM((5, 2, 2, 32, w), BF16) for w in WIDTHS],
        *[pltpu.VMEM((5, 2, 4, 32, w), BF16) for w in WIDTHS],
        *[pltpu.VMEM((3, 32, w), BF16) for w in WIDTHS],
    ]
    big = pltpu.VMEM((ROWS, HALF), F32)
    ends = pltpu.VMEM((TM, PAIR, HALF), F32)
    narrow = pltpu.VMEM((ROWS, 128), F32)
    scratch = [
        *[pltpu.VMEM(a.shape, a.dtype) for a in small],
        pltpu.VMEM((ROWS, D), BF16), pltpu.VMEM((ROWS, D), BF16),
        pltpu.VMEM((ROWS, D), BF16), pltpu.VMEM((ROWS, D), BF16),
        pltpu.VMEM((4, 4, 4, 32, ROWS), BF16), pltpu.VMEM((2, 16, HALF), BF16),
        *weights,
        pltpu.VMEM((6, PAIR, 128), F32), pltpu.VMEM((6, PAIR, 128), F32),
        narrow, narrow, narrow, narrow,
        big, big, big, big, big, big,
        pltpu.VMEM((TM, 2, PAIR, 128), F32), ends, ends, ends, ends, pltpu.VMEM((TM, PAIR, HALF), BF16),
        pltpu.VMEM((PAIR, HALF), F32),
        pltpu.VMEM((2, 2, PAIR, 128), F32), pltpu.VMEM((2, 2, PAIR, 128), F32),
        pltpu.VMEM((3, PAIR, 128), F32), pltpu.VMEM((3, PAIR, 128), F32),
        pltpu.VMEM((ROWS, HALF), BF16),
        *[pltpu.VMEM((4, 4, 4, 32, w), F32) for w in WIDTHS],
        *staged, *staged,
        pltpu.VMEM((16, HALF), F32), pltpu.VMEM((16, HALF), F32),
        pltpu.SemaphoreType.DMA((18,)), pltpu.SemaphoreType.DMA((6 * AG_SEMS + 3,)),
        pltpu.SemaphoreType.DMA((9,)), pltpu.SemaphoreType.DMA((3 * RS_SEMS,)),
        pltpu.SemaphoreType.DMA((8,)), pltpu.SemaphoreType.DMA((8,)),
        pltpu.SemaphoreType.DMA((2,)), pltpu.SemaphoreType.DMA((9,)),
        pltpu.SemaphoreType.DMA((8,)), pltpu.SemaphoreType.DMA((8,)),
        pltpu.SemaphoreType.DMA((2,)),
    ]
    rows_b, span, width = obs_feats.shape
    grad, returns = pl.pallas_call(
        kernel,
        name="critic_step",
        out_shape=(
            jax.ShapeDtypeStruct(online_w.shape, F32),
            jax.ShapeDtypeStruct(reward.shape, F32),
        ),
        in_specs=[hbm] * 11 + [smem] * 2,
        out_specs=(vmem, vmem),
        scratch_shapes=scratch,
        compiler_params=pltpu.CompilerParams(
            collective_id=0, has_side_effects=True, vmem_limit_bytes=VMEM_LIMIT * 1024 * 1024
        ),
    )(
        obs_feats.reshape(rows_b * span, width), next_feats.reshape(rows_b * span, width),
        *small, horizon, burn_in,
    )
    return pl.pallas_call(
        update,
        name="target_update",
        out_shape=(
            jax.ShapeDtypeStruct(online_w.shape, F32),
            jax.ShapeDtypeStruct(target_w.shape, F32),
            jax.ShapeDtypeStruct(reward.shape, F32),
        ),
        in_specs=[vmem] * 4,
        out_specs=(vmem, vmem, vmem),
    )(grad, returns, online_w, target_w)


def solution(mesh):
    return jax.shard_map(
        shards,
        mesh=mesh,
        in_specs=(
            P("batch", "tm", None), P("batch", "tm", None),
            P(("tm", "batch"), None), P(("tm", "batch"), None),
            P(), P("batch", "tm"), P(), P(),
            P("batch", "tm"), P("batch", "tm"), P("batch", "tm"), P("batch"), P("batch"),
        ),
        out_specs=(P(("tm", "batch"), None), P(("tm", "batch"), None), P("batch", "tm")),
        check_vma=False,
    )
```

```python
import jax
import jax.numpy as jnp
from jax import lax
from jax.experimental import pallas as pl
from jax.experimental.pallas import tpu as pltpu
from jax.sharding import PartitionSpec as P

NMAX = 8
DISCOUNT = 0.99
ENTROPY_COEFF = 0.2
POLYAK_RATE = 0.005
STEP_SIZE = 0.1

F32 = jnp.float32
BF16 = jnp.bfloat16
MESH = pl.DeviceIdType.MESH

D = 2048
H = 2048
HALF = H // 2
T = 64
PAIR = 8
ROWS = T * PAIR
TM = 16
VMEM_LIMIT = 56
SCALE = D ** (-0.5)

WIDTHS_T = (384, 256, 384)
OFFSETS_T = (0, 384, 640)
WIDTHS = (256, 384, 384)
OFFSETS = (0, 256, 640)
ORDERS = (("z", "x", "y"), ("y", "z", "x"), ("x", "y", "z"))
PARTS = (0, 2, 1)
AG_SEMS = 8
RS_SEMS = 11
LINES = (2, 3, 1, 0)


def kernel(
    obs, nxt, onw_in, tgw_in, ld_in, step_in, onh_in, tgh_in, rew_in, logp_in, rst_in, hor, burn,
    gw, ret,
    onw, tgw, ld, step, onh, tgh, rew, logp, rst,
    xr_o, xr_n, xp_o, xp_n, xt, wst,
    wt0, wt1, wt2, wo0, wo1, wo2,
    pk_m, pk_i, bc0, bc1, qa0, qa1, cc, ss, pf, tp, vt, vo,
    sf, dfor, dback, ends_t, ends_o, lv, carry,
    q_s, q_r, nb_s, nb_r, du,
    g0, g1, g2,
    sh0, sh1, sh2, sw0, sw1, sw2, sb0, sb1, sb2,
    rh0, rh1, rh2, rw0, rw1, rw2, rb0, rb1, rb2,
    gx_s, gx_r,
    ag_ss, ag_rs, rs_ss, rs_rs, pre_ss, pre_rs, loc_sem, in_sem, d2d_ss, d2d_rs, nb_sem,
):
    tm = lax.axis_index("tm")
    batch = lax.axis_index("batch")
    y, x = tm // 4, tm % 4
    z, c = batch // 2, batch % 2
    at = {"y": y, "x": x, "z": z}
    other = 1 - c
    wb = ((wt0, wt1, wt2), (wo0, wo1, wo2))
    gg = (g0, g1, g2)
    snd_h, snd_w, snd_b = (sh0, sh1, sh2), (sw0, sw1, sw2), (sb0, sb1, sb2)
    rcv_h, rcv_w, rcv_b = (rh0, rh1, rh2), (rw0, rw1, rw2), (rb0, rb1, rb2)
    pending = []

    def device(core=c, **moved):
        here = {**at, **moved}
        return {"tm": here["y"] * 4 + here["x"], "batch": here["z"] * 2 + core}

    partner = {"tm": tm, "batch": z * 2 + other}

    def remote(src, dst, ss_, rs_, dev):
        return pltpu.make_async_remote_copy(
            src_ref=src, dst_ref=dst, send_sem=ss_, recv_sem=rs_, device_id=dev,
            device_id_type=MESH,
        )

    def send(src, dst, ss_, rs_, dev):
        copy = remote(src, dst, ss_, rs_, dev)
        copy.start()
        pending.append(copy)

    barrier = pltpu.get_barrier_semaphore()
    peers = [partner] + [device(z=lax.rem(z + d, 4)) for d in range(1, 4)]
    for a in "yxz":
        peers += [device(core=other, **{a: lax.rem(at[a] + d, 4)}) for d in range(1, 4)]
    peers += [{"tm": lax.rem(tm + d, TM), "batch": batch} for d in range(1, TM)]
    for dev in peers:
        pl.semaphore_signal(barrier, inc=1, device_id=dev, device_id_type=MESH)

    own_half = pl.ds(pl.multiple_of(c * 256, 256), 256)
    other_half = pl.ds(pl.multiple_of(other * 256, 256), 256)
    loads = [
        pltpu.make_async_copy(src, dst, in_sem.at[i])
        for i, (src, dst) in enumerate((
            (tgw_in, tgw), (onw_in, onw), (step_in, step), (rew_in, rew), (logp_in, logp),
            (rst_in, rst), (ld_in, ld), (onh_in, onh), (tgh_in, tgh),
        ))
    ]
    local = [
        pltpu.make_async_copy(nxt, xr_n.at[own_half, :], loc_sem.at[0]),
        pltpu.make_async_copy(obs, xr_o.at[own_half, :], loc_sem.at[1]),
    ]
    for copy in loads + local:
        copy.start()
    for copy in loads:
        copy.wait()

    mine = pl.ds(pl.multiple_of(c * HALF, HALF), HALF)
    theirs = pl.ds(pl.multiple_of(other * HALF, HALF), HALF)
    own_rows = pl.ds(pl.multiple_of(c * 16, 16), 16)
    other_rows = pl.ds(pl.multiple_of(other * 16, 16), 16)
    for m, w in enumerate((tgw, onw)):
        wst[m] = w[:, theirs].astype(BF16)
        for p in range(3):
            off = (OFFSETS_T, OFFSETS)[m][p]
            cols = pl.ds(pl.multiple_of(c * HALF + off, 128), (WIDTHS_T, WIDTHS)[m][p])
            wb[m][p][y, x, z, own_rows, :] = w[:, cols].astype(BF16)

    row8 = lax.broadcasted_iota(jnp.int32, (PAIR, 128), 0)
    lane8 = lax.broadcasted_iota(jnp.int32, (PAIR, 128), 1)
    row_own = (row8[:, :T] // 4) == c

    def twice(v):
        return jnp.where(row_own, jnp.concatenate([v, v], axis=0), 0.0)

    pk_m[...] = jnp.zeros_like(pk_m)
    for slot, r in enumerate((step, rew, logp)):
        pk_m[slot, :, :T] = twice(r[...])
    pk_m[3, :, :T] = twice(rst[...].astype(F32))
    hz = jnp.zeros((PAIR, 128), F32)
    bz = jnp.zeros((PAIR, 128), F32)
    for i in range(4):
        sel = row8 == c * 4 + i
        hz = jnp.where(sel, hor[i].astype(F32), hz)
        bz = jnp.where(sel, burn[i].astype(F32), bz)
    pk_m[4] = hz
    pk_m[5] = bz

    pl.semaphore_wait(barrier, len(peers))

    def w_half(m, p):
        src, dst = wst.at[m, :, cols_of(p, m)], wb[m][p].at[y, x, z, own_rows, :]
        return remote(src, dst, d2d_ss.at[0], d2d_rs.at[m], partner)

    def w_half_in(m):
        remote(wst.at[m], wst.at[m], d2d_ss.at[0], d2d_rs.at[m], partner).wait_recv()

    def width(m, p):
        return (WIDTHS_T, WIDTHS)[m][p]

    def cols_of(p, m=1):
        return pl.ds((OFFSETS_T, OFFSETS)[m][p], width(m, p))

    for m in range(2):
        for p in range(3):
            w_half(m, p).start()
    send(pk_m, pk_i, d2d_ss.at[2], d2d_rs.at[2], partner)
    send(nxt, xr_n.at[own_half, :], d2d_ss.at[3], d2d_rs.at[3], partner)
    send(obs, xr_o.at[own_half, :], d2d_ss.at[4], d2d_rs.at[4], partner)

    def place(p, first, second, last):
        idx = dict(zip(ORDERS[p], (first, second, last)))
        return idx["y"], idx["x"], idx["z"]

    def turned(p, i, d):
        return lax.rem(at[ORDERS[p][i]] + d, 4)

    def toward(p, i, d, core=c):
        return device(core=core, **{ORDERS[p][i]: turned(p, i, d)})

    FULL = pl.ds(0, 4)

    def half_of(h):
        return FULL if h is None else pl.ds(2 * h, 2)

    def ag_copy(m, p, k, j, where, dev):
        ref = wb[m][p].at[where]
        n = m * 3 + p
        return remote(ref, ref, ag_ss.at[n * 3 + k], ag_rs.at[n * AG_SEMS + j], dev)

    def ag_end(m, p, l):
        return 7 + l if (m, p) == (1, 2) else 7

    def ag_send(m, p, k, j, where, dev):
        ag_copy(m, p, k, j, where, dev).start()

    def ag_wait(m, p, j, where):
        ag_copy(m, p, 0, j, where, partner).wait_recv()

    def ag_drain(m, p):
        for k, where in enumerate(((0, 0, pl.ds(0, 3)), (0, pl.ds(0, 3)), (pl.ds(0, 3),))):
            ag_copy(m, p, k, 0, where, partner).wait_send()

    def line(p, second, last, h=None):
        return place(p, half_of(h), second, last)

    def ag_one(m, p):
        dst = wb[m][p].at[y, x, z, own_rows, :]
        sem, n = ag_ss.at[(m * 3 + p) * 3], (m * 3 + p) * AG_SEMS
        for d in (2, 1, 3):
            remote(dst, dst, sem, ag_rs.at[n], toward(p, 0, d)).start()
            src = wst.at[m, :, cols_of(p, m)]
            remote(src, dst, sem, ag_rs.at[n], toward(p, 0, d, other)).start()

    def ag_one_in(m, p):
        ag_wait(m, p, 0, (0, 0, pl.ds(0, 3)))

    def ag_own(m, p, k):
        for d in (1, 3, 2):
            where = place(p, turned(p, 0, d), turned(p, 1, 0), turned(p, 2, 0))
            ag_send(m, p, k, 2 * k - 1, where, toward(p, k, 1))
            ag_send(m, p, k, 2 * k - 1, where, toward(p, k, 3))

    def ag_early(m, p):
        for k in (1, 2):
            ag_send(m, p, k, 2 * k - 1, (y, x, z), toward(p, k, 1))
            ag_send(m, p, k, 2 * k - 1, (y, x, z), toward(p, k, 3))

    def ag_two_forward(m, p):
        q3 = turned(p, 2, 0)
        ag_wait(m, p, 1, (0, pl.ds(0, 2)))
        ag_send(m, p, 1, 2, line(p, turned(p, 1, 3), q3, 0), toward(p, 1, 1))
        ag_send(m, p, 1, 2, line(p, turned(p, 1, 1), q3, 1), toward(p, 1, 3))

    def ag_two_last(m, p):
        ag_wait(m, p, 2, line(p, turned(p, 1, 2), turned(p, 2, 0)))

    def ag_three(m, p, l):
        own = line(p, turned(p, 1, l), turned(p, 2, 0))
        ag_send(m, p, 2, 3 + l, own, toward(p, 2, 1))
        ag_send(m, p, 2, 3 + l, own, toward(p, 2, 3))

    def ag_three_forward(m, p, l):
        second = turned(p, 1, l)
        ag_wait(m, p, 3 + l, (0, pl.ds(0, 2)))
        end = ag_end(m, p, l)
        ag_send(m, p, 2, end, line(p, second, turned(p, 2, 3), 0), toward(p, 2, 1))
        ag_send(m, p, 2, end, line(p, second, turned(p, 2, 1), 1), toward(p, 2, 3))

    def ag_three_last(m, p):
        ag_wait(m, p, 7, place(p, FULL, FULL, turned(p, 2, 2)))

    def ag_line_last(l):
        ag_wait(1, 2, 7 + l, line(2, turned(2, 1, l), turned(2, 2, 2)))

    def wide(v, w=HALF):
        return jnp.concatenate([v] * (w // 128), axis=1)

    def at_t(t):
        return pl.ds(pl.multiple_of(t * PAIR, PAIR), PAIR)

    def spread_lanes(dst, v):
        for t in range(T):
            dst[pl.ds(t * PAIR, PAIR), :] = jnp.broadcast_to(v[:, t : t + 1], (PAIR, 128))

    r_out = lax.broadcasted_iota(jnp.int32, (ROWS, ROWS), 0)
    r_in = lax.broadcasted_iota(jnp.int32, (ROWS, ROWS), 1)

    def permutation():
        return jnp.where(r_out == (r_in % T) * PAIR + r_in // T, 1.0, 0.0).astype(BF16)

    def permute_next():
        perm = permutation()

        def body(i, _):
            cols = pl.ds(pl.multiple_of(i * 256, 256), 256)
            xp_n[:, cols] = jnp.dot(perm, xr_n[:, cols], preferred_element_type=F32).astype(BF16)
            return 0

        lax.fori_loop(0, D // 256, body, 0)

    def permute_obs(lo, hi):
        perm = permutation()

        def body(i, _):
            cols = pl.ds(pl.multiple_of(i * 256, 256), 256)
            v = jnp.dot(perm, xr_o[:, cols], preferred_element_type=F32)
            xp_o[:, cols] = v.astype(BF16)
            xt[i // 2, pl.ds(2 * (i % 2), 2)] = v.T.astype(BF16).reshape(2, 4, 32, ROWS)
            return 0

        lax.fori_loop(lo, hi, body, 0)

    def project(m, p, xp, v):
        def tile(i, _):
            rows = pl.ds(pl.multiple_of(i * 256, 256), 256)
            w = wb[m][p][...].reshape(D, width(m, p))
            acc = jnp.dot(xp[rows, :], w, preferred_element_type=F32)
            v[rows, cols_of(p, m)] = acc * SCALE
            return 0

        lax.fori_loop(0, ROWS // 256, tile, 0)

    def project_planes(p, planes, fresh):
        axis = 1 if p == 2 else 2
        qs = [turned(p, axis, d) for d in planes]

        def tile(i, _):
            rows = pl.ds(pl.multiple_of(i * 256, 256), 256)
            acc = None if fresh else vo[rows, cols_of(p)]
            for q in qs:
                where = place(p, FULL, q, FULL) if p == 2 else place(p, FULL, FULL, q)
                w = wb[1][p][where].reshape(512, WIDTHS[p])
                if p == 1:
                    starts = [pl.multiple_of((k * 4 + q) * 128, 128) for k in range(4)]
                    lhs = jnp.concatenate([xp_o[rows, pl.ds(k, 128)] for k in starts], axis=1)
                else:
                    lhs = xp_o[rows, pl.ds(pl.multiple_of(q * 512, 512), 512)]
                v = jnp.dot(lhs, w, preferred_element_type=F32) * SCALE
                acc = v if acc is None else acc + v
            vo[rows, cols_of(p)] = acc
            return 0

        lax.fori_loop(0, ROWS // 256, tile, 0)

    def scan(m, v, p, ends):
        cols = cols_of(p, m)

        def body(i, st):
            for k in range(4):
                rows = at_t(i * 4 + k)
                st = cc[rows, cols] * st + ss[rows, cols] * v[rows, cols]
                v[rows, cols] = st
            return st

        last = lax.fori_loop(0, T // 4, body, jnp.zeros((PAIR, width(m, p)), F32))
        ends[tm, :, cols] = last.astype(BF16)

    def ends_copy(n, ends, p, slots, dev):
        cols = pl.ds(0, HALF) if p is None else cols_of(p)
        ref = ends.at[slots, :, cols]
        return remote(ref, ref, pre_ss.at[n], pre_rs.at[n], dev)

    def prefix_send(n, ends, p, forward):
        for d in range(TM - 1, 0, -1):
            to = tm + d if forward else tm - d

            @pl.when(to < TM if forward else to >= 0)
            def _(to=to):
                ends_copy(n, ends, p, tm, {"tm": to, "batch": batch}).start()

    def prefix_wait(n, ends, p, count, arrived):
        for k in range(1, TM):

            @pl.when(count == k)
            def _(k=k):
                copies = ends_copy(n, ends, p, pl.ds(0, k), partner)
                copies.wait_recv() if arrived else copies.wait_send()

    def prefix_take(n, ends, p, forward):
        cols, w = (pl.ds(0, HALF), HALF) if p is None else (cols_of(p), WIDTHS[p])
        prefix_wait(n, ends, p, tm if forward else TM - 1 - tm, True)
        decay = dfor if forward else dback
        v = jnp.zeros((PAIR, w), F32)
        for j in range(TM - 1) if forward else range(TM - 1, 0, -1):
            counted = jnp.where(j < tm if forward else j > tm, 1.0, 0.0)
            v = decay[j, :, cols] * v + counted * ends[j, :, cols].astype(F32)
        carry[:, cols] = v

    def prefix_drain(n, ends, p, forward):
        prefix_wait(n, ends, p, TM - 1 - tm if forward else tm, False)

    def quality(m, v, heads, p, fresh, slope):
        cols, w = cols_of(p, m), width(m, p)
        hcols = pl.ds(pl.multiple_of(c * HALF + (OFFSETS_T, OFFSETS)[m][p], 128), w)
        h0 = jnp.broadcast_to(heads[0:1, hcols], (PAIR, w))
        h1 = jnp.broadcast_to(heads[1:2, hcols], (PAIR, w))
        start = carry[:, cols]

        def fold(u):
            out = u[:, :128]
            for i in range(1, w // 128):
                out = out + u[:, i * 128 : (i + 1) * 128]
            return out

        def body(i, _):
            for k in range(8):
                rows = at_t(i * 8 + k)
                st = v[rows, cols] + pf[rows, cols] * start
                sig = 1.0 / (1.0 + jnp.exp(-st))
                act = st * sig
                if slope:
                    v[rows, cols] = sig + act * (1.0 - sig)
                f0, f1 = fold(act * h0), fold(act * h1)
                qa0[rows, :] = f0 if fresh else qa0[rows, :] + f0
                qa1[rows, :] = f1 if fresh else qa1[rows, :] + f1
            return 0

        lax.fori_loop(0, T // 8, body, 0)

    def quality_send(slot):
        def body(i, acc):
            a0, a1 = acc
            for k in range(16):
                rows = at_t(i * 16 + k)
                here = lane8 == i * 16 + k
                a0 = jnp.where(here, jnp.sum(qa0[rows, :], axis=1, keepdims=True), a0)
                a1 = jnp.where(here, jnp.sum(qa1[rows, :], axis=1, keepdims=True), a1)
            return a0, a1

        zero = jnp.zeros((PAIR, 128), F32)
        a0, a1 = lax.fori_loop(0, T // 16, body, (zero, zero))
        q_s[slot, 0] = a0
        q_s[slot, 1] = a1
        send(q_s.at[slot], q_r.at[slot], d2d_ss.at[5 + slot], d2d_rs.at[5 + slot], partner)

    def quality_sum(slot):
        remote(
            q_s.at[slot], q_r.at[slot], d2d_ss.at[5 + slot], d2d_rs.at[5 + slot], partner
        ).wait_recv()
        return [(q_s[slot, k] + q_r[slot, k]) * (H ** (-0.5)) for k in range(2)]

    for m in range(2):
        for p in range(3):
            ag_one(m, p)
    for m in range(2):
        w_half_in(m)
        for p in range(3):
            ag_early(m, p)
    for p in range(3):
        ag_one_in(0, p)
        ag_own(0, p, 1)
    for p in range(3):
        ag_own(0, p, 2)
    def clear(j, _):
        @pl.when(j > tm)
        def _():
            ends_t[j] = jnp.zeros((PAIR, HALF), BF16)
            ends_o[j] = jnp.zeros((PAIR, HALF), BF16)

        @pl.when(j < tm)
        def _():
            lv[j] = jnp.zeros((PAIR, HALF), BF16)

        return 0

    lax.fori_loop(0, TM, clear, 0)
    remote(pk_m, pk_i, d2d_ss.at[2], d2d_rs.at[2], partner).wait_recv()
    step8 = pk_m[0] + pk_i[0]
    rew8 = pk_m[1] + pk_i[1]
    logp8 = pk_m[2] + pk_i[2]
    rst8 = pk_m[3] + pk_i[3]
    keep8 = 1.0 - rst8
    hor8 = pk_m[4] + pk_i[4]
    burn8 = pk_m[5] + pk_i[5]

    sf[tm, 0] = jnp.broadcast_to(jnp.sum(step8, axis=1, keepdims=True), (PAIR, 128))
    sf[tm, 1] = jnp.broadcast_to(1.0 - jnp.max(rst8, axis=1, keepdims=True), (PAIR, 128))
    for d in range(1, TM):
        dev = {"tm": lax.rem(tm + d, TM), "batch": batch}
        remote(sf.at[tm], sf.at[tm], pre_ss.at[0], pre_rs.at[0], dev).start()

    spread_lanes(bc0, step8)
    spread_lanes(bc1, keep8)
    ld8 = jnp.broadcast_to(ld[:, mine], (PAIR, HALF))

    def factors(t, prod):
        e = jnp.exp(wide(bc0[at_t(t), :]) * ld8)
        f = e * wide(bc1[at_t(t), :])
        cc[at_t(t), :] = f
        ss[at_t(t), :] = jnp.sqrt(1.0 - e * e)
        prod = prod * f
        pf[at_t(t), :] = prod
        return prod

    lax.fori_loop(0, T, factors, jnp.ones((PAIR, HALF), F32))
    for p in range(3):
        ag_one_in(1, p)
        ag_own(1, p, 1)
    for p in range(3):
        ag_two_forward(0, p)
        ag_three(0, p, 3)
        ag_three(0, p, 1)
    local[0].wait()
    remote(nxt, xr_n.at[other_half, :], d2d_ss.at[3], d2d_rs.at[3], partner).wait_recv()
    permute_next()
    for p in range(3):
        ag_three_forward(0, p, 0)
    local[1].wait()
    remote(obs, xr_o.at[other_half, :], d2d_ss.at[4], d2d_rs.at[4], partner).wait_recv()
    permute_obs(0, 8)
    for p in range(3):
        ag_two_last(0, p)
        ag_three(0, p, 2)
    for l in (3, 1):
        for p in range(3):
            ag_three_forward(0, p, l)
    for p in range(3):
        ag_two_forward(1, p)
        ag_own(1, p, 2)
    def tails(i, prod):
        t = T - 1 - i
        tp[at_t(t), :] = prod
        return prod * cc[at_t(t), :]

    lax.fori_loop(0, T, tails, jnp.ones((PAIR, HALF), F32))
    for p in range(3):
        ag_three_forward(0, p, 2)
        ag_three(1, p, 3)
        ag_three(1, p, 1)
    for p in range(3):
        ag_two_last(1, p)
        ag_three(1, p, 2)
    sums = remote(
        sf.at[pl.ds(0, TM - 1)], sf.at[pl.ds(0, TM - 1)], pre_ss.at[0], pre_rs.at[0], partner
    )
    sums.wait_recv()

    def block_decay(j, _):
        v = jnp.exp(wide(sf[j, 0]) * ld8) * wide(sf[j, 1])
        dfor[j] = jnp.where(j < tm, v, 1.0)
        dback[j] = jnp.where(j > tm, v, 1.0)
        return 0

    lax.fori_loop(0, TM, block_decay, 0)
    for p in range(3):
        ag_three_forward(1, p, 0)
    for p in PARTS[:2]:
        ag_three_last(0, p)
        project(0, p, xp_n, vt)
        scan(0, vt, p, ends_t)
    for p in range(3):
        ag_three_forward(1, p, 3)
    for p in PARTS[2:]:
        ag_three_last(0, p)
        project(0, p, xp_n, vt)
        scan(0, vt, p, ends_t)
    prefix_send(1, ends_t, None, True)
    for p in range(3):
        ag_three_forward(1, p, 1)
    for p in range(3):
        ag_three_forward(1, p, 2)
    for p in (0, 1):
        project_planes(p, (0, 1, 3), True)
    for l in (0, 3, 1):
        ag_line_last(l)
    project_planes(2, (0, 1, 3), True)
    ag_three_last(1, 0)
    project_planes(0, (2,), False)
    scan(1, vo, PARTS[0], ends_o)
    prefix_send(2 + PARTS[0], ends_o, PARTS[0], True)
    ag_line_last(2)
    project_planes(2, (2,), False)
    scan(1, vo, PARTS[1], ends_o)
    prefix_send(2 + PARTS[1], ends_o, PARTS[1], True)
    ag_three_last(1, 1)
    project_planes(1, (2,), False)
    scan(1, vo, PARTS[2], ends_o)
    prefix_send(2 + PARTS[2], ends_o, PARTS[2], True)
    prefix_take(1, ends_t, None, True)
    for p in PARTS:
        quality(0, vt, tgh, p, p == PARTS[0], False)
    quality_send(0)
    prefix_take(2 + PARTS[0], ends_o, PARTS[0], True)
    quality(1, vo, onh, PARTS[0], True, True)

    tq = quality_sum(0)
    value8 = jnp.minimum(tq[0], tq[1]) - ENTROPY_COEFF * logp8
    nb_s[0] = rew8
    nb_s[1] = value8
    nb_s[2] = keep8
    before = {"tm": lax.rem(tm + TM - 1, TM), "batch": batch}
    send(nb_s, nb_r, nb_sem.at[0], nb_sem.at[1], before)
    for p in PARTS[1:]:
        prefix_take(2 + p, ends_o, p, True)
        quality(1, vo, onh, p, False, True)
    quality_send(1)
    remote(nb_s, nb_r, nb_sem.at[0], nb_sem.at[1], before).wait_recv()
    inside = (lane8 >= T) & (lane8 < T + NMAX) & (tm < TM - 1)

    def extended(own, slot):
        later = jnp.where(inside, pltpu.roll(nb_r[slot], T, 1), 0.0)
        return jnp.where(lane8 < T, own, later)

    ext_r, ext_v, ext_k = extended(rew8, 0), extended(value8, 1), extended(keep8, 2)

    def shifted(v, n):
        return v if n == 0 else pltpu.roll(v, 128 - n, 1)

    total = jnp.zeros((PAIR, 128), F32)
    alive = jnp.ones((PAIR, 128), F32)
    for n in range(NMAX):
        total = total + jnp.where(hor8 > n, DISCOUNT**n * alive * shifted(ext_r, n), 0.0)
        alive = alive * shifted(ext_k, n + 1)
        total = total + jnp.where(
            hor8 == n + 1, DISCOUNT ** (n + 1) * alive * shifted(ext_v, n + 1), 0.0
        )
    ret[...] = jnp.where(c == 0, total[:4, :T], total[4:, :T])
    weight = jnp.where((lane8 + tm * T).astype(F32) >= burn8, 1.0, 0.0)

    oq = quality_sum(1)
    spread_lanes(bc0, weight * (oq[0] - total) * (H ** (-0.5)))
    spread_lanes(bc1, weight * (oq[1] - total) * (H ** (-0.5)))

    h0 = jnp.broadcast_to(onh[0:1, mine], (PAIR, HALF))
    h1 = jnp.broadcast_to(onh[1:2, mine], (PAIR, HALF))

    def back(i, adj):
        for k in range(4):
            rows = at_t(T - 1 - (i * 4 + k))
            dh = wide(bc0[rows, :]) * h0 + wide(bc1[rows, :]) * h1
            adj = dh * vo[rows, :] + adj
            vo[rows, :] = adj
            adj = cc[rows, :] * adj
        return adj

    leaving = lax.fori_loop(0, T // 4, back, jnp.zeros((PAIR, HALF), F32))
    lv[tm] = leaving.astype(BF16)
    prefix_send(5, lv, None, False)

    def finish(p):
        cols = cols_of(p)
        incoming = carry[:, cols]
        both = jnp.concatenate([incoming, incoming], axis=0)

        def body(i, _):
            for k in range(2):
                rows = pl.ds(pl.multiple_of(i * 32 + k * 16, 16), 16)
                adj = vo[rows, cols] + tp[rows, cols] * both
                du[rows, cols] = (ss[rows, cols] * adj).astype(BF16)
            return 0

        lax.fori_loop(0, ROWS // 32, body, 0)

    def gradient(p, l):
        where = place(p, FULL, turned(p, 1, l), FULL)
        lhs = xt[where].reshape(512, ROWS)
        v = jnp.dot(lhs, du[:, cols_of(p)], preferred_element_type=F32)
        gg[p][where] = v.reshape(4, 4, 32, WIDTHS[p])

    def rs_copy(p, k, j, src, dst, dev):
        return remote(src, dst, rs_ss.at[p * 3 + k], rs_rs.at[p * RS_SEMS + j], dev)

    def rs_half(p, s, h, dev):
        return rs_copy(p, 0, s, snd_h[p].at[s, h], rcv_h[p].at[s, h], dev)

    def rs_whole(p, s, h, dev):
        return rs_copy(p, 1, 5 + s, snd_w[p].at[s, h], rcv_w[p].at[s, h], dev)

    def rs_drain(p):
        for k, (src, dst) in enumerate(
            ((snd_h[p], rcv_h[p]), (snd_w[p], rcv_w[p]), (snd_b[p], rcv_b[p]))
        ):
            rs_copy(p, k, 0, src, dst, partner).wait_send()

    def rs_ref(p, s, d, h=None):
        if s < 4:
            return line(p, turned(p, 1, s), turned(p, 2, d), h)
        return line(p, turned(p, 1, d), turned(p, 2, 0), h)

    def rs_axis(s):
        return 2 if s < 4 else 1

    def rs_opposite(p, s):
        for h, d in ((0, 3), (1, 1)):
            snd_h[p][s, h] = gg[p][rs_ref(p, s, 2, h)].astype(BF16)
            rs_half(p, s, h, toward(p, rs_axis(s), d)).start()

    def rs_arrived(p, s):
        rs_copy(p, 0, s, snd_h[p].at[s], rcv_h[p].at[s], partner).wait_recv()

    def rs_neighbour(p, s, h):
        d = (3, 1)[h]
        with_recv = gg[p][rs_ref(p, s, d, h)] + rcv_h[p][s, h].astype(F32)
        snd_w[p][s, h, pl.ds(2 * h, 2)] = with_recv.astype(BF16)
        snd_w[p][s, h, pl.ds(2 - 2 * h, 2)] = gg[p][rs_ref(p, s, d, 1 - h)].astype(BF16)
        rs_whole(p, s, h, toward(p, rs_axis(s), d)).start()

    def rs_neighbours(p, s):
        rs_arrived(p, s)
        rs_neighbour(p, s, 0)
        rs_neighbour(p, s, 1)

    def rs_sum(p, s):
        rs_copy(p, 1, 5 + s, snd_w[p].at[s], rcv_w[p].at[s], partner).wait_recv()
        own = rs_ref(p, s, 0)
        both = rcv_w[p][s, 0].astype(F32) + rcv_w[p][s, 1].astype(F32)
        gg[p][own] = gg[p][own] + both

    def rs_one(p):
        for d in (2, 1, 3):
            where = place(p, turned(p, 0, d), turned(p, 1, 0), turned(p, 2, 0))
            for core in range(2):
                block = gg[p][(*where, pl.ds(16 * core, 16))]
                snd_b[p][core, d - 1] = block.astype(BF16)
                rs_copy(
                    p, 2, 10, snd_b[p].at[core, d - 1], rcv_b[p].at[c, d - 1],
                    toward(p, 0, d, core),
                ).start()
        gx_s[:, cols_of(p)] = gg[p][y, x, z, other_rows, :]

    prefix_take(5, lv, None, False)
    for p in PARTS:
        finish(p)
        gradient(p, LINES[0])
        rs_opposite(p, LINES[0])
    for p in PARTS:
        gradient(p, LINES[1])
        rs_opposite(p, LINES[1])
    for p in PARTS:
        rs_neighbours(p, LINES[0])
        gradient(p, LINES[2])
        rs_opposite(p, LINES[2])
    for p in PARTS:
        rs_neighbours(p, LINES[1])
        gradient(p, LINES[3])
        rs_opposite(p, LINES[3])
    for p in PARTS:
        rs_sum(p, LINES[0])
        rs_opposite(p, 4)
    for p in PARTS:
        rs_neighbours(p, LINES[2])
    for p in PARTS:
        rs_sum(p, LINES[1])
        rs_arrived(p, 4)
        rs_neighbour(p, 4, 0)
    for p in PARTS:
        rs_neighbours(p, LINES[3])
    for p in PARTS:
        rs_sum(p, LINES[2])
        rs_neighbour(p, 4, 1)
    prefix_drain(1, ends_t, None, True)
    for p in range(3):
        prefix_drain(2 + p, ends_o, p, True)
        ag_drain(0, p)
        ag_drain(1, p)
    prefix_drain(5, lv, None, False)
    remote(wst, wst, d2d_ss.at[0], d2d_rs.at[0], partner).wait_send()
    sums.wait_send()
    for copy in pending:
        copy.wait_send()
    pending.clear()
    for p in PARTS:
        rs_sum(p, LINES[3])
    for p in PARTS:
        rs_sum(p, 4)
        rs_one(p)
    send(gx_s, gx_r, d2d_ss.at[7], d2d_rs.at[7], partner)
    remote(gx_s, gx_r, d2d_ss.at[7], d2d_rs.at[7], partner).wait_recv()
    for p in range(3):
        rs_copy(p, 2, 10, snd_b[p], rcv_b[p], partner).wait_recv()
        for core, v in (
            (c, gg[p][y, x, z, own_rows, :]), (other, gx_r[:, cols_of(p)]),
        ):
            for d in range(3):
                v = v + rcv_b[p][core, d].astype(F32)
            cols = pl.ds(pl.multiple_of(core * HALF + OFFSETS[p], 128), WIDTHS[p])
            gw[:, cols] = v

    for p in range(3):
        rs_drain(p)
    for copy in pending:
        copy.wait_send()


def update(grad, returns, onw, tgw, grad_w, new_target, returns_out):
    g = grad[...] * SCALE
    grad_w[...] = g
    new_target[...] = (1.0 - POLYAK_RATE) * tgw[...] + POLYAK_RATE * (onw[...] - STEP_SIZE * g)
    returns_out[...] = returns[...]


def shards(
    obs_feats, next_feats, online_w, target_w, log_decay, step_scale, online_heads, target_heads,
    reward, next_action_log_prob, resets, horizon, burn_in,
):
    vmem = pl.BlockSpec(memory_space=pltpu.VMEM)
    smem = pl.BlockSpec(memory_space=pltpu.SMEM)
    hbm = pl.BlockSpec(memory_space=pltpu.HBM)
    small = (
        online_w, target_w, log_decay[None], step_scale, online_heads, target_heads,
        reward, next_action_log_prob, resets,
    )
    weights = [pltpu.VMEM((4, 4, 4, 32, w), BF16) for w in WIDTHS_T + WIDTHS]
    staged = [
        *[pltpu.VMEM((5, 2, 2, 32, w), BF16) for w in WIDTHS],
        *[pltpu.VMEM((5, 2, 4, 32, w), BF16) for w in WIDTHS],
        *[pltpu.VMEM((2, 3, 16, w), BF16) for w in WIDTHS],
    ]
    big = pltpu.VMEM((ROWS, HALF), F32)
    table = pltpu.VMEM((TM, PAIR, HALF), F32)
    ends = pltpu.VMEM((TM, PAIR, HALF), BF16)
    narrow = pltpu.VMEM((ROWS, 128), F32)
    scratch = [
        *[pltpu.VMEM(a.shape, a.dtype) for a in small],
        pltpu.VMEM((ROWS, D), BF16), pltpu.VMEM((ROWS, D), BF16),
        pltpu.VMEM((ROWS, D), BF16), pltpu.VMEM((ROWS, D), BF16),
        pltpu.VMEM((4, 4, 4, 32, ROWS), BF16), pltpu.VMEM((2, 16, HALF), BF16),
        *weights,
        pltpu.VMEM((6, PAIR, 128), F32), pltpu.VMEM((6, PAIR, 128), F32),
        narrow, narrow, narrow, narrow,
        big, big, big, big, big, big,
        pltpu.VMEM((TM, 2, PAIR, 128), F32), table, table, ends, ends, ends,
        pltpu.VMEM((PAIR, HALF), F32),
        pltpu.VMEM((2, 2, PAIR, 128), F32), pltpu.VMEM((2, 2, PAIR, 128), F32),
        pltpu.VMEM((3, PAIR, 128), F32), pltpu.VMEM((3, PAIR, 128), F32),
        pltpu.VMEM((ROWS, HALF), BF16),
        *[pltpu.VMEM((4, 4, 4, 32, w), F32) for w in WIDTHS],
        *staged, *staged,
        pltpu.VMEM((16, HALF), F32), pltpu.VMEM((16, HALF), F32),
        pltpu.SemaphoreType.DMA((18,)), pltpu.SemaphoreType.DMA((6 * AG_SEMS + 3,)),
        pltpu.SemaphoreType.DMA((9,)), pltpu.SemaphoreType.DMA((3 * RS_SEMS,)),
        pltpu.SemaphoreType.DMA((6,)), pltpu.SemaphoreType.DMA((6,)),
        pltpu.SemaphoreType.DMA((2,)), pltpu.SemaphoreType.DMA((9,)),
        pltpu.SemaphoreType.DMA((8,)), pltpu.SemaphoreType.DMA((8,)),
        pltpu.SemaphoreType.DMA((2,)),
    ]
    rows_b, span, width = obs_feats.shape
    grad, returns = pl.pallas_call(
        kernel,
        name="critic_step",
        out_shape=(
            jax.ShapeDtypeStruct(online_w.shape, F32),
            jax.ShapeDtypeStruct(reward.shape, F32),
        ),
        in_specs=[hbm] * 11 + [smem] * 2,
        out_specs=(vmem, vmem),
        scratch_shapes=scratch,
        compiler_params=pltpu.CompilerParams(
            collective_id=0, has_side_effects=True, vmem_limit_bytes=VMEM_LIMIT * 1024 * 1024
        ),
    )(
        obs_feats.reshape(rows_b * span, width), next_feats.reshape(rows_b * span, width),
        *small, horizon, burn_in,
    )
    return pl.pallas_call(
        update,
        name="target_update",
        out_shape=(
            jax.ShapeDtypeStruct(online_w.shape, F32),
            jax.ShapeDtypeStruct(target_w.shape, F32),
            jax.ShapeDtypeStruct(reward.shape, F32),
        ),
        in_specs=[vmem] * 4,
        out_specs=(vmem, vmem, vmem),
    )(grad, returns, online_w, target_w)


def solution(mesh):
    return jax.shard_map(
        shards,
        mesh=mesh,
        in_specs=(
            P("batch", "tm", None), P("batch", "tm", None),
            P(("tm", "batch"), None), P(("tm", "batch"), None),
            P(), P("batch", "tm"), P(), P(),
            P("batch", "tm"), P("batch", "tm"), P("batch", "tm"), P("batch"), P("batch"),
        ),
        out_specs=(P(("tm", "batch"), None), P(("tm", "batch"), None), P("batch", "tm")),
        check_vma=False,
    )
```

```python
import jax
import jax.numpy as jnp
from jax import lax
from jax.experimental import pallas as pl
from jax.experimental.pallas import tpu as pltpu
from jax.sharding import PartitionSpec as P

NMAX = 8
DISCOUNT = 0.99
ENTROPY_COEFF = 0.2
POLYAK_RATE = 0.005
STEP_SIZE = 0.1

F32 = jnp.float32
BF16 = jnp.bfloat16
MESH = pl.DeviceIdType.MESH

D = 2048
H = 2048
HALF = H // 2
T = 64
PAIR = 8
ROWS = T * PAIR
TM = 16
VMEM_LIMIT = 56
SCALE = D ** (-0.5)

WIDTHS_T = (384, 256, 384)
OFFSETS_T = (0, 384, 640)
WIDTHS = (256, 384, 384)
OFFSETS = (0, 256, 640)
ORDERS = (("z", "x", "y"), ("y", "z", "x"), ("x", "y", "z"))
PARTS = (0, 2, 1)
RS_PARTS = (2, 1, 0)
AG_SEMS = 8
RS_SEMS = 11
LINES = (2, 3, 1, 0)


def kernel(
    obs, nxt, onw_in, tgw_in, ld_in, step_in, onh_in, tgh_in, rew_in, logp_in, rst_in, hor, burn,
    gw, ret,
    onw, tgw, ld, step, onh, tgh, rew, logp, rst,
    xr_o, xr_n, xp_o, xp_n, xt, wst,
    wt0, wt1, wt2, wo0, wo1, wo2,
    pk_m, pk_i, bc0, bc1, qa0, qa1, cc, ss, pf, tp, vt, vo,
    sf, dfor, dback, ends_t, ends_o, lv, carry,
    q_s, q_r, q_n, nb_s, nb_r, du,
    g0, g1, g2,
    sh0, sh1, sh2, sw0, sw1, sw2, sb0, sb1, sb2,
    rh0, rh1, rh2, rw0, rw1, rw2, rb0, rb1, rb2,
    gx_s, gx_r,
    ag_ss, ag_rs, rs_ss, rs_rs, pre_ss, pre_rs, loc_sem, in_sem, d2d_ss, d2d_rs, nb_sem,
):
    tm = lax.axis_index("tm")
    batch = lax.axis_index("batch")
    y, x = tm // 4, tm % 4
    z, c = batch // 2, batch % 2
    at = {"y": y, "x": x, "z": z}
    other = 1 - c
    wb = ((wt0, wt1, wt2), (wo0, wo1, wo2))
    gg = (g0, g1, g2)
    snd_h, snd_w, snd_b = (sh0, sh1, sh2), (sw0, sw1, sw2), (sb0, sb1, sb2)
    rcv_h, rcv_w, rcv_b = (rh0, rh1, rh2), (rw0, rw1, rw2), (rb0, rb1, rb2)
    pending = []

    def device(core=c, **moved):
        here = {**at, **moved}
        return {"tm": here["y"] * 4 + here["x"], "batch": here["z"] * 2 + core}

    partner = {"tm": tm, "batch": z * 2 + other}

    def remote(src, dst, ss_, rs_, dev):
        return pltpu.make_async_remote_copy(
            src_ref=src, dst_ref=dst, send_sem=ss_, recv_sem=rs_, device_id=dev,
            device_id_type=MESH,
        )

    def send(src, dst, ss_, rs_, dev):
        copy = remote(src, dst, ss_, rs_, dev)
        copy.start()
        pending.append(copy)

    own_half = pl.ds(pl.multiple_of(c * 256, 256), 256)
    other_half = pl.ds(pl.multiple_of(other * 256, 256), 256)
    loads = [
        pltpu.make_async_copy(src, dst, in_sem.at[i])
        for i, (src, dst) in enumerate((
            (tgw_in, tgw), (onw_in, onw), (step_in, step), (rew_in, rew), (logp_in, logp),
            (rst_in, rst), (ld_in, ld), (onh_in, onh), (tgh_in, tgh),
        ))
    ]
    local = [
        pltpu.make_async_copy(nxt, xr_n.at[own_half, :], loc_sem.at[0]),
        pltpu.make_async_copy(obs, xr_o.at[own_half, :], loc_sem.at[1]),
    ]
    for copy in loads + local:
        copy.start()
    barrier = pltpu.get_barrier_semaphore()
    peers = [partner] + [device(z=lax.rem(z + d, 4)) for d in range(1, 4)]
    for a in "yxz":
        peers += [device(core=other, **{a: lax.rem(at[a] + d, 4)}) for d in range(1, 4)]
    peers += [{"tm": lax.rem(tm + d, TM), "batch": batch} for d in range(1, TM)]
    peers += [{"tm": lax.rem(tm + d, TM), "batch": z * 2 + other} for d in (1, TM - 1)]
    for dev in peers:
        pl.semaphore_signal(barrier, inc=1, device_id=dev, device_id_type=MESH)
    for copy in loads:
        copy.wait()

    mine = pl.ds(pl.multiple_of(c * HALF, HALF), HALF)
    theirs = pl.ds(pl.multiple_of(other * HALF, HALF), HALF)
    own_rows = pl.ds(pl.multiple_of(c * 16, 16), 16)
    other_rows = pl.ds(pl.multiple_of(other * 16, 16), 16)
    for m, w in enumerate((tgw, onw)):
        wst[m] = w[:, theirs].astype(BF16)
        for p in range(3):
            off = (OFFSETS_T, OFFSETS)[m][p]
            cols = pl.ds(pl.multiple_of(c * HALF + off, 128), (WIDTHS_T, WIDTHS)[m][p])
            wb[m][p][y, x, z, own_rows, :] = w[:, cols].astype(BF16)

    row8 = lax.broadcasted_iota(jnp.int32, (PAIR, 128), 0)
    lane8 = lax.broadcasted_iota(jnp.int32, (PAIR, 128), 1)
    row_own = (row8[:, :T] // 4) == c

    def twice(v):
        return jnp.where(row_own, jnp.concatenate([v, v], axis=0), 0.0)

    pk_m[...] = jnp.zeros_like(pk_m)
    for slot, r in enumerate((step, rew, logp)):
        pk_m[slot, :, :T] = twice(r[...])
    pk_m[3, :, :T] = twice(rst[...].astype(F32))
    hz = jnp.zeros((PAIR, 128), F32)
    bz = jnp.zeros((PAIR, 128), F32)
    for i in range(4):
        sel = row8 == c * 4 + i
        hz = jnp.where(sel, hor[i].astype(F32), hz)
        bz = jnp.where(sel, burn[i].astype(F32), bz)
    pk_m[4] = hz
    pk_m[5] = bz

    pl.semaphore_wait(barrier, len(peers))

    def w_half(m, p):
        src, dst = wst.at[m, :, cols_of(p, m)], wb[m][p].at[y, x, z, own_rows, :]
        return remote(src, dst, d2d_ss.at[0], d2d_rs.at[m], partner)

    def w_half_in(m):
        remote(wst.at[m], wst.at[m], d2d_ss.at[0], d2d_rs.at[m], partner).wait_recv()

    def width(m, p):
        return (WIDTHS_T, WIDTHS)[m][p]

    def cols_of(p, m=1):
        return pl.ds((OFFSETS_T, OFFSETS)[m][p], width(m, p))

    for m in range(2):
        for p in range(3):
            w_half(m, p).start()
    send(pk_m, pk_i, d2d_ss.at[2], d2d_rs.at[2], partner)
    send(nxt, xr_n.at[own_half, :], d2d_ss.at[3], d2d_rs.at[3], partner)
    send(obs, xr_o.at[own_half, :], d2d_ss.at[4], d2d_rs.at[4], partner)

    def place(p, first, second, last):
        idx = dict(zip(ORDERS[p], (first, second, last)))
        return idx["y"], idx["x"], idx["z"]

    def turned(p, i, d):
        return lax.rem(at[ORDERS[p][i]] + d, 4)

    def toward(p, i, d, core=c):
        return device(core=core, **{ORDERS[p][i]: turned(p, i, d)})

    FULL = pl.ds(0, 4)

    def half_of(h):
        return FULL if h is None else pl.ds(2 * h, 2)

    def ag_copy(m, p, k, j, where, dev):
        ref = wb[m][p].at[where]
        n = m * 3 + p
        return remote(ref, ref, ag_ss.at[n * 3 + k], ag_rs.at[n * AG_SEMS + 3 * m + j], dev)

    def ag_end(m, p, l):
        return 7 + l if p == 2 else 7

    def ag_send(m, p, k, j, where, dev):
        ag_copy(m, p, k, j, where, dev).start()

    def ag_wait(m, p, j, where):
        ag_copy(m, p, 0, j, where, partner).wait_recv()

    def ag_drain(m, p):
        for k, where in enumerate(((0, 0, pl.ds(0, 3)), (0, pl.ds(0, 3)), (pl.ds(0, 3),))):
            ag_copy(m, p, k, 0, where, partner).wait_send()

    def line(p, second, last, h=None):
        return place(p, half_of(h), second, last)

    def ag_one(m, p):
        dst = wb[m][p].at[y, x, z, own_rows, :]
        sem, n = ag_ss.at[(m * 3 + p) * 3], (m * 3 + p) * AG_SEMS + 3 * m
        for d in (2, 1, 3):
            remote(dst, dst, sem, ag_rs.at[n], toward(p, 0, d)).start()
            src = wst.at[m, :, cols_of(p, m)]
            remote(src, dst, sem, ag_rs.at[n], toward(p, 0, d, other)).start()

    def ag_one_in(m, p):
        ag_wait(m, p, 0, (0, 0, pl.ds(0, 3)))

    def ag_own(m, p, k):
        for d in (1, 3, 2):
            where = place(p, turned(p, 0, d), turned(p, 1, 0), turned(p, 2, 0))
            ag_send(m, p, k, 2 * k - 1, where, toward(p, k, 1))
            ag_send(m, p, k, 2 * k - 1, where, toward(p, k, 3))

    def ag_early(m, p):
        for k in (1, 2):
            ag_send(m, p, k, 2 * k - 1, (y, x, z), toward(p, k, 1))
            ag_send(m, p, k, 2 * k - 1, (y, x, z), toward(p, k, 3))

    def ag_two_forward(m, p):
        q3 = turned(p, 2, 0)
        ag_wait(m, p, 1, (0, pl.ds(0, 2)))
        ag_send(m, p, 1, 2, line(p, turned(p, 1, 3), q3, 0), toward(p, 1, 1))
        ag_send(m, p, 1, 2, line(p, turned(p, 1, 1), q3, 1), toward(p, 1, 3))

    def ag_two_last(m, p):
        ag_wait(m, p, 2, line(p, turned(p, 1, 2), turned(p, 2, 0)))

    def ag_three(m, p, l):
        own = line(p, turned(p, 1, l), turned(p, 2, 0))
        ag_send(m, p, 2, 3 + l, own, toward(p, 2, 1))
        ag_send(m, p, 2, 3 + l, own, toward(p, 2, 3))

    def ag_three_forward(m, p, l):
        second = turned(p, 1, l)
        ag_wait(m, p, 3 + l, (0, pl.ds(0, 2)))
        end = ag_end(m, p, l)
        ag_send(m, p, 2, end, line(p, second, turned(p, 2, 3), 0), toward(p, 2, 1))
        ag_send(m, p, 2, end, line(p, second, turned(p, 2, 1), 1), toward(p, 2, 3))

    def ag_three_last(m, p):
        ag_wait(m, p, 7, place(p, FULL, FULL, turned(p, 2, 2)))

    def ag_line_last(m, l):
        ag_wait(m, 2, 7 + l, line(2, turned(2, 1, l), turned(2, 2, 2)))

    def wide(v, w=HALF):
        return jnp.concatenate([v] * (w // 128), axis=1)

    def at_t(t):
        return pl.ds(pl.multiple_of(t * PAIR, PAIR), PAIR)

    def spread_lanes(dst, v):
        for t in range(T):
            dst[pl.ds(t * PAIR, PAIR), :] = jnp.broadcast_to(v[:, t : t + 1], (PAIR, 128))

    r_out = lax.broadcasted_iota(jnp.int32, (ROWS, ROWS), 0)
    r_in = lax.broadcasted_iota(jnp.int32, (ROWS, ROWS), 1)

    def permutation():
        return jnp.where(r_out == (r_in % T) * PAIR + r_in // T, 1.0, 0.0).astype(BF16)

    def permute_next():
        perm = permutation()

        def body(i, _):
            cols = pl.ds(pl.multiple_of(i * 256, 256), 256)
            xp_n[:, cols] = jnp.dot(perm, xr_n[:, cols], preferred_element_type=F32).astype(BF16)
            return 0

        lax.fori_loop(0, D // 256, body, 0)

    def permute_obs(lo, hi):
        perm = permutation()

        def body(i, _):
            cols = pl.ds(pl.multiple_of(i * 256, 256), 256)
            v = jnp.dot(perm, xr_o[:, cols], preferred_element_type=F32)
            xp_o[:, cols] = v.astype(BF16)
            xt[i // 2, pl.ds(2 * (i % 2), 2)] = v.T.astype(BF16).reshape(2, 4, 32, ROWS)
            return 0

        lax.fori_loop(lo, hi, body, 0)

    def project_planes(m, p, planes, fresh):
        xp, v = (xp_n, vt) if m == 0 else (xp_o, vo)
        cols, w = cols_of(p, m), width(m, p)
        axis = 1 if p == 2 else 2
        qs = [turned(p, axis, d) for d in planes]

        def tile(i, _):
            rows = pl.ds(pl.multiple_of(i * 256, 256), 256)
            acc = None if fresh else v[rows, cols]
            for q in qs:
                where = place(p, FULL, q, FULL) if p == 2 else place(p, FULL, FULL, q)
                rhs = wb[m][p][where].reshape(512, w)
                if p == 1:
                    starts = [pl.multiple_of((k * 4 + q) * 128, 128) for k in range(4)]
                    lhs = jnp.concatenate([xp[rows, pl.ds(k, 128)] for k in starts], axis=1)
                else:
                    lhs = xp[rows, pl.ds(pl.multiple_of(q * 512, 512), 512)]
                part = jnp.dot(lhs, rhs, preferred_element_type=F32) * SCALE
                acc = part if acc is None else acc + part
            v[rows, cols] = acc
            return 0

        lax.fori_loop(0, ROWS // 256, tile, 0)

    def scan(m, v, p, ends):
        cols = cols_of(p, m)

        def body(i, st):
            steps = [at_t(i * 4 + k) for k in range(4)]
            added = [ss[rows, cols] * v[rows, cols] for rows in steps]
            kept = [cc[rows, cols] for rows in steps]
            states = []
            for f, u in zip(kept, added):
                st = f * st + u
                states.append(st)
            for rows, state in zip(steps, states):
                v[rows, cols] = state
            return st

        last = lax.fori_loop(0, T // 4, body, jnp.zeros((PAIR, width(m, p)), F32))
        ends[tm, :, cols] = last.astype(BF16)

    def ends_copy(n, ends, p, slots, dev):
        cols = pl.ds(0, HALF) if p is None else cols_of(p)
        ref = ends.at[slots, :, cols]
        return remote(ref, ref, pre_ss.at[n], pre_rs.at[n], dev)

    def prefix_send(n, ends, p, forward):
        for d in range(TM - 1, 0, -1):
            to = tm + d if forward else tm - d

            @pl.when(to < TM if forward else to >= 0)
            def _(to=to):
                ends_copy(n, ends, p, tm, {"tm": to, "batch": batch}).start()

    def prefix_wait(n, ends, p, count, arrived):
        for k in range(1, TM):

            @pl.when(count == k)
            def _(k=k):
                copies = ends_copy(n, ends, p, pl.ds(0, k), partner)
                copies.wait_recv() if arrived else copies.wait_send()

    def prefix_take(n, ends, p, forward):
        cols, w = (pl.ds(0, HALF), HALF) if p is None else (cols_of(p), WIDTHS[p])
        prefix_wait(n, ends, p, tm if forward else TM - 1 - tm, True)
        decay = dfor if forward else dback
        v = jnp.zeros((PAIR, w), F32)
        for j in range(TM - 1) if forward else range(TM - 1, 0, -1):
            counted = jnp.where(j < tm if forward else j > tm, 1.0, 0.0)
            v = decay[j, :, cols] * v + counted * ends[j, :, cols].astype(F32)
        carry[:, cols] = v

    def prefix_drain(n, ends, p, forward):
        prefix_wait(n, ends, p, TM - 1 - tm if forward else tm, False)

    def quality(m, v, heads, p, fresh, slope):
        cols, w = cols_of(p, m), width(m, p)
        hcols = pl.ds(pl.multiple_of(c * HALF + (OFFSETS_T, OFFSETS)[m][p], 128), w)
        h0 = jnp.broadcast_to(heads[0:1, hcols], (PAIR, w))
        h1 = jnp.broadcast_to(heads[1:2, hcols], (PAIR, w))
        start = carry[:, cols]

        def fold(u):
            out = u[:, :128]
            for i in range(1, w // 128):
                out = out + u[:, i * 128 : (i + 1) * 128]
            return out

        def body(i, _):
            steps = [at_t(i * 8 + k) for k in range(8)]
            states = [v[rows, cols] + pf[rows, cols] * start for rows in steps]
            before = None if fresh else [(qa0[rows, :], qa1[rows, :]) for rows in steps]
            out = []
            for st in states:
                sig = 1.0 / (1.0 + jnp.exp(-st))
                act = st * sig
                out.append((fold(act * h0), fold(act * h1), sig + act * (1.0 - sig)))
            for k, (rows, (f0, f1, rise)) in enumerate(zip(steps, out)):
                qa0[rows, :] = f0 if fresh else before[k][0] + f0
                qa1[rows, :] = f1 if fresh else before[k][1] + f1
                if slope:
                    v[rows, cols] = rise
            return 0

        lax.fori_loop(0, T // 8, body, 0)

    def quality_send(slot):
        def body(i, acc):
            a0, a1 = acc
            for k in range(16):
                rows = at_t(i * 16 + k)
                here = lane8 == i * 16 + k
                a0 = jnp.where(here, jnp.sum(qa0[rows, :], axis=1, keepdims=True), a0)
                a1 = jnp.where(here, jnp.sum(qa1[rows, :], axis=1, keepdims=True), a1)
            return a0, a1

        zero = jnp.zeros((PAIR, 128), F32)
        a0, a1 = lax.fori_loop(0, T // 16, body, (zero, zero))
        q_s[slot, 0] = a0
        q_s[slot, 1] = a1
        send(q_s.at[slot], q_r.at[slot], d2d_ss.at[5 + slot], d2d_rs.at[5 + slot], partner)

    def quality_sum(slot):
        remote(
            q_s.at[slot], q_r.at[slot], d2d_ss.at[5 + slot], d2d_rs.at[5 + slot], partner
        ).wait_recv()
        return [q_s[slot, k] + q_r[slot, k] for k in range(2)]

    for m in range(2):
        for p in range(3):
            ag_one(m, p)
    for m in range(2):
        w_half_in(m)
        for p in range(3):
            ag_early(m, p)
    for p in range(3):
        ag_one_in(0, p)
        ag_own(0, p, 1)
    for p in range(3):
        ag_own(0, p, 2)
    def clear(j, _):
        @pl.when(j > tm)
        def _():
            ends_t[j] = jnp.zeros((PAIR, HALF), BF16)
            ends_o[j] = jnp.zeros((PAIR, HALF), BF16)

        @pl.when(j < tm)
        def _():
            lv[j] = jnp.zeros((PAIR, HALF), BF16)

        return 0

    lax.fori_loop(0, TM, clear, 0)
    remote(pk_m, pk_i, d2d_ss.at[2], d2d_rs.at[2], partner).wait_recv()
    step8 = pk_m[0] + pk_i[0]
    rew8 = pk_m[1] + pk_i[1]
    logp8 = pk_m[2] + pk_i[2]
    rst8 = pk_m[3] + pk_i[3]
    keep8 = 1.0 - rst8
    hor8 = pk_m[4] + pk_i[4]
    burn8 = pk_m[5] + pk_i[5]

    sf[tm, 0] = jnp.broadcast_to(jnp.sum(step8, axis=1, keepdims=True), (PAIR, 128))
    sf[tm, 1] = jnp.broadcast_to(1.0 - jnp.max(rst8, axis=1, keepdims=True), (PAIR, 128))
    for d in range(1, TM):
        dev = {"tm": lax.rem(tm + d, TM), "batch": batch}
        remote(sf.at[tm], sf.at[tm], pre_ss.at[0], pre_rs.at[0], dev).start()

    nb_s[0] = rew8
    nb_s[1] = logp8
    nb_s[2] = keep8
    earlier = lax.rem(tm + TM - 1, TM)
    before = {"tm": earlier, "batch": batch}
    send(nb_s, nb_r, nb_sem.at[0], nb_sem.at[1], before)
    spread_lanes(bc0, step8)
    spread_lanes(bc1, keep8)
    ld8 = jnp.broadcast_to(ld[:, mine], (PAIR, HALF))

    def factors(t, prod):
        e = jnp.exp(wide(bc0[at_t(t), :]) * ld8)
        f = e * wide(bc1[at_t(t), :])
        cc[at_t(t), :] = f
        ss[at_t(t), :] = jnp.sqrt(1.0 - e * e)
        prod = prod * f
        pf[at_t(t), :] = prod
        return prod

    lax.fori_loop(0, T, factors, jnp.ones((PAIR, HALF), F32))
    for p in range(3):
        ag_one_in(1, p)
        ag_own(1, p, 1)
    for p in range(3):
        ag_two_forward(0, p)
        ag_three(0, p, 3)
        ag_three(0, p, 1)
    local[0].wait()
    remote(nxt, xr_n.at[other_half, :], d2d_ss.at[3], d2d_rs.at[3], partner).wait_recv()
    permute_next()
    for p in range(3):
        ag_three_forward(0, p, 0)
    local[1].wait()
    remote(obs, xr_o.at[other_half, :], d2d_ss.at[4], d2d_rs.at[4], partner).wait_recv()
    permute_obs(0, 8)
    for p in range(3):
        ag_two_last(0, p)
        ag_three(0, p, 2)
    for l in (3, 1):
        for p in range(3):
            ag_three_forward(0, p, l)
    for p in range(3):
        ag_two_forward(1, p)
        ag_own(1, p, 2)
    def tails(i, prod):
        t = T - 1 - i
        tp[at_t(t), :] = prod
        return prod * cc[at_t(t), :]

    lax.fori_loop(0, T, tails, jnp.ones((PAIR, HALF), F32))
    for p in range(3):
        ag_three_forward(0, p, 2)
        ag_three(1, p, 3)
        ag_three(1, p, 1)
    for p in (0, 1):
        project_planes(0, p, (0, 1, 3), True)
    for p in range(3):
        ag_two_last(1, p)
        ag_three(1, p, 2)
    sums = remote(
        sf.at[pl.ds(0, TM - 1)], sf.at[pl.ds(0, TM - 1)], pre_ss.at[0], pre_rs.at[0], partner
    )
    sums.wait_recv()

    def block_decay(j, _):
        v = jnp.exp(wide(sf[j, 0]) * ld8) * wide(sf[j, 1])
        dfor[j] = jnp.where(j < tm, v, 1.0)
        dback[j] = jnp.where(j > tm, v, 1.0)
        return 0

    lax.fori_loop(0, TM, block_decay, 0)
    for p in range(3):
        ag_three_forward(1, p, 0)
    for p in (0, 1, 2):
        if p == 2:
            for l in range(4):
                ag_line_last(0, l)
            project_planes(0, p, (0, 1, 3, 2), True)
        else:
            ag_three_last(0, p)
            project_planes(0, p, (2,), False)
        scan(0, vt, p, ends_t)
    prefix_send(1, ends_t, None, True)
    for p in range(3):
        ag_three_forward(1, p, 3)
    for p in range(3):
        ag_three_forward(1, p, 1)
    for p in (0, 1):
        project_planes(1, p, (0,), True)
    for p in range(3):
        ag_three_forward(1, p, 2)
    for p in (0, 1):
        project_planes(1, p, (1, 3), False)
    for l in (0, 3, 1):
        ag_line_last(1, l)
    project_planes(1, 2, (0, 1, 3), True)
    ag_three_last(1, 0)
    project_planes(1, 0, (2,), False)
    scan(1, vo, PARTS[0], ends_o)
    prefix_send(2 + PARTS[0], ends_o, PARTS[0], True)
    ag_line_last(1, 2)
    project_planes(1, 2, (2,), False)
    scan(1, vo, PARTS[1], ends_o)
    prefix_send(2 + PARTS[1], ends_o, PARTS[1], True)
    ag_three_last(1, 1)
    project_planes(1, 1, (2,), False)
    scan(1, vo, PARTS[2], ends_o)
    prefix_send(2 + PARTS[2], ends_o, PARTS[2], True)
    prefix_take(1, ends_t, None, True)
    for p in PARTS:
        quality(0, vt, tgh, p, p == PARTS[0], False)
    quality_send(0)
    for core in range(2):
        dev = {"tm": earlier, "batch": z * 2 + core}
        remote(q_s.at[0], q_n.at[c], nb_sem.at[2], nb_sem.at[3], dev).start()
    prefix_take(2 + PARTS[0], ends_o, PARTS[0], True)
    quality(1, vo, onh, PARTS[0], True, True)

    for p in PARTS[1:]:
        prefix_take(2 + p, ends_o, p, True)
        quality(1, vo, onh, p, False, True)
    quality_send(1)
    def value_of(products, log_prob):
        tq = [v * (H ** (-0.5)) for v in products]
        return jnp.minimum(tq[0], tq[1]) - ENTROPY_COEFF * log_prob

    value8 = value_of(quality_sum(0), logp8)
    remote(nb_s, nb_r, nb_sem.at[0], nb_sem.at[1], before).wait_recv()
    later_q = remote(q_n, q_n, nb_sem.at[2], nb_sem.at[3], before)
    later_q.wait_recv()
    later_value = value_of([q_n[0, k] + q_n[1, k] for k in range(2)], nb_r[1])
    inside = (lane8 >= T) & (lane8 < T + NMAX) & (tm < TM - 1)

    def extended(own, later):
        later = jnp.where(inside, pltpu.roll(later, T, 1), 0.0)
        return jnp.where(lane8 < T, own, later)

    ext_r, ext_v = extended(rew8, nb_r[0]), extended(value8, later_value)
    ext_k = extended(keep8, nb_r[2])

    def shifted(v, n):
        return v if n == 0 else pltpu.roll(v, 128 - n, 1)

    total = jnp.zeros((PAIR, 128), F32)
    alive = jnp.ones((PAIR, 128), F32)
    for n in range(NMAX):
        total = total + jnp.where(hor8 > n, DISCOUNT**n * alive * shifted(ext_r, n), 0.0)
        alive = alive * shifted(ext_k, n + 1)
        total = total + jnp.where(
            hor8 == n + 1, DISCOUNT ** (n + 1) * alive * shifted(ext_v, n + 1), 0.0
        )
    ret[...] = jnp.where(c == 0, total[:4, :T], total[4:, :T])
    weight = jnp.where((lane8 + tm * T).astype(F32) >= burn8, 1.0, 0.0)

    oq = quality_sum(1)
    spread_lanes(bc0, weight * (oq[0] * (H ** (-0.5)) - total) * (H ** (-0.5)))
    spread_lanes(bc1, weight * (oq[1] * (H ** (-0.5)) - total) * (H ** (-0.5)))

    h0 = jnp.broadcast_to(onh[0:1, mine], (PAIR, HALF))
    h1 = jnp.broadcast_to(onh[1:2, mine], (PAIR, HALF))

    def back(i, adj):
        steps = [at_t(T - 1 - (i * 2 + k)) for k in range(2)]
        own = [
            (wide(bc0[rows, :]) * h0 + wide(bc1[rows, :]) * h1) * vo[rows, :] for rows in steps
        ]
        for rows, dh in zip(steps, own):
            adj = dh + adj
            vo[rows, :] = adj
            adj = cc[rows, :] * adj
        return adj

    leaving = lax.fori_loop(0, T // 2, back, jnp.zeros((PAIR, HALF), F32))
    lv[tm] = leaving.astype(BF16)
    prefix_send(5, lv, None, False)

    def finish(p):
        cols = cols_of(p)
        incoming = carry[:, cols]
        both = jnp.concatenate([incoming, incoming], axis=0)

        def body(i, _):
            for k in range(2):
                rows = pl.ds(pl.multiple_of(i * 32 + k * 16, 16), 16)
                adj = vo[rows, cols] + tp[rows, cols] * both
                du[rows, cols] = (ss[rows, cols] * adj).astype(BF16)
            return 0

        lax.fori_loop(0, ROWS // 32, body, 0)

    def gradient(p, l):
        where = place(p, FULL, turned(p, 1, l), FULL)
        lhs = xt[where].reshape(512, ROWS)
        v = jnp.dot(lhs, du[:, cols_of(p)], preferred_element_type=F32)
        gg[p][where] = v.reshape(4, 4, 32, WIDTHS[p])

    def rs_copy(p, k, j, src, dst, dev):
        return remote(src, dst, rs_ss.at[p * 3 + k], rs_rs.at[p * RS_SEMS + j], dev)

    def rs_half(p, s, h, dev):
        return rs_copy(p, 0, s, snd_h[p].at[s, h], rcv_h[p].at[s, h], dev)

    def rs_whole(p, s, h, dev):
        return rs_copy(p, 1, 5 + s, snd_w[p].at[s, h], rcv_w[p].at[s, h], dev)

    def rs_drain(p):
        for k, (src, dst) in enumerate(
            ((snd_h[p], rcv_h[p]), (snd_w[p], rcv_w[p]), (snd_b[p], rcv_b[p]))
        ):
            rs_copy(p, k, 0, src, dst, partner).wait_send()

    def rs_ref(p, s, d, h=None):
        if s < 4:
            return line(p, turned(p, 1, s), turned(p, 2, d), h)
        return line(p, turned(p, 1, d), turned(p, 2, 0), h)

    def rs_axis(s):
        return 2 if s < 4 else 1

    def rs_opposite(p, s):
        for h, d in ((0, 3), (1, 1)):
            snd_h[p][s, h] = gg[p][rs_ref(p, s, 2, h)].astype(BF16)
            rs_half(p, s, h, toward(p, rs_axis(s), d)).start()

    def rs_arrived(p, s):
        rs_copy(p, 0, s, snd_h[p].at[s], rcv_h[p].at[s], partner).wait_recv()

    def rs_neighbour(p, s, h):
        d = (3, 1)[h]
        with_recv = gg[p][rs_ref(p, s, d, h)] + rcv_h[p][s, h].astype(F32)
        snd_w[p][s, h, pl.ds(2 * h, 2)] = with_recv.astype(BF16)
        snd_w[p][s, h, pl.ds(2 - 2 * h, 2)] = gg[p][rs_ref(p, s, d, 1 - h)].astype(BF16)
        rs_whole(p, s, h, toward(p, rs_axis(s), d)).start()

    def rs_neighbours(p, s):
        rs_arrived(p, s)
        rs_neighbour(p, s, 0)
        rs_neighbour(p, s, 1)

    def rs_sum(p, s):
        rs_copy(p, 1, 5 + s, snd_w[p].at[s], rcv_w[p].at[s], partner).wait_recv()
        own = rs_ref(p, s, 0)
        both = rcv_w[p][s, 0].astype(F32) + rcv_w[p][s, 1].astype(F32)
        gg[p][own] = gg[p][own] + both

    def rs_one(p):
        for d in (2, 1, 3):
            where = place(p, turned(p, 0, d), turned(p, 1, 0), turned(p, 2, 0))
            for core in range(2):
                block = gg[p][(*where, pl.ds(16 * core, 16))]
                snd_b[p][core, d - 1] = block.astype(BF16)
                rs_copy(
                    p, 2, 10, snd_b[p].at[core, d - 1], rcv_b[p].at[c, d - 1],
                    toward(p, 0, d, core),
                ).start()
        gx_s[:, cols_of(p)] = gg[p][y, x, z, other_rows, :]

    prefix_take(5, lv, None, False)
    for p in RS_PARTS:
        finish(p)
        gradient(p, LINES[0])
        rs_opposite(p, LINES[0])
    for p in RS_PARTS:
        gradient(p, LINES[1])
        rs_opposite(p, LINES[1])
    for p in RS_PARTS:
        rs_neighbours(p, LINES[0])
        gradient(p, LINES[2])
        rs_opposite(p, LINES[2])
    for p in RS_PARTS:
        rs_neighbours(p, LINES[1])
        gradient(p, LINES[3])
        rs_opposite(p, LINES[3])
    for p in RS_PARTS:
        rs_sum(p, LINES[0])
        rs_opposite(p, 4)
    for p in RS_PARTS:
        rs_neighbours(p, LINES[2])
    for p in RS_PARTS:
        rs_sum(p, LINES[1])
        rs_arrived(p, 4)
        rs_neighbour(p, 4, 0)
    for p in RS_PARTS:
        rs_neighbours(p, LINES[3])
    for p in RS_PARTS:
        rs_sum(p, LINES[2])
        rs_neighbour(p, 4, 1)
    prefix_drain(1, ends_t, None, True)
    for p in range(3):
        prefix_drain(2 + p, ends_o, p, True)
        ag_drain(0, p)
        ag_drain(1, p)
    prefix_drain(5, lv, None, False)
    remote(wst, wst, d2d_ss.at[0], d2d_rs.at[0], partner).wait_send()
    sums.wait_send()
    later_q.wait_send()
    for copy in pending:
        copy.wait_send()
    pending.clear()
    for p in RS_PARTS:
        rs_sum(p, LINES[3])
    for p in RS_PARTS:
        rs_sum(p, 4)
        rs_one(p)
    send(gx_s, gx_r, d2d_ss.at[7], d2d_rs.at[7], partner)
    remote(gx_s, gx_r, d2d_ss.at[7], d2d_rs.at[7], partner).wait_recv()
    for p in range(3):
        rs_copy(p, 2, 10, snd_b[p], rcv_b[p], partner).wait_recv()
        for core, v in (
            (c, gg[p][y, x, z, own_rows, :]), (other, gx_r[:, cols_of(p)]),
        ):
            for d in range(3):
                v = v + rcv_b[p][core, d].astype(F32)
            cols = pl.ds(pl.multiple_of(core * HALF + OFFSETS[p], 128), WIDTHS[p])
            gw[:, cols] = v

    for p in range(3):
        rs_drain(p)
    for copy in pending:
        copy.wait_send()


def update(grad, returns, onw, tgw, grad_w, new_target, returns_out):
    g = grad[...] * SCALE
    grad_w[...] = g
    new_target[...] = (1.0 - POLYAK_RATE) * tgw[...] + POLYAK_RATE * (onw[...] - STEP_SIZE * g)
    returns_out[...] = returns[...]


def shards(
    obs_feats, next_feats, online_w, target_w, log_decay, step_scale, online_heads, target_heads,
    reward, next_action_log_prob, resets, horizon, burn_in,
):
    vmem = pl.BlockSpec(memory_space=pltpu.VMEM)
    smem = pl.BlockSpec(memory_space=pltpu.SMEM)
    hbm = pl.BlockSpec(memory_space=pltpu.HBM)
    small = (
        online_w, target_w, log_decay[None], step_scale, online_heads, target_heads,
        reward, next_action_log_prob, resets,
    )
    weights = [pltpu.VMEM((4, 4, 4, 32, w), BF16) for w in WIDTHS_T + WIDTHS]
    staged = [
        *[pltpu.VMEM((5, 2, 2, 32, w), BF16) for w in WIDTHS],
        *[pltpu.VMEM((5, 2, 4, 32, w), BF16) for w in WIDTHS],
        *[pltpu.VMEM((2, 3, 16, w), BF16) for w in WIDTHS],
    ]
    big = pltpu.VMEM((ROWS, HALF), F32)
    table = pltpu.VMEM((TM, PAIR, HALF), F32)
    ends = pltpu.VMEM((TM, PAIR, HALF), BF16)
    narrow = pltpu.VMEM((ROWS, 128), F32)
    scratch = [
        *[pltpu.VMEM(a.shape, a.dtype) for a in small],
        pltpu.VMEM((ROWS, D), BF16), pltpu.VMEM((ROWS, D), BF16),
        pltpu.VMEM((ROWS, D), BF16), pltpu.VMEM((ROWS, D), BF16),
        pltpu.VMEM((4, 4, 4, 32, ROWS), BF16), pltpu.VMEM((2, 16, HALF), BF16),
        *weights,
        pltpu.VMEM((6, PAIR, 128), F32), pltpu.VMEM((6, PAIR, 128), F32),
        narrow, narrow, narrow, narrow,
        big, big, big, big, big, big,
        pltpu.VMEM((TM, 2, PAIR, 128), F32), table, table, ends, ends, ends,
        pltpu.VMEM((PAIR, HALF), F32),
        pltpu.VMEM((2, 2, PAIR, 128), F32), pltpu.VMEM((2, 2, PAIR, 128), F32),
        pltpu.VMEM((2, 2, PAIR, 128), F32),
        pltpu.VMEM((3, PAIR, 128), F32), pltpu.VMEM((3, PAIR, 128), F32),
        pltpu.VMEM((ROWS, HALF), BF16),
        *[pltpu.VMEM((4, 4, 4, 32, w), F32) for w in WIDTHS],
        *staged, *staged,
        pltpu.VMEM((16, HALF), F32), pltpu.VMEM((16, HALF), F32),
        pltpu.SemaphoreType.DMA((18,)), pltpu.SemaphoreType.DMA((6 * AG_SEMS + 6,)),
        pltpu.SemaphoreType.DMA((9,)), pltpu.SemaphoreType.DMA((3 * RS_SEMS,)),
        pltpu.SemaphoreType.DMA((6,)), pltpu.SemaphoreType.DMA((6,)),
        pltpu.SemaphoreType.DMA((2,)), pltpu.SemaphoreType.DMA((9,)),
        pltpu.SemaphoreType.DMA((8,)), pltpu.SemaphoreType.DMA((8,)),
        pltpu.SemaphoreType.DMA((4,)),
    ]
    rows_b, span, width = obs_feats.shape
    grad, returns = pl.pallas_call(
        kernel,
        name="critic_step",
        out_shape=(
            jax.ShapeDtypeStruct(online_w.shape, F32),
            jax.ShapeDtypeStruct(reward.shape, F32),
        ),
        in_specs=[hbm] * 11 + [smem] * 2,
        out_specs=(vmem, vmem),
        scratch_shapes=scratch,
        compiler_params=pltpu.CompilerParams(
            collective_id=0, has_side_effects=True, vmem_limit_bytes=VMEM_LIMIT * 1024 * 1024
        ),
    )(
        obs_feats.reshape(rows_b * span, width), next_feats.reshape(rows_b * span, width),
        *small, horizon, burn_in,
    )
    return pl.pallas_call(
        update,
        name="target_update",
        out_shape=(
            jax.ShapeDtypeStruct(online_w.shape, F32),
            jax.ShapeDtypeStruct(target_w.shape, F32),
            jax.ShapeDtypeStruct(reward.shape, F32),
        ),
        in_specs=[vmem] * 4,
        out_specs=(vmem, vmem, vmem),
    )(grad, returns, online_w, target_w)


def solution(mesh):
    return jax.shard_map(
        shards,
        mesh=mesh,
        in_specs=(
            P("batch", "tm", None), P("batch", "tm", None),
            P(("tm", "batch"), None), P(("tm", "batch"), None),
            P(), P("batch", "tm"), P(), P(),
            P("batch", "tm"), P("batch", "tm"), P("batch", "tm"), P("batch"), P("batch"),
        ),
        out_specs=(P(("tm", "batch"), None), P(("tm", "batch"), None), P("batch", "tm")),
        check_vma=False,
    )
```

```python
import jax
import jax.numpy as jnp
from jax import lax
from jax.experimental import pallas as pl
from jax.experimental.pallas import tpu as pltpu
from jax.sharding import PartitionSpec as P

NMAX = 8
DISCOUNT = 0.99
ENTROPY_COEFF = 0.2
POLYAK_RATE = 0.005
STEP_SIZE = 0.1

F32 = jnp.float32
BF16 = jnp.bfloat16
MESH = pl.DeviceIdType.MESH

D = 2048
H = 2048
HALF = H // 2
T = 64
PAIR = 8
ROWS = T * PAIR
TM = 16
VMEM_LIMIT = 56
SCALE = D ** (-0.5)

WIDTHS_T = (384, 384, 256)
OFFSETS_T = (0, 384, 768)
WIDTHS = (256, 384, 384)
OFFSETS = (0, 256, 640)
ORDERS = (("z", "x", "y"), ("y", "z", "x"), ("x", "y", "z"))
PARTS = (0, 2, 1)
RS_PARTS = (2, 1, 0)
PROJECTED = 512
AG_SEMS = 8
RS_SEMS = 11
LINES = (2, 3, 1, 0)


def kernel(
    obs, nxt, onw_in, tgw_in, ld_in, step_in, onh_in, tgh_in, rew_in, logp_in, rst_in, hor, burn,
    gw, ret,
    onw, tgw, ld, step, onh, tgh, rew, logp, rst,
    xr_o, xr_n, xp_o, xp_n, xt, wst,
    wt0, wt1, wt2, wo0, wo1, wo2,
    pk_m, pk_i, bc0, bc1, qa0, qa1, cc, ss, pf, tp, vt, vo,
    sf, dfor, dback, ends_t, ends_o, lv, carry,
    q_s, q_r, q_n, nb_s, nb_r, du,
    g0, g1, g2,
    sh0, sh1, sh2, sw0, sw1, sw2, sb0, sb1, sb2,
    rh0, rh1, rh2, rw0, rw1, rw2, rb0, rb1, rb2,
    gx_s, gx_r,
    ag_ss, ag_rs, rs_ss, rs_rs, pre_ss, pre_rs, loc_sem, in_sem, d2d_ss, d2d_rs, nb_sem,
):
    tm = lax.axis_index("tm")
    batch = lax.axis_index("batch")
    y, x = tm // 4, tm % 4
    z, c = batch // 2, batch % 2
    at = {"y": y, "x": x, "z": z}
    other = 1 - c
    wb = ((wt0, wt1, wt2), (wo0, wo1, wo2))
    gg = (g0, g1, g2)
    snd_h, snd_w, snd_b = (sh0, sh1, sh2), (sw0, sw1, sw2), (sb0, sb1, sb2)
    rcv_h, rcv_w, rcv_b = (rh0, rh1, rh2), (rw0, rw1, rw2), (rb0, rb1, rb2)
    pending = []

    def device(core=c, **moved):
        here = {**at, **moved}
        return {"tm": here["y"] * 4 + here["x"], "batch": here["z"] * 2 + core}

    partner = {"tm": tm, "batch": z * 2 + other}

    def remote(src, dst, ss_, rs_, dev):
        return pltpu.make_async_remote_copy(
            src_ref=src, dst_ref=dst, send_sem=ss_, recv_sem=rs_, device_id=dev,
            device_id_type=MESH,
        )

    def send(src, dst, ss_, rs_, dev):
        copy = remote(src, dst, ss_, rs_, dev)
        copy.start()
        pending.append(copy)

    own_half = pl.ds(pl.multiple_of(c * 256, 256), 256)
    other_half = pl.ds(pl.multiple_of(other * 256, 256), 256)
    loads = [
        pltpu.make_async_copy(src, dst, in_sem.at[i])
        for i, (src, dst) in enumerate((
            (tgw_in, tgw), (onw_in, onw), (step_in, step), (rew_in, rew), (logp_in, logp),
            (rst_in, rst), (ld_in, ld), (onh_in, onh), (tgh_in, tgh),
        ))
    ]
    local = [
        pltpu.make_async_copy(nxt, xr_n.at[own_half, :], loc_sem.at[0]),
        pltpu.make_async_copy(obs, xr_o.at[own_half, :], loc_sem.at[1]),
    ]
    for copy in loads + local:
        copy.start()
    barrier = pltpu.get_barrier_semaphore()
    peers = [partner] + [device(z=lax.rem(z + d, 4)) for d in range(1, 4)]
    for a in "yxz":
        peers += [device(core=other, **{a: lax.rem(at[a] + d, 4)}) for d in range(1, 4)]
    peers += [{"tm": lax.rem(tm + d, TM), "batch": batch} for d in range(1, TM)]
    peers += [{"tm": lax.rem(tm + d, TM), "batch": z * 2 + other} for d in (1, TM - 1)]
    for dev in peers:
        pl.semaphore_signal(barrier, inc=1, device_id=dev, device_id_type=MESH)
    for copy in loads:
        copy.wait()

    mine = pl.ds(pl.multiple_of(c * HALF, HALF), HALF)
    theirs = pl.ds(pl.multiple_of(other * HALF, HALF), HALF)
    own_rows = pl.ds(pl.multiple_of(c * 16, 16), 16)
    other_rows = pl.ds(pl.multiple_of(other * 16, 16), 16)
    for m, w in enumerate((tgw, onw)):
        wst[m] = w[:, theirs].astype(BF16)
        for p in range(3):
            off = (OFFSETS_T, OFFSETS)[m][p]
            cols = pl.ds(pl.multiple_of(c * HALF + off, 128), (WIDTHS_T, WIDTHS)[m][p])
            wb[m][p][y, x, z, own_rows, :] = w[:, cols].astype(BF16)

    row8 = lax.broadcasted_iota(jnp.int32, (PAIR, 128), 0)
    lane8 = lax.broadcasted_iota(jnp.int32, (PAIR, 128), 1)
    row_own = (row8[:, :T] // 4) == c

    def twice(v):
        return jnp.where(row_own, jnp.concatenate([v, v], axis=0), 0.0)

    pk_m[...] = jnp.zeros_like(pk_m)
    for slot, r in enumerate((step, rew, logp)):
        pk_m[slot, :, :T] = twice(r[...])
    pk_m[3, :, :T] = twice(rst[...].astype(F32))
    hz = jnp.zeros((PAIR, 128), F32)
    bz = jnp.zeros((PAIR, 128), F32)
    for i in range(4):
        sel = row8 == c * 4 + i
        hz = jnp.where(sel, hor[i].astype(F32), hz)
        bz = jnp.where(sel, burn[i].astype(F32), bz)
    pk_m[4] = hz
    pk_m[5] = bz

    pl.semaphore_wait(barrier, len(peers))

    def w_half(m, p):
        src, dst = wst.at[m, :, cols_of(p, m)], wb[m][p].at[y, x, z, own_rows, :]
        return remote(src, dst, d2d_ss.at[0], d2d_rs.at[m], partner)

    def w_half_in(m):
        remote(wst.at[m], wst.at[m], d2d_ss.at[0], d2d_rs.at[m], partner).wait_recv()

    def width(m, p):
        return (WIDTHS_T, WIDTHS)[m][p]

    def cols_of(p, m=1):
        return pl.ds((OFFSETS_T, OFFSETS)[m][p], width(m, p))

    for m in range(2):
        for p in range(3):
            w_half(m, p).start()
    send(pk_m, pk_i, d2d_ss.at[2], d2d_rs.at[2], partner)
    send(nxt, xr_n.at[own_half, :], d2d_ss.at[3], d2d_rs.at[3], partner)
    send(obs, xr_o.at[own_half, :], d2d_ss.at[4], d2d_rs.at[4], partner)

    def place(p, first, second, last):
        idx = dict(zip(ORDERS[p], (first, second, last)))
        return idx["y"], idx["x"], idx["z"]

    def turned(p, i, d):
        return lax.rem(at[ORDERS[p][i]] + d, 4)

    def toward(p, i, d, core=c):
        return device(core=core, **{ORDERS[p][i]: turned(p, i, d)})

    FULL = pl.ds(0, 4)

    def half_of(h):
        return FULL if h is None else pl.ds(2 * h, 2)

    def ag_copy(m, p, k, j, where, dev):
        ref = wb[m][p].at[where]
        n = m * 3 + p
        return remote(ref, ref, ag_ss.at[n * 3 + k], ag_rs.at[n * AG_SEMS + 3 * m + j], dev)

    def ag_end(m, p, l):
        return 7 + l if p == 2 else 7

    def ag_send(m, p, k, j, where, dev):
        ag_copy(m, p, k, j, where, dev).start()

    def ag_wait(m, p, j, where):
        ag_copy(m, p, 0, j, where, partner).wait_recv()

    def ag_drain(m, p):
        for k, where in enumerate(((0, 0, pl.ds(0, 3)), (0, pl.ds(0, 3)), (pl.ds(0, 3),))):
            ag_copy(m, p, k, 0, where, partner).wait_send()

    def line(p, second, last, h=None):
        return place(p, half_of(h), second, last)

    def ag_one(m, p):
        dst = wb[m][p].at[y, x, z, own_rows, :]
        sem, n = ag_ss.at[(m * 3 + p) * 3], (m * 3 + p) * AG_SEMS + 3 * m
        for d in (2, 1, 3):
            remote(dst, dst, sem, ag_rs.at[n], toward(p, 0, d)).start()
            src = wst.at[m, :, cols_of(p, m)]
            remote(src, dst, sem, ag_rs.at[n], toward(p, 0, d, other)).start()

    def ag_one_in(m, p):
        ag_wait(m, p, 0, (0, 0, pl.ds(0, 3)))

    def ag_own(m, p, k):
        for d in (1, 3, 2):
            where = place(p, turned(p, 0, d), turned(p, 1, 0), turned(p, 2, 0))
            ag_send(m, p, k, 2 * k - 1, where, toward(p, k, 1))
            ag_send(m, p, k, 2 * k - 1, where, toward(p, k, 3))

    def ag_early(m, p):
        for k in (1, 2):
            ag_send(m, p, k, 2 * k - 1, (y, x, z), toward(p, k, 1))
            ag_send(m, p, k, 2 * k - 1, (y, x, z), toward(p, k, 3))

    def ag_two_forward(m, p):
        q3 = turned(p, 2, 0)
        ag_wait(m, p, 1, (0, pl.ds(0, 2)))
        ag_send(m, p, 1, 2, line(p, turned(p, 1, 3), q3, 0), toward(p, 1, 1))
        ag_send(m, p, 1, 2, line(p, turned(p, 1, 1), q3, 1), toward(p, 1, 3))

    def ag_two_last(m, p):
        ag_wait(m, p, 2, line(p, turned(p, 1, 2), turned(p, 2, 0)))

    def ag_three(m, p, l):
        own = line(p, turned(p, 1, l), turned(p, 2, 0))
        ag_send(m, p, 2, 3 + l, own, toward(p, 2, 1))
        ag_send(m, p, 2, 3 + l, own, toward(p, 2, 3))

    def ag_three_forward(m, p, l):
        second = turned(p, 1, l)
        ag_wait(m, p, 3 + l, (0, pl.ds(0, 2)))
        end = ag_end(m, p, l)
        ag_send(m, p, 2, end, line(p, second, turned(p, 2, 3), 0), toward(p, 2, 1))
        ag_send(m, p, 2, end, line(p, second, turned(p, 2, 1), 1), toward(p, 2, 3))

    def ag_three_last(m, p):
        ag_wait(m, p, 7, place(p, FULL, FULL, turned(p, 2, 2)))

    def ag_line_last(m, l):
        ag_wait(m, 2, 7 + l, line(2, turned(2, 1, l), turned(2, 2, 2)))

    def wide(v, w=HALF):
        return jnp.concatenate([v] * (w // 128), axis=1)

    def at_t(t):
        return pl.ds(pl.multiple_of(t * PAIR, PAIR), PAIR)

    def spread_lanes(dst, v):
        for t in range(T):
            dst[pl.ds(t * PAIR, PAIR), :] = jnp.broadcast_to(v[:, t : t + 1], (PAIR, 128))

    r_out = lax.broadcasted_iota(jnp.int32, (ROWS, ROWS), 0)
    r_in = lax.broadcasted_iota(jnp.int32, (ROWS, ROWS), 1)

    def permutation():
        return jnp.where(r_out == (r_in % T) * PAIR + r_in // T, 1.0, 0.0).astype(BF16)

    def permute_next():
        perm = permutation()

        def body(i, _):
            cols = pl.ds(pl.multiple_of(i * 256, 256), 256)
            xp_n[:, cols] = jnp.dot(perm, xr_n[:, cols], preferred_element_type=F32).astype(BF16)
            return 0

        lax.fori_loop(0, D // 256, body, 0)

    def permute_obs(lo, hi):
        perm = permutation()

        def body(i, _):
            cols = pl.ds(pl.multiple_of(i * 256, 256), 256)
            v = jnp.dot(perm, xr_o[:, cols], preferred_element_type=F32)
            xp_o[:, cols] = v.astype(BF16)
            xt[i // 2, pl.ds(2 * (i % 2), 2)] = v.T.astype(BF16).reshape(2, 4, 32, ROWS)
            return 0

        lax.fori_loop(lo, hi, body, 0)

    def project_planes(m, p, planes, fresh):
        xp, v = (xp_n, vt) if m == 0 else (xp_o, vo)
        cols, w = cols_of(p, m), width(m, p)
        axis = 1 if p == 2 else 2
        qs = [turned(p, axis, d) for d in planes]

        def tile(i, _):
            rows = pl.ds(pl.multiple_of(i * PROJECTED, PROJECTED), PROJECTED)
            acc = None if fresh else v[rows, cols]
            for q in qs:
                where = place(p, FULL, q, FULL) if p == 2 else place(p, FULL, FULL, q)
                rhs = wb[m][p][where].reshape(512, w)
                if p == 1:
                    starts = [pl.multiple_of((k * 4 + q) * 128, 128) for k in range(4)]
                    lhs = jnp.concatenate([xp[rows, pl.ds(k, 128)] for k in starts], axis=1)
                else:
                    lhs = xp[rows, pl.ds(pl.multiple_of(q * 512, 512), 512)]
                part = jnp.dot(lhs, rhs, preferred_element_type=F32) * SCALE
                acc = part if acc is None else acc + part
            v[rows, cols] = acc
            return 0

        lax.fori_loop(0, ROWS // PROJECTED, tile, 0)

    def scan(m, v, p, ends):
        cols = cols_of(p, m)

        def body(i, st):
            steps = [at_t(i * 4 + k) for k in range(4)]
            added = [ss[rows, cols] * v[rows, cols] for rows in steps]
            kept = [cc[rows, cols] for rows in steps]
            states = []
            for f, u in zip(kept, added):
                st = f * st + u
                states.append(st)
            for rows, state in zip(steps, states):
                v[rows, cols] = state
            return st

        last = lax.fori_loop(0, T // 4, body, jnp.zeros((PAIR, width(m, p)), F32))
        ends[tm, :, cols] = last.astype(BF16)

    def ends_copy(n, ends, p, slots, dev):
        cols = pl.ds(0, HALF) if p is None else cols_of(p)
        ref = ends.at[slots, :, cols]
        return remote(ref, ref, pre_ss.at[n], pre_rs.at[n], dev)

    def prefix_send(n, ends, p, forward):
        for d in range(TM - 1, 0, -1):
            to = tm + d if forward else tm - d

            @pl.when(to < TM if forward else to >= 0)
            def _(to=to):
                ends_copy(n, ends, p, tm, {"tm": to, "batch": batch}).start()

    def prefix_wait(n, ends, p, count, arrived):
        for k in range(1, TM):

            @pl.when(count == k)
            def _(k=k):
                copies = ends_copy(n, ends, p, pl.ds(0, k), partner)
                copies.wait_recv() if arrived else copies.wait_send()

    def prefix_take(n, ends, p, forward):
        cols, w = (pl.ds(0, HALF), HALF) if p is None else (cols_of(p), WIDTHS[p])
        prefix_wait(n, ends, p, tm if forward else TM - 1 - tm, True)
        decay = dfor if forward else dback
        v = jnp.zeros((PAIR, w), F32)
        for j in range(TM - 1) if forward else range(TM - 1, 0, -1):
            counted = jnp.where(j < tm if forward else j > tm, 1.0, 0.0)
            v = decay[j, :, cols] * v + counted * ends[j, :, cols].astype(F32)
        carry[:, cols] = v

    def prefix_drain(n, ends, p, forward):
        prefix_wait(n, ends, p, TM - 1 - tm if forward else tm, False)

    def quality(m, v, heads, p, fresh, slope):
        cols, w = cols_of(p, m), width(m, p)
        hcols = pl.ds(pl.multiple_of(c * HALF + (OFFSETS_T, OFFSETS)[m][p], 128), w)
        h0 = jnp.broadcast_to(heads[0:1, hcols], (PAIR, w))
        h1 = jnp.broadcast_to(heads[1:2, hcols], (PAIR, w))
        start = carry[:, cols]

        def fold(u):
            out = u[:, :128]
            for i in range(1, w // 128):
                out = out + u[:, i * 128 : (i + 1) * 128]
            return out

        def body(i, _):
            steps = [at_t(i * 8 + k) for k in range(8)]
            states = [v[rows, cols] + pf[rows, cols] * start for rows in steps]
            before = None if fresh else [(qa0[rows, :], qa1[rows, :]) for rows in steps]
            out = []
            for st in states:
                sig = 1.0 / (1.0 + jnp.exp(-st))
                act = st * sig
                out.append((fold(act * h0), fold(act * h1), sig + act * (1.0 - sig)))
            for k, (rows, (f0, f1, rise)) in enumerate(zip(steps, out)):
                qa0[rows, :] = f0 if fresh else before[k][0] + f0
                qa1[rows, :] = f1 if fresh else before[k][1] + f1
                if slope:
                    v[rows, cols] = rise
            return 0

        lax.fori_loop(0, T // 8, body, 0)

    def quality_send(slot):
        def body(i, acc):
            a0, a1 = acc
            for k in range(16):
                rows = at_t(i * 16 + k)
                here = lane8 == i * 16 + k
                a0 = jnp.where(here, jnp.sum(qa0[rows, :], axis=1, keepdims=True), a0)
                a1 = jnp.where(here, jnp.sum(qa1[rows, :], axis=1, keepdims=True), a1)
            return a0, a1

        zero = jnp.zeros((PAIR, 128), F32)
        a0, a1 = lax.fori_loop(0, T // 16, body, (zero, zero))
        q_s[slot, 0] = a0
        q_s[slot, 1] = a1
        send(q_s.at[slot], q_r.at[slot], d2d_ss.at[5 + slot], d2d_rs.at[5 + slot], partner)

    def quality_sum(slot):
        remote(
            q_s.at[slot], q_r.at[slot], d2d_ss.at[5 + slot], d2d_rs.at[5 + slot], partner
        ).wait_recv()
        return [q_s[slot, k] + q_r[slot, k] for k in range(2)]

    for m in range(2):
        for p in range(3):
            ag_one(m, p)
    for m in range(2):
        w_half_in(m)
        for p in range(3):
            ag_early(m, p)
    for p in range(3):
        ag_one_in(0, p)
        ag_own(0, p, 1)
    for p in range(3):
        ag_own(0, p, 2)
    def clear(j, _):
        @pl.when(j > tm)
        def _():
            ends_t[j] = jnp.zeros((PAIR, HALF), BF16)
            ends_o[j] = jnp.zeros((PAIR, HALF), BF16)

        @pl.when(j < tm)
        def _():
            lv[j] = jnp.zeros((PAIR, HALF), BF16)

        return 0

    lax.fori_loop(0, TM, clear, 0)
    remote(pk_m, pk_i, d2d_ss.at[2], d2d_rs.at[2], partner).wait_recv()
    step8 = pk_m[0] + pk_i[0]
    rew8 = pk_m[1] + pk_i[1]
    logp8 = pk_m[2] + pk_i[2]
    rst8 = pk_m[3] + pk_i[3]
    keep8 = 1.0 - rst8
    hor8 = pk_m[4] + pk_i[4]
    burn8 = pk_m[5] + pk_i[5]

    sf[tm, 0] = jnp.broadcast_to(jnp.sum(step8, axis=1, keepdims=True), (PAIR, 128))
    sf[tm, 1] = jnp.broadcast_to(1.0 - jnp.max(rst8, axis=1, keepdims=True), (PAIR, 128))
    for d in range(1, TM):
        dev = {"tm": lax.rem(tm + d, TM), "batch": batch}
        remote(sf.at[tm], sf.at[tm], pre_ss.at[0], pre_rs.at[0], dev).start()

    nb_s[0] = rew8
    nb_s[1] = logp8
    nb_s[2] = keep8
    earlier = lax.rem(tm + TM - 1, TM)
    before = {"tm": earlier, "batch": batch}
    send(nb_s, nb_r, nb_sem.at[0], nb_sem.at[1], before)
    spread_lanes(bc0, step8)
    spread_lanes(bc1, keep8)
    ld8 = jnp.broadcast_to(ld[:, mine], (PAIR, HALF))

    def factors(t, prod):
        e = jnp.exp(wide(bc0[at_t(t), :]) * ld8)
        f = e * wide(bc1[at_t(t), :])
        cc[at_t(t), :] = f
        ss[at_t(t), :] = jnp.sqrt(1.0 - e * e)
        prod = prod * f
        pf[at_t(t), :] = prod
        return prod

    lax.fori_loop(0, T, factors, jnp.ones((PAIR, HALF), F32))
    for p in range(3):
        ag_one_in(1, p)
        ag_own(1, p, 1)
    for p in range(3):
        ag_two_forward(0, p)
        ag_three(0, p, 3)
        ag_three(0, p, 1)
    local[0].wait()
    remote(nxt, xr_n.at[other_half, :], d2d_ss.at[3], d2d_rs.at[3], partner).wait_recv()
    permute_next()
    for p in range(3):
        ag_three_forward(0, p, 0)
    local[1].wait()
    remote(obs, xr_o.at[other_half, :], d2d_ss.at[4], d2d_rs.at[4], partner).wait_recv()
    permute_obs(0, 8)
    for p in range(3):
        ag_two_last(0, p)
        ag_three(0, p, 2)
    for l in (3, 1):
        for p in range(3):
            ag_three_forward(0, p, l)
    for p in range(3):
        ag_two_forward(1, p)
        ag_own(1, p, 2)
    def tails(i, prod):
        t = T - 1 - i
        tp[at_t(t), :] = prod
        return prod * cc[at_t(t), :]

    lax.fori_loop(0, T, tails, jnp.ones((PAIR, HALF), F32))
    for p in range(3):
        ag_three_forward(0, p, 2)
        ag_three(1, p, 3)
        ag_three(1, p, 1)
    for p in (0, 1):
        project_planes(0, p, (0, 1, 3), True)
    for p in range(3):
        ag_two_last(1, p)
        ag_three(1, p, 2)
    sums = remote(
        sf.at[pl.ds(0, TM - 1)], sf.at[pl.ds(0, TM - 1)], pre_ss.at[0], pre_rs.at[0], partner
    )
    sums.wait_recv()

    def block_decay(j, _):
        v = jnp.exp(wide(sf[j, 0]) * ld8) * wide(sf[j, 1])
        dfor[j] = jnp.where(j < tm, v, 1.0)
        dback[j] = jnp.where(j > tm, v, 1.0)
        return 0

    lax.fori_loop(0, TM, block_decay, 0)
    for p in range(3):
        ag_three_forward(1, p, 0)
    for p in (0, 1, 2):
        if p == 2:
            for l in range(4):
                ag_line_last(0, l)
            project_planes(0, p, (0, 1, 3, 2), True)
        else:
            ag_three_last(0, p)
            project_planes(0, p, (2,), False)
        scan(0, vt, p, ends_t)
    prefix_send(1, ends_t, None, True)
    for p in range(3):
        ag_three_forward(1, p, 3)
    for p in range(3):
        ag_three_forward(1, p, 1)
    for p in (0, 1):
        project_planes(1, p, (0,), True)
    for p in range(3):
        ag_three_forward(1, p, 2)
    for p in (0, 1):
        project_planes(1, p, (1, 3), False)
    for l in (0, 3, 1):
        ag_line_last(1, l)
    project_planes(1, 2, (0, 1, 3), True)
    ag_three_last(1, 0)
    project_planes(1, 0, (2,), False)
    scan(1, vo, PARTS[0], ends_o)
    prefix_send(2 + PARTS[0], ends_o, PARTS[0], True)
    ag_line_last(1, 2)
    project_planes(1, 2, (2,), False)
    scan(1, vo, PARTS[1], ends_o)
    prefix_send(2 + PARTS[1], ends_o, PARTS[1], True)
    ag_three_last(1, 1)
    project_planes(1, 1, (2,), False)
    scan(1, vo, PARTS[2], ends_o)
    prefix_send(2 + PARTS[2], ends_o, PARTS[2], True)
    prefix_take(1, ends_t, None, True)
    for p in PARTS:
        quality(0, vt, tgh, p, p == PARTS[0], False)
    quality_send(0)
    for core in range(2):
        dev = {"tm": earlier, "batch": z * 2 + core}
        remote(q_s.at[0], q_n.at[c], nb_sem.at[2], nb_sem.at[3], dev).start()
    prefix_take(2 + PARTS[0], ends_o, PARTS[0], True)
    quality(1, vo, onh, PARTS[0], True, True)

    for p in PARTS[1:]:
        prefix_take(2 + p, ends_o, p, True)
        quality(1, vo, onh, p, False, True)
    quality_send(1)
    def value_of(products, log_prob):
        tq = [v * (H ** (-0.5)) for v in products]
        return jnp.minimum(tq[0], tq[1]) - ENTROPY_COEFF * log_prob

    value8 = value_of(quality_sum(0), logp8)
    remote(nb_s, nb_r, nb_sem.at[0], nb_sem.at[1], before).wait_recv()
    later_q = remote(q_n, q_n, nb_sem.at[2], nb_sem.at[3], before)
    later_q.wait_recv()
    later_value = value_of([q_n[0, k] + q_n[1, k] for k in range(2)], nb_r[1])
    inside = (lane8 >= T) & (lane8 < T + NMAX) & (tm < TM - 1)

    def extended(own, later):
        later = jnp.where(inside, pltpu.roll(later, T, 1), 0.0)
        return jnp.where(lane8 < T, own, later)

    ext_r, ext_v = extended(rew8, nb_r[0]), extended(value8, later_value)
    ext_k = extended(keep8, nb_r[2])

    def shifted(v, n):
        return v if n == 0 else pltpu.roll(v, 128 - n, 1)

    total = jnp.zeros((PAIR, 128), F32)
    alive = jnp.ones((PAIR, 128), F32)
    for n in range(NMAX):
        total = total + jnp.where(hor8 > n, DISCOUNT**n * alive * shifted(ext_r, n), 0.0)
        alive = alive * shifted(ext_k, n + 1)
        total = total + jnp.where(
            hor8 == n + 1, DISCOUNT ** (n + 1) * alive * shifted(ext_v, n + 1), 0.0
        )
    ret[...] = jnp.where(c == 0, total[:4, :T], total[4:, :T])
    weight = jnp.where((lane8 + tm * T).astype(F32) >= burn8, 1.0, 0.0)

    oq = quality_sum(1)
    spread_lanes(bc0, weight * (oq[0] * (H ** (-0.5)) - total) * (H ** (-0.5)))
    spread_lanes(bc1, weight * (oq[1] * (H ** (-0.5)) - total) * (H ** (-0.5)))

    h0 = jnp.broadcast_to(onh[0:1, mine], (PAIR, HALF))
    h1 = jnp.broadcast_to(onh[1:2, mine], (PAIR, HALF))

    def back(i, adj):
        for k in range(4):
            rows = at_t(T - 1 - (i * 4 + k))
            dh = wide(bc0[rows, :]) * h0 + wide(bc1[rows, :]) * h1
            adj = dh * vo[rows, :] + adj
            vo[rows, :] = adj
            adj = cc[rows, :] * adj
        return adj

    leaving = lax.fori_loop(0, T // 4, back, jnp.zeros((PAIR, HALF), F32))
    lv[tm] = leaving.astype(BF16)
    prefix_send(5, lv, None, False)

    def finish(p):
        cols = cols_of(p)
        incoming = carry[:, cols]
        both = jnp.concatenate([incoming, incoming], axis=0)

        def body(i, _):
            for k in range(4):
                rows = pl.ds(pl.multiple_of(i * 64 + k * 16, 16), 16)
                adj = vo[rows, cols] + tp[rows, cols] * both
                du[rows, cols] = (ss[rows, cols] * adj).astype(BF16)
            return 0

        lax.fori_loop(0, ROWS // 64, body, 0)

    def gradient(p, l):
        where = place(p, FULL, turned(p, 1, l), FULL)
        lhs = xt[where].reshape(512, ROWS)
        v = jnp.dot(lhs, du[:, cols_of(p)], preferred_element_type=F32)
        gg[p][where] = v.reshape(4, 4, 32, WIDTHS[p])

    def rs_copy(p, k, j, src, dst, dev):
        return remote(src, dst, rs_ss.at[p * 3 + k], rs_rs.at[p * RS_SEMS + j], dev)

    def rs_half(p, s, h, dev):
        return rs_copy(p, 0, s, snd_h[p].at[s, h], rcv_h[p].at[s, h], dev)

    def rs_whole(p, s, h, dev):
        return rs_copy(p, 1, 5 + s, snd_w[p].at[s, h], rcv_w[p].at[s, h], dev)

    def rs_drain(p):
        for k, (src, dst) in enumerate(
            ((snd_h[p], rcv_h[p]), (snd_w[p], rcv_w[p]), (snd_b[p], rcv_b[p]))
        ):
            rs_copy(p, k, 0, src, dst, partner).wait_send()

    def rs_ref(p, s, d, h=None):
        if s < 4:
            return line(p, turned(p, 1, s), turned(p, 2, d), h)
        return line(p, turned(p, 1, d), turned(p, 2, 0), h)

    def rs_axis(s):
        return 2 if s < 4 else 1

    def rs_opposite(p, s):
        for h, d in ((0, 3), (1, 1)):
            snd_h[p][s, h] = gg[p][rs_ref(p, s, 2, h)].astype(BF16)
            rs_half(p, s, h, toward(p, rs_axis(s), d)).start()

    def rs_arrived(p, s):
        rs_copy(p, 0, s, snd_h[p].at[s], rcv_h[p].at[s], partner).wait_recv()

    def rs_neighbour(p, s, h):
        d = (3, 1)[h]
        with_recv = gg[p][rs_ref(p, s, d, h)] + rcv_h[p][s, h].astype(F32)
        snd_w[p][s, h, pl.ds(2 * h, 2)] = with_recv.astype(BF16)
        snd_w[p][s, h, pl.ds(2 - 2 * h, 2)] = gg[p][rs_ref(p, s, d, 1 - h)].astype(BF16)
        rs_whole(p, s, h, toward(p, rs_axis(s), d)).start()

    def rs_neighbours(p, s):
        rs_arrived(p, s)
        rs_neighbour(p, s, 0)
        rs_neighbour(p, s, 1)

    def rs_sum(p, s):
        rs_copy(p, 1, 5 + s, snd_w[p].at[s], rcv_w[p].at[s], partner).wait_recv()
        own = rs_ref(p, s, 0)
        both = rcv_w[p][s, 0].astype(F32) + rcv_w[p][s, 1].astype(F32)
        gg[p][own] = gg[p][own] + both

    def rs_one(p):
        for d in (2, 1, 3):
            where = place(p, turned(p, 0, d), turned(p, 1, 0), turned(p, 2, 0))
            for core in range(2):
                block = gg[p][(*where, pl.ds(16 * core, 16))]
                snd_b[p][core, d - 1] = block.astype(BF16)
                rs_copy(
                    p, 2, 10, snd_b[p].at[core, d - 1], rcv_b[p].at[c, d - 1],
                    toward(p, 0, d, core),
                ).start()
        gx_s[:, cols_of(p)] = gg[p][y, x, z, other_rows, :]

    prefix_take(5, lv, None, False)
    for p in RS_PARTS:
        finish(p)
        gradient(p, LINES[0])
        rs_opposite(p, LINES[0])
    for p in RS_PARTS:
        gradient(p, LINES[1])
        rs_opposite(p, LINES[1])
    for p in RS_PARTS:
        rs_neighbours(p, LINES[0])
        gradient(p, LINES[2])
        rs_opposite(p, LINES[2])
    for p in RS_PARTS:
        rs_neighbours(p, LINES[1])
        gradient(p, LINES[3])
        rs_opposite(p, LINES[3])
    for p in RS_PARTS:
        rs_sum(p, LINES[0])
        rs_opposite(p, 4)
    for p in RS_PARTS:
        rs_neighbours(p, LINES[2])
    for p in RS_PARTS:
        rs_sum(p, LINES[1])
        rs_arrived(p, 4)
        rs_neighbour(p, 4, 0)
    for p in RS_PARTS:
        rs_neighbours(p, LINES[3])
    for p in RS_PARTS:
        rs_sum(p, LINES[2])
        rs_neighbour(p, 4, 1)
    prefix_drain(1, ends_t, None, True)
    for p in range(3):
        prefix_drain(2 + p, ends_o, p, True)
        ag_drain(0, p)
        ag_drain(1, p)
    prefix_drain(5, lv, None, False)
    remote(wst, wst, d2d_ss.at[0], d2d_rs.at[0], partner).wait_send()
    sums.wait_send()
    later_q.wait_send()
    for copy in pending:
        copy.wait_send()
    pending.clear()
    for p in RS_PARTS:
        rs_sum(p, LINES[3])
    for p in RS_PARTS:
        rs_sum(p, 4)
        rs_one(p)
    send(gx_s, gx_r, d2d_ss.at[7], d2d_rs.at[7], partner)
    remote(gx_s, gx_r, d2d_ss.at[7], d2d_rs.at[7], partner).wait_recv()
    for p in range(3):
        rs_copy(p, 2, 10, snd_b[p], rcv_b[p], partner).wait_recv()
        for core, v in (
            (c, gg[p][y, x, z, own_rows, :]), (other, gx_r[:, cols_of(p)]),
        ):
            for d in range(3):
                v = v + rcv_b[p][core, d].astype(F32)
            cols = pl.ds(pl.multiple_of(core * HALF + OFFSETS[p], 128), WIDTHS[p])
            gw[:, cols] = v

    for p in range(3):
        rs_drain(p)
    for copy in pending:
        copy.wait_send()


def update(grad, returns, onw, tgw, grad_w, new_target, returns_out):
    g = grad[...] * SCALE
    grad_w[...] = g
    new_target[...] = (1.0 - POLYAK_RATE) * tgw[...] + POLYAK_RATE * (onw[...] - STEP_SIZE * g)
    returns_out[...] = returns[...]


def shards(
    obs_feats, next_feats, online_w, target_w, log_decay, step_scale, online_heads, target_heads,
    reward, next_action_log_prob, resets, horizon, burn_in,
):
    vmem = pl.BlockSpec(memory_space=pltpu.VMEM)
    smem = pl.BlockSpec(memory_space=pltpu.SMEM)
    hbm = pl.BlockSpec(memory_space=pltpu.HBM)
    small = (
        online_w, target_w, log_decay[None], step_scale, online_heads, target_heads,
        reward, next_action_log_prob, resets,
    )
    weights = [pltpu.VMEM((4, 4, 4, 32, w), BF16) for w in WIDTHS_T + WIDTHS]
    staged = [
        *[pltpu.VMEM((5, 2, 2, 32, w), BF16) for w in WIDTHS],
        *[pltpu.VMEM((5, 2, 4, 32, w), BF16) for w in WIDTHS],
        *[pltpu.VMEM((2, 3, 16, w), BF16) for w in WIDTHS],
    ]
    big = pltpu.VMEM((ROWS, HALF), F32)
    table = pltpu.VMEM((TM, PAIR, HALF), F32)
    ends = pltpu.VMEM((TM, PAIR, HALF), BF16)
    narrow = pltpu.VMEM((ROWS, 128), F32)
    scratch = [
        *[pltpu.VMEM(a.shape, a.dtype) for a in small],
        pltpu.VMEM((ROWS, D), BF16), pltpu.VMEM((ROWS, D), BF16),
        pltpu.VMEM((ROWS, D), BF16), pltpu.VMEM((ROWS, D), BF16),
        pltpu.VMEM((4, 4, 4, 32, ROWS), BF16), pltpu.VMEM((2, 16, HALF), BF16),
        *weights,
        pltpu.VMEM((6, PAIR, 128), F32), pltpu.VMEM((6, PAIR, 128), F32),
        narrow, narrow, narrow, narrow,
        big, big, big, big, big, big,
        pltpu.VMEM((TM, 2, PAIR, 128), F32), table, table, ends, ends, ends,
        pltpu.VMEM((PAIR, HALF), F32),
        pltpu.VMEM((2, 2, PAIR, 128), F32), pltpu.VMEM((2, 2, PAIR, 128), F32),
        pltpu.VMEM((2, 2, PAIR, 128), F32),
        pltpu.VMEM((3, PAIR, 128), F32), pltpu.VMEM((3, PAIR, 128), F32),
        pltpu.VMEM((ROWS, HALF), BF16),
        *[pltpu.VMEM((4, 4, 4, 32, w), F32) for w in WIDTHS],
        *staged, *staged,
        pltpu.VMEM((16, HALF), F32), pltpu.VMEM((16, HALF), F32),
        pltpu.SemaphoreType.DMA((18,)), pltpu.SemaphoreType.DMA((6 * AG_SEMS + 6,)),
        pltpu.SemaphoreType.DMA((9,)), pltpu.SemaphoreType.DMA((3 * RS_SEMS,)),
        pltpu.SemaphoreType.DMA((6,)), pltpu.SemaphoreType.DMA((6,)),
        pltpu.SemaphoreType.DMA((2,)), pltpu.SemaphoreType.DMA((9,)),
        pltpu.SemaphoreType.DMA((8,)), pltpu.SemaphoreType.DMA((8,)),
        pltpu.SemaphoreType.DMA((4,)),
    ]
    rows_b, span, width = obs_feats.shape
    grad, returns = pl.pallas_call(
        kernel,
        name="critic_step",
        out_shape=(
            jax.ShapeDtypeStruct(online_w.shape, F32),
            jax.ShapeDtypeStruct(reward.shape, F32),
        ),
        in_specs=[hbm] * 11 + [smem] * 2,
        out_specs=(vmem, vmem),
        scratch_shapes=scratch,
        compiler_params=pltpu.CompilerParams(
            collective_id=0, has_side_effects=True, vmem_limit_bytes=VMEM_LIMIT * 1024 * 1024
        ),
    )(
        obs_feats.reshape(rows_b * span, width), next_feats.reshape(rows_b * span, width),
        *small, horizon, burn_in,
    )
    return pl.pallas_call(
        update,
        name="target_update",
        out_shape=(
            jax.ShapeDtypeStruct(online_w.shape, F32),
            jax.ShapeDtypeStruct(target_w.shape, F32),
            jax.ShapeDtypeStruct(reward.shape, F32),
        ),
        in_specs=[vmem] * 4,
        out_specs=(vmem, vmem, vmem),
    )(grad, returns, online_w, target_w)


def solution(mesh):
    return jax.shard_map(
        shards,
        mesh=mesh,
        in_specs=(
            P("batch", "tm", None), P("batch", "tm", None),
            P(("tm", "batch"), None), P(("tm", "batch"), None),
            P(), P("batch", "tm"), P(), P(),
            P("batch", "tm"), P("batch", "tm"), P("batch", "tm"), P("batch"), P("batch"),
        ),
        out_specs=(P(("tm", "batch"), None), P(("tm", "batch"), None), P("batch", "tm")),
        check_vma=False,
    )
```

```python
import jax
import jax.numpy as jnp
from jax import lax
from jax.experimental import pallas as pl
from jax.experimental.pallas import tpu as pltpu
from jax.sharding import PartitionSpec as P

NMAX = 8
DISCOUNT = 0.99
ENTROPY_COEFF = 0.2
POLYAK_RATE = 0.005
STEP_SIZE = 0.1

F32 = jnp.float32
BF16 = jnp.bfloat16
MESH = pl.DeviceIdType.MESH

D = 2048
H = 2048
HALF = H // 2
T = 64
PAIR = 8
ROWS = T * PAIR
TM = 16
VMEM_LIMIT = 56
SCALE = D ** (-0.5)

WIDTHS_T = (256, 384, 384)
OFFSETS_T = (0, 256, 640)
WIDTHS = (384, 256, 384)
OFFSETS = (0, 384, 640)
ORDERS = (("z", "x", "y"), ("y", "z", "x"), ("x", "y", "z"))
PARTS = (1, 0, 2)
RS_PARTS = (2, 0, 1)
PROJECTED = 512
AG_SEMS = 8
RS_SEMS = 11
LINES = (2, 3, 1, 0)


def kernel(
    obs, nxt, onw_in, tgw_in, ld_in, step_in, onh_in, tgh_in, rew_in, logp_in, rst_in, hor, burn,
    gw, ret,
    onw, tgw, ld, step, onh, tgh, rew, logp, rst,
    xr_o, xr_n, xp_o, xp_n, xt, wst,
    wt0, wt1, wt2, wo0, wo1, wo2,
    pk_m, pk_i, bc0, bc1, qa0, qa1, cc, ss, pf, tp, vt, vo,
    sf, dfor, dback, ends_t, ends_o, lv, carry,
    q_s, q_r, q_n, nb_s, nb_r, du,
    g0, g1, g2,
    sh0, sh1, sh2, sw0, sw1, sw2, sb0, sb1, sb2,
    rh0, rh1, rh2, rw0, rw1, rw2, rb0, rb1, rb2,
    gx_s, gx_r,
    ag_ss, ag_rs, rs_ss, rs_rs, pre_ss, pre_rs, loc_sem, in_sem, d2d_ss, d2d_rs, nb_sem,
):
    tm = lax.axis_index("tm")
    batch = lax.axis_index("batch")
    y, x = tm // 4, tm % 4
    z, c = batch // 2, batch % 2
    at = {"y": y, "x": x, "z": z}
    other = 1 - c
    wb = ((wt0, wt1, wt2), (wo0, wo1, wo2))
    gg = (g0, g1, g2)
    snd_h, snd_w, snd_b = (sh0, sh1, sh2), (sw0, sw1, sw2), (sb0, sb1, sb2)
    rcv_h, rcv_w, rcv_b = (rh0, rh1, rh2), (rw0, rw1, rw2), (rb0, rb1, rb2)
    pending = []

    def device(core=c, **moved):
        here = {**at, **moved}
        return {"tm": here["y"] * 4 + here["x"], "batch": here["z"] * 2 + core}

    partner = {"tm": tm, "batch": z * 2 + other}

    def remote(src, dst, ss_, rs_, dev):
        return pltpu.make_async_remote_copy(
            src_ref=src, dst_ref=dst, send_sem=ss_, recv_sem=rs_, device_id=dev,
            device_id_type=MESH,
        )

    def send(src, dst, ss_, rs_, dev):
        copy = remote(src, dst, ss_, rs_, dev)
        copy.start()
        pending.append(copy)

    own_half = pl.ds(pl.multiple_of(c * 256, 256), 256)
    other_half = pl.ds(pl.multiple_of(other * 256, 256), 256)
    loads = [
        pltpu.make_async_copy(src, dst, in_sem.at[i])
        for i, (src, dst) in enumerate((
            (tgw_in, tgw), (onw_in, onw), (step_in, step), (rew_in, rew), (logp_in, logp),
            (rst_in, rst), (ld_in, ld), (onh_in, onh), (tgh_in, tgh),
        ))
    ]
    local = [
        pltpu.make_async_copy(nxt, xr_n.at[own_half, :], loc_sem.at[0]),
        pltpu.make_async_copy(obs, xr_o.at[own_half, :], loc_sem.at[1]),
    ]
    for copy in loads + local:
        copy.start()
    barrier = pltpu.get_barrier_semaphore()
    peers = [partner] + [device(z=lax.rem(z + d, 4)) for d in range(1, 4)]
    for a in "yxz":
        peers += [device(core=other, **{a: lax.rem(at[a] + d, 4)}) for d in range(1, 4)]
    peers += [{"tm": lax.rem(tm + d, TM), "batch": batch} for d in range(1, TM)]
    peers += [{"tm": lax.rem(tm + d, TM), "batch": z * 2 + other} for d in (1, TM - 1)]
    for dev in peers:
        pl.semaphore_signal(barrier, inc=1, device_id=dev, device_id_type=MESH)
    for copy in loads:
        copy.wait()

    mine = pl.ds(pl.multiple_of(c * HALF, HALF), HALF)
    theirs = pl.ds(pl.multiple_of(other * HALF, HALF), HALF)
    own_rows = pl.ds(pl.multiple_of(c * 16, 16), 16)
    other_rows = pl.ds(pl.multiple_of(other * 16, 16), 16)
    for m, w in enumerate((tgw, onw)):
        wst[m] = w[:, theirs].astype(BF16)
        for p in range(3):
            off = (OFFSETS_T, OFFSETS)[m][p]
            cols = pl.ds(pl.multiple_of(c * HALF + off, 128), (WIDTHS_T, WIDTHS)[m][p])
            wb[m][p][y, x, z, own_rows, :] = w[:, cols].astype(BF16)

    row8 = lax.broadcasted_iota(jnp.int32, (PAIR, 128), 0)
    lane8 = lax.broadcasted_iota(jnp.int32, (PAIR, 128), 1)
    row_own = (row8[:, :T] // 4) == c

    def twice(v):
        return jnp.where(row_own, jnp.concatenate([v, v], axis=0), 0.0)

    pk_m[...] = jnp.zeros_like(pk_m)
    for slot, r in enumerate((step, rew, logp)):
        pk_m[slot, :, :T] = twice(r[...])
    pk_m[3, :, :T] = twice(rst[...].astype(F32))
    hz = jnp.zeros((PAIR, 128), F32)
    bz = jnp.zeros((PAIR, 128), F32)
    for i in range(4):
        sel = row8 == c * 4 + i
        hz = jnp.where(sel, hor[i].astype(F32), hz)
        bz = jnp.where(sel, burn[i].astype(F32), bz)
    pk_m[4] = hz
    pk_m[5] = bz

    pl.semaphore_wait(barrier, len(peers))

    def w_half(m, p):
        src, dst = wst.at[m, :, cols_of(p, m)], wb[m][p].at[y, x, z, own_rows, :]
        return remote(src, dst, d2d_ss.at[0], d2d_rs.at[m], partner)

    def w_half_in(m):
        remote(wst.at[m], wst.at[m], d2d_ss.at[0], d2d_rs.at[m], partner).wait_recv()

    def width(m, p):
        return (WIDTHS_T, WIDTHS)[m][p]

    def cols_of(p, m=1):
        return pl.ds((OFFSETS_T, OFFSETS)[m][p], width(m, p))

    for m in range(2):
        for p in range(3):
            w_half(m, p).start()
    send(pk_m, pk_i, d2d_ss.at[2], d2d_rs.at[2], partner)
    send(nxt, xr_n.at[own_half, :], d2d_ss.at[3], d2d_rs.at[3], partner)
    send(obs, xr_o.at[own_half, :], d2d_ss.at[4], d2d_rs.at[4], partner)

    def place(p, first, second, last):
        idx = dict(zip(ORDERS[p], (first, second, last)))
        return idx["y"], idx["x"], idx["z"]

    def turned(p, i, d):
        return lax.rem(at[ORDERS[p][i]] + d, 4)

    def toward(p, i, d, core=c):
        return device(core=core, **{ORDERS[p][i]: turned(p, i, d)})

    FULL = pl.ds(0, 4)

    def half_of(h):
        return FULL if h is None else pl.ds(2 * h, 2)

    def ag_copy(m, p, k, j, where, dev):
        ref = wb[m][p].at[where]
        n = m * 3 + p
        return remote(ref, ref, ag_ss.at[n * 3 + k], ag_rs.at[n * AG_SEMS + 3 * m + j], dev)

    def ag_end(m, p, l):
        return 7 + l if p == 2 else 7

    def ag_send(m, p, k, j, where, dev):
        ag_copy(m, p, k, j, where, dev).start()

    def ag_wait(m, p, j, where):
        ag_copy(m, p, 0, j, where, partner).wait_recv()

    def ag_drain(m, p):
        for k, where in enumerate(((0, 0, pl.ds(0, 3)), (0, pl.ds(0, 3)), (pl.ds(0, 3),))):
            ag_copy(m, p, k, 0, where, partner).wait_send()

    def line(p, second, last, h=None):
        return place(p, half_of(h), second, last)

    def ag_one(m, p):
        dst = wb[m][p].at[y, x, z, own_rows, :]
        sem, n = ag_ss.at[(m * 3 + p) * 3], (m * 3 + p) * AG_SEMS + 3 * m
        for d in (2, 1, 3):
            remote(dst, dst, sem, ag_rs.at[n], toward(p, 0, d)).start()
            src = wst.at[m, :, cols_of(p, m)]
            remote(src, dst, sem, ag_rs.at[n], toward(p, 0, d, other)).start()

    def ag_one_in(m, p):
        ag_wait(m, p, 0, (0, 0, pl.ds(0, 3)))

    def ag_own(m, p, k):
        for d in (1, 3, 2):
            where = place(p, turned(p, 0, d), turned(p, 1, 0), turned(p, 2, 0))
            ag_send(m, p, k, 2 * k - 1, where, toward(p, k, 1))
            ag_send(m, p, k, 2 * k - 1, where, toward(p, k, 3))

    def ag_early(m, p):
        for k in (1, 2):
            ag_send(m, p, k, 2 * k - 1, (y, x, z), toward(p, k, 1))
            ag_send(m, p, k, 2 * k - 1, (y, x, z), toward(p, k, 3))

    def ag_two_forward(m, p):
        q3 = turned(p, 2, 0)
        ag_wait(m, p, 1, (0, pl.ds(0, 2)))
        ag_send(m, p, 1, 2, line(p, turned(p, 1, 3), q3, 0), toward(p, 1, 1))
        ag_send(m, p, 1, 2, line(p, turned(p, 1, 1), q3, 1), toward(p, 1, 3))

    def ag_two_last(m, p):
        ag_wait(m, p, 2, line(p, turned(p, 1, 2), turned(p, 2, 0)))

    def ag_three(m, p, l):
        own = line(p, turned(p, 1, l), turned(p, 2, 0))
        ag_send(m, p, 2, 3 + l, own, toward(p, 2, 1))
        ag_send(m, p, 2, 3 + l, own, toward(p, 2, 3))

    def ag_three_forward(m, p, l):
        second = turned(p, 1, l)
        ag_wait(m, p, 3 + l, (0, pl.ds(0, 2)))
        end = ag_end(m, p, l)
        ag_send(m, p, 2, end, line(p, second, turned(p, 2, 3), 0), toward(p, 2, 1))
        ag_send(m, p, 2, end, line(p, second, turned(p, 2, 1), 1), toward(p, 2, 3))

    def ag_three_last(m, p):
        ag_wait(m, p, 7, place(p, FULL, FULL, turned(p, 2, 2)))

    def ag_line_last(m, l):
        ag_wait(m, 2, 7 + l, line(2, turned(2, 1, l), turned(2, 2, 2)))

    def wide(v, w=HALF):
        return jnp.concatenate([v] * (w // 128), axis=1)

    def at_t(t):
        return pl.ds(pl.multiple_of(t * PAIR, PAIR), PAIR)

    def spread_lanes(dst, v):
        for t in range(T):
            dst[pl.ds(t * PAIR, PAIR), :] = jnp.broadcast_to(v[:, t : t + 1], (PAIR, 128))

    r_out = lax.broadcasted_iota(jnp.int32, (ROWS, ROWS), 0)
    r_in = lax.broadcasted_iota(jnp.int32, (ROWS, ROWS), 1)

    def permutation():
        return jnp.where(r_out == (r_in % T) * PAIR + r_in // T, 1.0, 0.0).astype(BF16)

    def permute_next():
        perm = permutation()

        def body(i, _):
            cols = pl.ds(pl.multiple_of(i * 256, 256), 256)
            xp_n[:, cols] = jnp.dot(perm, xr_n[:, cols], preferred_element_type=F32).astype(BF16)
            return 0

        lax.fori_loop(0, D // 256, body, 0)

    def permute_obs(lo, hi):
        perm = permutation()

        def body(i, _):
            cols = pl.ds(pl.multiple_of(i * 256, 256), 256)
            v = jnp.dot(perm, xr_o[:, cols], preferred_element_type=F32)
            xp_o[:, cols] = v.astype(BF16)
            xt[i // 2, pl.ds(2 * (i % 2), 2)] = v.T.astype(BF16).reshape(2, 4, 32, ROWS)
            return 0

        lax.fori_loop(lo, hi, body, 0)

    def project_planes(m, p, planes, fresh):
        xp, v = (xp_n, vt) if m == 0 else (xp_o, vo)
        cols, w = cols_of(p, m), width(m, p)
        axis = 1 if p == 2 else 2
        qs = [turned(p, axis, d) for d in planes]

        def tile(i, _):
            rows = pl.ds(pl.multiple_of(i * PROJECTED, PROJECTED), PROJECTED)
            acc = None if fresh else v[rows, cols]
            for q in qs:
                where = place(p, FULL, q, FULL) if p == 2 else place(p, FULL, FULL, q)
                rhs = wb[m][p][where].reshape(512, w)
                if p == 1:
                    starts = [pl.multiple_of((k * 4 + q) * 128, 128) for k in range(4)]
                    lhs = jnp.concatenate([xp[rows, pl.ds(k, 128)] for k in starts], axis=1)
                else:
                    lhs = xp[rows, pl.ds(pl.multiple_of(q * 512, 512), 512)]
                part = jnp.dot(lhs, rhs, preferred_element_type=F32) * SCALE
                acc = part if acc is None else acc + part
            v[rows, cols] = acc
            return 0

        lax.fori_loop(0, ROWS // PROJECTED, tile, 0)

    def scan(m, v, p, ends):
        cols = cols_of(p, m)

        def body(i, st):
            steps = [at_t(i * 4 + k) for k in range(4)]
            added = [ss[rows, cols] * v[rows, cols] for rows in steps]
            kept = [cc[rows, cols] for rows in steps]
            states = []
            for f, u in zip(kept, added):
                st = f * st + u
                states.append(st)
            for rows, state in zip(steps, states):
                v[rows, cols] = state
            return st

        last = lax.fori_loop(0, T // 4, body, jnp.zeros((PAIR, width(m, p)), F32))
        ends[tm, :, cols] = last.astype(BF16)

    def ends_copy(n, ends, p, slots, dev):
        cols = pl.ds(0, HALF) if p is None else cols_of(p)
        ref = ends.at[slots, :, cols]
        return remote(ref, ref, pre_ss.at[n], pre_rs.at[n], dev)

    def prefix_send(n, ends, p, forward):
        for d in range(TM - 1, 0, -1):
            to = tm + d if forward else tm - d

            @pl.when(to < TM if forward else to >= 0)
            def _(to=to):
                ends_copy(n, ends, p, tm, {"tm": to, "batch": batch}).start()

    def prefix_wait(n, ends, p, count, arrived):
        for k in range(1, TM):

            @pl.when(count == k)
            def _(k=k):
                copies = ends_copy(n, ends, p, pl.ds(0, k), partner)
                copies.wait_recv() if arrived else copies.wait_send()

    def prefix_take(n, ends, p, forward):
        cols, w = (pl.ds(0, HALF), HALF) if p is None else (cols_of(p), WIDTHS[p])
        prefix_wait(n, ends, p, tm if forward else TM - 1 - tm, True)
        decay = dfor if forward else dback
        v = jnp.zeros((PAIR, w), F32)
        for j in range(TM - 1) if forward else range(TM - 1, 0, -1):
            counted = jnp.where(j < tm if forward else j > tm, 1.0, 0.0)
            v = decay[j, :, cols] * v + counted * ends[j, :, cols].astype(F32)
        carry[:, cols] = v

    def prefix_drain(n, ends, p, forward):
        prefix_wait(n, ends, p, TM - 1 - tm if forward else tm, False)

    def quality(m, v, heads, p, fresh, slope):
        cols, w = cols_of(p, m), width(m, p)
        hcols = pl.ds(pl.multiple_of(c * HALF + (OFFSETS_T, OFFSETS)[m][p], 128), w)
        h0 = jnp.broadcast_to(heads[0:1, hcols], (PAIR, w))
        h1 = jnp.broadcast_to(heads[1:2, hcols], (PAIR, w))
        start = carry[:, cols]

        def fold(u):
            out = u[:, :128]
            for i in range(1, w // 128):
                out = out + u[:, i * 128 : (i + 1) * 128]
            return out

        def body(i, _):
            steps = [at_t(i * 8 + k) for k in range(8)]
            states = [v[rows, cols] + pf[rows, cols] * start for rows in steps]
            before = None if fresh else [(qa0[rows, :], qa1[rows, :]) for rows in steps]
            out = []
            for st in states:
                sig = 1.0 / (1.0 + jnp.exp(-st))
                act = st * sig
                out.append((fold(act * h0), fold(act * h1), sig + act * (1.0 - sig)))
            for k, (rows, (f0, f1, rise)) in enumerate(zip(steps, out)):
                qa0[rows, :] = f0 if fresh else before[k][0] + f0
                qa1[rows, :] = f1 if fresh else before[k][1] + f1
                if slope:
                    v[rows, cols] = rise
            return 0

        lax.fori_loop(0, T // 8, body, 0)

    def quality_send(slot):
        def body(i, acc):
            a0, a1 = acc
            for k in range(16):
                rows = at_t(i * 16 + k)
                here = lane8 == i * 16 + k
                a0 = jnp.where(here, jnp.sum(qa0[rows, :], axis=1, keepdims=True), a0)
                a1 = jnp.where(here, jnp.sum(qa1[rows, :], axis=1, keepdims=True), a1)
            return a0, a1

        zero = jnp.zeros((PAIR, 128), F32)
        a0, a1 = lax.fori_loop(0, T // 16, body, (zero, zero))
        q_s[slot, 0] = a0
        q_s[slot, 1] = a1
        send(q_s.at[slot], q_r.at[slot], d2d_ss.at[5 + slot], d2d_rs.at[5 + slot], partner)

    def quality_sum(slot):
        remote(
            q_s.at[slot], q_r.at[slot], d2d_ss.at[5 + slot], d2d_rs.at[5 + slot], partner
        ).wait_recv()
        return [q_s[slot, k] + q_r[slot, k] for k in range(2)]

    for m in range(2):
        for p in range(3):
            ag_one(m, p)
    for m in range(2):
        w_half_in(m)
        for p in range(3):
            ag_early(m, p)
    for p in range(3):
        ag_one_in(0, p)
        ag_own(0, p, 1)
    for p in range(3):
        ag_own(0, p, 2)
    def clear(j, _):
        @pl.when(j > tm)
        def _():
            ends_t[j] = jnp.zeros((PAIR, HALF), BF16)
            ends_o[j] = jnp.zeros((PAIR, HALF), BF16)

        @pl.when(j < tm)
        def _():
            lv[j] = jnp.zeros((PAIR, HALF), BF16)

        return 0

    lax.fori_loop(0, TM, clear, 0)
    remote(pk_m, pk_i, d2d_ss.at[2], d2d_rs.at[2], partner).wait_recv()
    step8 = pk_m[0] + pk_i[0]
    rew8 = pk_m[1] + pk_i[1]
    logp8 = pk_m[2] + pk_i[2]
    rst8 = pk_m[3] + pk_i[3]
    keep8 = 1.0 - rst8
    hor8 = pk_m[4] + pk_i[4]
    burn8 = pk_m[5] + pk_i[5]

    sf[tm, 0] = jnp.broadcast_to(jnp.sum(step8, axis=1, keepdims=True), (PAIR, 128))
    sf[tm, 1] = jnp.broadcast_to(1.0 - jnp.max(rst8, axis=1, keepdims=True), (PAIR, 128))
    for d in range(1, TM):
        dev = {"tm": lax.rem(tm + d, TM), "batch": batch}
        remote(sf.at[tm], sf.at[tm], pre_ss.at[0], pre_rs.at[0], dev).start()

    nb_s[0] = rew8
    nb_s[1] = logp8
    nb_s[2] = keep8
    earlier = lax.rem(tm + TM - 1, TM)
    before = {"tm": earlier, "batch": batch}
    send(nb_s, nb_r, nb_sem.at[0], nb_sem.at[1], before)
    spread_lanes(bc0, step8)
    spread_lanes(bc1, keep8)
    ld8 = jnp.broadcast_to(ld[:, mine], (PAIR, HALF))

    def factors(t, prod):
        e = jnp.exp(wide(bc0[at_t(t), :]) * ld8)
        f = e * wide(bc1[at_t(t), :])
        cc[at_t(t), :] = f
        ss[at_t(t), :] = jnp.sqrt(1.0 - e * e)
        prod = prod * f
        pf[at_t(t), :] = prod
        return prod

    lax.fori_loop(0, T, factors, jnp.ones((PAIR, HALF), F32))
    for p in range(3):
        ag_one_in(1, p)
        ag_own(1, p, 1)
    for p in range(3):
        ag_two_forward(0, p)
        ag_three(0, p, 3)
        ag_three(0, p, 1)
    local[0].wait()
    remote(nxt, xr_n.at[other_half, :], d2d_ss.at[3], d2d_rs.at[3], partner).wait_recv()
    permute_next()
    for p in range(3):
        ag_three_forward(0, p, 0)
    local[1].wait()
    remote(obs, xr_o.at[other_half, :], d2d_ss.at[4], d2d_rs.at[4], partner).wait_recv()
    permute_obs(0, 8)
    for p in range(3):
        ag_two_last(0, p)
        ag_three(0, p, 2)
    for l in (3, 1):
        for p in range(3):
            ag_three_forward(0, p, l)
    for p in range(3):
        ag_two_forward(1, p)
        ag_own(1, p, 2)
    def tails(i, prod):
        t = T - 1 - i
        tp[at_t(t), :] = prod
        return prod * cc[at_t(t), :]

    lax.fori_loop(0, T, tails, jnp.ones((PAIR, HALF), F32))
    for p in range(3):
        ag_three_forward(0, p, 2)
        ag_three(1, p, 3)
        ag_three(1, p, 1)
    for p in (0, 1):
        project_planes(0, p, (0, 1, 3), True)
    for p in range(3):
        ag_two_last(1, p)
        ag_three(1, p, 2)
    sums = remote(
        sf.at[pl.ds(0, TM - 1)], sf.at[pl.ds(0, TM - 1)], pre_ss.at[0], pre_rs.at[0], partner
    )
    sums.wait_recv()

    def block_decay(j, _):
        v = jnp.exp(wide(sf[j, 0]) * ld8) * wide(sf[j, 1])
        dfor[j] = jnp.where(j < tm, v, 1.0)
        dback[j] = jnp.where(j > tm, v, 1.0)
        return 0

    lax.fori_loop(0, TM, block_decay, 0)
    for p in range(3):
        ag_three_forward(1, p, 0)
    for p in (0, 1, 2):
        if p == 2:
            for l in range(4):
                ag_line_last(0, l)
            project_planes(0, p, (0, 1, 3, 2), True)
        else:
            ag_three_last(0, p)
            project_planes(0, p, (2,), False)
        scan(0, vt, p, ends_t)
    prefix_send(1, ends_t, None, True)
    for p in range(3):
        ag_three_forward(1, p, 3)
    for p in range(3):
        ag_three_forward(1, p, 1)
    for p in (0, 1):
        project_planes(1, p, (0,), True)
    for p in range(3):
        ag_three_forward(1, p, 2)
    for p in (0, 1):
        project_planes(1, p, (1, 3), False)
    for l in (0, 3, 1):
        ag_line_last(1, l)
    project_planes(1, 2, (0, 1, 3), True)
    for p in PARTS:
        ag_line_last(1, 2) if p == 2 else ag_three_last(1, p)
        project_planes(1, p, (2,), False)
        scan(1, vo, p, ends_o)
        prefix_send(2 + p, ends_o, p, True)
    prefix_take(1, ends_t, None, True)
    for p in PARTS:
        quality(0, vt, tgh, p, p == PARTS[0], False)
    quality_send(0)
    for core in range(2):
        dev = {"tm": earlier, "batch": z * 2 + core}
        remote(q_s.at[0], q_n.at[c], nb_sem.at[2], nb_sem.at[3], dev).start()
    prefix_take(2 + PARTS[0], ends_o, PARTS[0], True)
    quality(1, vo, onh, PARTS[0], True, True)

    for p in PARTS[1:]:
        prefix_take(2 + p, ends_o, p, True)
        quality(1, vo, onh, p, False, True)
    quality_send(1)
    def value_of(products, log_prob):
        tq = [v * (H ** (-0.5)) for v in products]
        return jnp.minimum(tq[0], tq[1]) - ENTROPY_COEFF * log_prob

    value8 = value_of(quality_sum(0), logp8)
    remote(nb_s, nb_r, nb_sem.at[0], nb_sem.at[1], before).wait_recv()
    later_q = remote(q_n, q_n, nb_sem.at[2], nb_sem.at[3], before)
    later_q.wait_recv()
    later_value = value_of([q_n[0, k] + q_n[1, k] for k in range(2)], nb_r[1])
    inside = (lane8 >= T) & (lane8 < T + NMAX) & (tm < TM - 1)

    def extended(own, later):
        later = jnp.where(inside, pltpu.roll(later, T, 1), 0.0)
        return jnp.where(lane8 < T, own, later)

    ext_r, ext_v = extended(rew8, nb_r[0]), extended(value8, later_value)
    ext_k = extended(keep8, nb_r[2])

    def shifted(v, n):
        return v if n == 0 else pltpu.roll(v, 128 - n, 1)

    total = jnp.zeros((PAIR, 128), F32)
    alive = jnp.ones((PAIR, 128), F32)
    for n in range(NMAX):
        total = total + jnp.where(hor8 > n, DISCOUNT**n * alive * shifted(ext_r, n), 0.0)
        alive = alive * shifted(ext_k, n + 1)
        total = total + jnp.where(
            hor8 == n + 1, DISCOUNT ** (n + 1) * alive * shifted(ext_v, n + 1), 0.0
        )
    ret[...] = jnp.where(c == 0, total[:4, :T], total[4:, :T])
    weight = jnp.where((lane8 + tm * T).astype(F32) >= burn8, 1.0, 0.0)

    oq = quality_sum(1)
    spread_lanes(bc0, weight * (oq[0] * (H ** (-0.5)) - total) * (H ** (-0.5)))
    spread_lanes(bc1, weight * (oq[1] * (H ** (-0.5)) - total) * (H ** (-0.5)))

    h0 = jnp.broadcast_to(onh[0:1, mine], (PAIR, HALF))
    h1 = jnp.broadcast_to(onh[1:2, mine], (PAIR, HALF))

    def back(i, adj):
        for k in range(4):
            rows = at_t(T - 1 - (i * 4 + k))
            dh = wide(bc0[rows, :]) * h0 + wide(bc1[rows, :]) * h1
            adj = dh * vo[rows, :] + adj
            vo[rows, :] = adj
            adj = cc[rows, :] * adj
        return adj

    leaving = lax.fori_loop(0, T // 4, back, jnp.zeros((PAIR, HALF), F32))
    lv[tm] = leaving.astype(BF16)
    prefix_send(5, lv, None, False)

    def finish(p):
        cols = cols_of(p)
        incoming = carry[:, cols]
        both = jnp.concatenate([incoming, incoming], axis=0)

        def body(i, _):
            for k in range(4):
                rows = pl.ds(pl.multiple_of(i * 64 + k * 16, 16), 16)
                adj = vo[rows, cols] + tp[rows, cols] * both
                du[rows, cols] = (ss[rows, cols] * adj).astype(BF16)
            return 0

        lax.fori_loop(0, ROWS // 64, body, 0)

    def gradient(p, l):
        where = place(p, FULL, turned(p, 1, l), FULL)
        lhs = xt[where].reshape(512, ROWS)
        v = jnp.dot(lhs, du[:, cols_of(p)], preferred_element_type=F32)
        gg[p][where] = v.reshape(4, 4, 32, WIDTHS[p])

    def rs_copy(p, k, j, src, dst, dev):
        return remote(src, dst, rs_ss.at[p * 3 + k], rs_rs.at[p * RS_SEMS + j], dev)

    def rs_half(p, s, h, dev):
        return rs_copy(p, 0, s, snd_h[p].at[s, h], rcv_h[p].at[s, h], dev)

    def rs_whole(p, s, h, dev):
        return rs_copy(p, 1, 5 + s, snd_w[p].at[s, h], rcv_w[p].at[s, h], dev)

    def rs_drain(p):
        for k, (src, dst) in enumerate(
            ((snd_h[p], rcv_h[p]), (snd_w[p], rcv_w[p]), (snd_b[p], rcv_b[p]))
        ):
            rs_copy(p, k, 0, src, dst, partner).wait_send()

    def rs_ref(p, s, d, h=None):
        if s < 4:
            return line(p, turned(p, 1, s), turned(p, 2, d), h)
        return line(p, turned(p, 1, d), turned(p, 2, 0), h)

    def rs_axis(s):
        return 2 if s < 4 else 1

    def rs_opposite(p, s):
        for h, d in ((0, 3), (1, 1)):
            snd_h[p][s, h] = gg[p][rs_ref(p, s, 2, h)].astype(BF16)
            rs_half(p, s, h, toward(p, rs_axis(s), d)).start()

    def rs_arrived(p, s):
        rs_copy(p, 0, s, snd_h[p].at[s], rcv_h[p].at[s], partner).wait_recv()

    def rs_neighbour(p, s, h):
        d = (3, 1)[h]
        with_recv = gg[p][rs_ref(p, s, d, h)] + rcv_h[p][s, h].astype(F32)
        snd_w[p][s, h, pl.ds(2 * h, 2)] = with_recv.astype(BF16)
        snd_w[p][s, h, pl.ds(2 - 2 * h, 2)] = gg[p][rs_ref(p, s, d, 1 - h)].astype(BF16)
        rs_whole(p, s, h, toward(p, rs_axis(s), d)).start()

    def rs_neighbours(p, s):
        rs_arrived(p, s)
        rs_neighbour(p, s, 0)
        rs_neighbour(p, s, 1)

    def rs_sum(p, s):
        rs_copy(p, 1, 5 + s, snd_w[p].at[s], rcv_w[p].at[s], partner).wait_recv()
        own = rs_ref(p, s, 0)
        both = rcv_w[p][s, 0].astype(F32) + rcv_w[p][s, 1].astype(F32)
        gg[p][own] = gg[p][own] + both

    def rs_one(p):
        for d in (2, 1, 3):
            where = place(p, turned(p, 0, d), turned(p, 1, 0), turned(p, 2, 0))
            for core in range(2):
                block = gg[p][(*where, pl.ds(16 * core, 16))]
                snd_b[p][core, d - 1] = block.astype(BF16)
                rs_copy(
                    p, 2, 10, snd_b[p].at[core, d - 1], rcv_b[p].at[c, d - 1],
                    toward(p, 0, d, core),
                ).start()
        gx_s[:, cols_of(p)] = gg[p][y, x, z, other_rows, :]

    prefix_take(5, lv, None, False)
    for p in RS_PARTS:
        finish(p)
        gradient(p, LINES[0])
        rs_opposite(p, LINES[0])
    for p in RS_PARTS:
        gradient(p, LINES[1])
        rs_opposite(p, LINES[1])
    for p in RS_PARTS:
        rs_neighbours(p, LINES[0])
        gradient(p, LINES[2])
        rs_opposite(p, LINES[2])
    for p in RS_PARTS:
        rs_neighbours(p, LINES[1])
        gradient(p, LINES[3])
        rs_opposite(p, LINES[3])
    for p in RS_PARTS:
        rs_sum(p, LINES[0])
        rs_opposite(p, 4)
    for p in RS_PARTS:
        rs_neighbours(p, LINES[2])
    for p in RS_PARTS:
        rs_sum(p, LINES[1])
        rs_arrived(p, 4)
        rs_neighbour(p, 4, 0)
    for p in RS_PARTS:
        rs_neighbours(p, LINES[3])
    for p in RS_PARTS:
        rs_sum(p, LINES[2])
        rs_neighbour(p, 4, 1)
    prefix_drain(1, ends_t, None, True)
    for p in range(3):
        prefix_drain(2 + p, ends_o, p, True)
        ag_drain(0, p)
        ag_drain(1, p)
    prefix_drain(5, lv, None, False)
    remote(wst, wst, d2d_ss.at[0], d2d_rs.at[0], partner).wait_send()
    sums.wait_send()
    later_q.wait_send()
    for copy in pending:
        copy.wait_send()
    pending.clear()
    for p in RS_PARTS:
        rs_sum(p, LINES[3])
    for p in RS_PARTS:
        rs_sum(p, 4)
        rs_one(p)
    send(gx_s, gx_r, d2d_ss.at[7], d2d_rs.at[7], partner)
    remote(gx_s, gx_r, d2d_ss.at[7], d2d_rs.at[7], partner).wait_recv()
    for p in range(3):
        rs_copy(p, 2, 10, snd_b[p], rcv_b[p], partner).wait_recv()
        for core, v in (
            (c, gg[p][y, x, z, own_rows, :]), (other, gx_r[:, cols_of(p)]),
        ):
            for d in range(3):
                v = v + rcv_b[p][core, d].astype(F32)
            cols = pl.ds(pl.multiple_of(core * HALF + OFFSETS[p], 128), WIDTHS[p])
            gw[:, cols] = v

    for p in range(3):
        rs_drain(p)
    for copy in pending:
        copy.wait_send()


def update(grad, returns, onw, tgw, grad_w, new_target, returns_out):
    g = grad[...] * SCALE
    grad_w[...] = g
    new_target[...] = (1.0 - POLYAK_RATE) * tgw[...] + POLYAK_RATE * (onw[...] - STEP_SIZE * g)
    returns_out[...] = returns[...]


def shards(
    obs_feats, next_feats, online_w, target_w, log_decay, step_scale, online_heads, target_heads,
    reward, next_action_log_prob, resets, horizon, burn_in,
):
    vmem = pl.BlockSpec(memory_space=pltpu.VMEM)
    smem = pl.BlockSpec(memory_space=pltpu.SMEM)
    hbm = pl.BlockSpec(memory_space=pltpu.HBM)
    small = (
        online_w, target_w, log_decay[None], step_scale, online_heads, target_heads,
        reward, next_action_log_prob, resets,
    )
    weights = [pltpu.VMEM((4, 4, 4, 32, w), BF16) for w in WIDTHS_T + WIDTHS]
    staged = [
        *[pltpu.VMEM((5, 2, 2, 32, w), BF16) for w in WIDTHS],
        *[pltpu.VMEM((5, 2, 4, 32, w), BF16) for w in WIDTHS],
        *[pltpu.VMEM((2, 3, 16, w), BF16) for w in WIDTHS],
    ]
    big = pltpu.VMEM((ROWS, HALF), F32)
    table = pltpu.VMEM((TM, PAIR, HALF), F32)
    ends = pltpu.VMEM((TM, PAIR, HALF), BF16)
    narrow = pltpu.VMEM((ROWS, 128), F32)
    scratch = [
        *[pltpu.VMEM(a.shape, a.dtype) for a in small],
        pltpu.VMEM((ROWS, D), BF16), pltpu.VMEM((ROWS, D), BF16),
        pltpu.VMEM((ROWS, D), BF16), pltpu.VMEM((ROWS, D), BF16),
        pltpu.VMEM((4, 4, 4, 32, ROWS), BF16), pltpu.VMEM((2, 16, HALF), BF16),
        *weights,
        pltpu.VMEM((6, PAIR, 128), F32), pltpu.VMEM((6, PAIR, 128), F32),
        narrow, narrow, narrow, narrow,
        big, big, big, big, big, big,
        pltpu.VMEM((TM, 2, PAIR, 128), F32), table, table, ends, ends, ends,
        pltpu.VMEM((PAIR, HALF), F32),
        pltpu.VMEM((2, 2, PAIR, 128), F32), pltpu.VMEM((2, 2, PAIR, 128), F32),
        pltpu.VMEM((2, 2, PAIR, 128), F32),
        pltpu.VMEM((3, PAIR, 128), F32), pltpu.VMEM((3, PAIR, 128), F32),
        pltpu.VMEM((ROWS, HALF), BF16),
        *[pltpu.VMEM((4, 4, 4, 32, w), F32) for w in WIDTHS],
        *staged, *staged,
        pltpu.VMEM((16, HALF), F32), pltpu.VMEM((16, HALF), F32),
        pltpu.SemaphoreType.DMA((18,)), pltpu.SemaphoreType.DMA((6 * AG_SEMS + 6,)),
        pltpu.SemaphoreType.DMA((9,)), pltpu.SemaphoreType.DMA((3 * RS_SEMS,)),
        pltpu.SemaphoreType.DMA((6,)), pltpu.SemaphoreType.DMA((6,)),
        pltpu.SemaphoreType.DMA((2,)), pltpu.SemaphoreType.DMA((9,)),
        pltpu.SemaphoreType.DMA((8,)), pltpu.SemaphoreType.DMA((8,)),
        pltpu.SemaphoreType.DMA((4,)),
    ]
    rows_b, span, width = obs_feats.shape
    grad, returns = pl.pallas_call(
        kernel,
        name="critic_step",
        out_shape=(
            jax.ShapeDtypeStruct(online_w.shape, F32),
            jax.ShapeDtypeStruct(reward.shape, F32),
        ),
        in_specs=[hbm] * 11 + [smem] * 2,
        out_specs=(vmem, vmem),
        scratch_shapes=scratch,
        compiler_params=pltpu.CompilerParams(
            collective_id=0, has_side_effects=True, vmem_limit_bytes=VMEM_LIMIT * 1024 * 1024
        ),
    )(
        obs_feats.reshape(rows_b * span, width), next_feats.reshape(rows_b * span, width),
        *small, horizon, burn_in,
    )
    return pl.pallas_call(
        update,
        name="target_update",
        out_shape=(
            jax.ShapeDtypeStruct(online_w.shape, F32),
            jax.ShapeDtypeStruct(target_w.shape, F32),
            jax.ShapeDtypeStruct(reward.shape, F32),
        ),
        in_specs=[vmem] * 4,
        out_specs=(vmem, vmem, vmem),
    )(grad, returns, online_w, target_w)


def solution(mesh):
    return jax.shard_map(
        shards,
        mesh=mesh,
        in_specs=(
            P("batch", "tm", None), P("batch", "tm", None),
            P(("tm", "batch"), None), P(("tm", "batch"), None),
            P(), P("batch", "tm"), P(), P(),
            P("batch", "tm"), P("batch", "tm"), P("batch", "tm"), P("batch"), P("batch"),
        ),
        out_specs=(P(("tm", "batch"), None), P(("tm", "batch"), None), P("batch", "tm")),
        check_vma=False,
    )
```

```python
import jax
import jax.numpy as jnp
from jax import lax
from jax.experimental import pallas as pl
from jax.experimental.pallas import tpu as pltpu
from jax.sharding import PartitionSpec as P

NMAX = 8
DISCOUNT = 0.99
ENTROPY_COEFF = 0.2
POLYAK_RATE = 0.005
STEP_SIZE = 0.1

F32 = jnp.float32
BF16 = jnp.bfloat16
MESH = pl.DeviceIdType.MESH

D = 2048
H = 2048
HALF = H // 2
T = 64
PAIR = 8
ROWS = T * PAIR
TM = 16
VMEM_LIMIT = 56
SCALE = D ** (-0.5)

WIDTHS_T = (256, 384, 384)
OFFSETS_T = (0, 256, 640)
WIDTHS = (384, 256, 384)
OFFSETS = (0, 384, 640)
ORDERS = (("z", "x", "y"), ("y", "z", "x"), ("x", "y", "z"))
PARTS = (1, 0, 2)
RS_PARTS = (2, 0, 1)
PROJECTED = 512
AG_SEMS = 8
RS_SEMS = 11
LINES = (2, 3, 1, 0)


def kernel(
    obs, nxt, onw_in, tgw_in, ld_in, step_in, onh_in, tgh_in, rew_in, logp_in, rst_in, hor, burn,
    gw, ret,
    onw, tgw, ld, step, onh, tgh, rew, logp, rst,
    xr_o, xr_n, xp_o, xp_n, xt, wst,
    wt0, wt1, wt2, wo0, wo1, wo2,
    pk_m, pk_i, bc0, bc1, qa0, qa1, cc, ss, pf, tp, vt, vo,
    sf, dfor, dback, ends_t, ends_o, lv, carry,
    q_s, q_r, q_n, nb_s, nb_r, du,
    g0, g1, g2,
    sh0, sh1, sh2, sw0, sw1, sw2, sb0, sb1, sb2,
    rh0, rh1, rh2, rw0, rw1, rw2, rb0, rb1, rb2,
    gx_s, gx_r,
    ag_ss, ag_rs, rs_ss, rs_rs, pre_ss, pre_rs, loc_sem, in_sem, d2d_ss, d2d_rs, nb_sem,
):
    tm = lax.axis_index("tm")
    batch = lax.axis_index("batch")
    y, x = tm // 4, tm % 4
    z, c = batch // 2, batch % 2
    at = {"y": y, "x": x, "z": z}
    other = 1 - c
    wb = ((wt0, wt1, wt2), (wo0, wo1, wo2))
    gg = (g0, g1, g2)
    snd_h, snd_w, snd_b = (sh0, sh1, sh2), (sw0, sw1, sw2), (sb0, sb1, sb2)
    rcv_h, rcv_w, rcv_b = (rh0, rh1, rh2), (rw0, rw1, rw2), (rb0, rb1, rb2)
    pending = []

    def device(core=c, **moved):
        here = {**at, **moved}
        return {"tm": here["y"] * 4 + here["x"], "batch": here["z"] * 2 + core}

    partner = {"tm": tm, "batch": z * 2 + other}

    def remote(src, dst, ss_, rs_, dev):
        return pltpu.make_async_remote_copy(
            src_ref=src, dst_ref=dst, send_sem=ss_, recv_sem=rs_, device_id=dev,
            device_id_type=MESH,
        )

    def send(src, dst, ss_, rs_, dev):
        copy = remote(src, dst, ss_, rs_, dev)
        copy.start()
        pending.append(copy)

    own_half = pl.ds(pl.multiple_of(c * 256, 256), 256)
    other_half = pl.ds(pl.multiple_of(other * 256, 256), 256)
    loads = [
        pltpu.make_async_copy(src, dst, in_sem.at[i])
        for i, (src, dst) in enumerate((
            (tgw_in, tgw), (onw_in, onw), (step_in, step), (rew_in, rew), (logp_in, logp),
            (rst_in, rst), (ld_in, ld), (onh_in, onh), (tgh_in, tgh),
        ))
    ]
    local = [
        pltpu.make_async_copy(nxt, xr_n.at[own_half, :], loc_sem.at[0]),
        pltpu.make_async_copy(obs, xr_o.at[own_half, :], loc_sem.at[1]),
    ]
    for copy in loads + local:
        copy.start()
    barrier = pltpu.get_barrier_semaphore()
    peers = [partner] + [device(z=lax.rem(z + d, 4)) for d in range(1, 4)]
    for a in "yxz":
        peers += [device(core=other, **{a: lax.rem(at[a] + d, 4)}) for d in range(1, 4)]
    peers += [{"tm": lax.rem(tm + d, TM), "batch": batch} for d in range(1, TM)]
    peers += [{"tm": lax.rem(tm + d, TM), "batch": z * 2 + other} for d in (1, TM - 1)]
    for dev in peers:
        pl.semaphore_signal(barrier, inc=1, device_id=dev, device_id_type=MESH)
    for copy in loads:
        copy.wait()

    mine = pl.ds(pl.multiple_of(c * HALF, HALF), HALF)
    theirs = pl.ds(pl.multiple_of(other * HALF, HALF), HALF)
    own_rows = pl.ds(pl.multiple_of(c * 16, 16), 16)
    other_rows = pl.ds(pl.multiple_of(other * 16, 16), 16)
    for m, w in enumerate((tgw, onw)):
        wst[m] = w[:, theirs].astype(BF16)
        for p in range(3):
            off = (OFFSETS_T, OFFSETS)[m][p]
            cols = pl.ds(pl.multiple_of(c * HALF + off, 128), (WIDTHS_T, WIDTHS)[m][p])
            wb[m][p][y, x, z, own_rows, :] = w[:, cols].astype(BF16)

    row8 = lax.broadcasted_iota(jnp.int32, (PAIR, 128), 0)
    lane8 = lax.broadcasted_iota(jnp.int32, (PAIR, 128), 1)
    row_own = (row8[:, :T] // 4) == c

    def twice(v):
        return jnp.where(row_own, jnp.concatenate([v, v], axis=0), 0.0)

    pk_m[...] = jnp.zeros_like(pk_m)
    for slot, r in enumerate((step, rew, logp)):
        pk_m[slot, :, :T] = twice(r[...])
    pk_m[3, :, :T] = twice(rst[...].astype(F32))
    hz = jnp.zeros((PAIR, 128), F32)
    bz = jnp.zeros((PAIR, 128), F32)
    for i in range(4):
        sel = row8 == c * 4 + i
        hz = jnp.where(sel, hor[i].astype(F32), hz)
        bz = jnp.where(sel, burn[i].astype(F32), bz)
    pk_m[4] = hz
    pk_m[5] = bz

    pl.semaphore_wait(barrier, len(peers))

    def w_half(m, p):
        src, dst = wst.at[m, :, cols_of(p, m)], wb[m][p].at[y, x, z, own_rows, :]
        return remote(src, dst, d2d_ss.at[0], d2d_rs.at[m], partner)

    def w_half_in(m):
        remote(wst.at[m], wst.at[m], d2d_ss.at[0], d2d_rs.at[m], partner).wait_recv()

    def width(m, p):
        return (WIDTHS_T, WIDTHS)[m][p]

    def cols_of(p, m=1):
        return pl.ds((OFFSETS_T, OFFSETS)[m][p], width(m, p))

    for m in range(2):
        for p in range(3):
            w_half(m, p).start()
    send(pk_m, pk_i, d2d_ss.at[2], d2d_rs.at[2], partner)
    send(nxt, xr_n.at[own_half, :], d2d_ss.at[3], d2d_rs.at[3], partner)
    send(obs, xr_o.at[own_half, :], d2d_ss.at[4], d2d_rs.at[4], partner)

    def place(p, first, second, last):
        idx = dict(zip(ORDERS[p], (first, second, last)))
        return idx["y"], idx["x"], idx["z"]

    def turned(p, i, d):
        return lax.rem(at[ORDERS[p][i]] + d, 4)

    def toward(p, i, d, core=c):
        return device(core=core, **{ORDERS[p][i]: turned(p, i, d)})

    FULL = pl.ds(0, 4)

    def half_of(h):
        return FULL if h is None else pl.ds(2 * h, 2)

    def ag_copy(m, p, k, j, where, dev):
        ref = wb[m][p].at[where]
        n = m * 3 + p
        return remote(ref, ref, ag_ss.at[n * 3 + k], ag_rs.at[n * AG_SEMS + 3 * m + j], dev)

    def ag_end(m, p, l):
        return 7 + l if p == 2 else 7

    def ag_send(m, p, k, j, where, dev):
        ag_copy(m, p, k, j, where, dev).start()

    def ag_wait(m, p, j, where):
        ag_copy(m, p, 0, j, where, partner).wait_recv()

    def ag_drain(m, p):
        for k, where in enumerate(((0, 0, pl.ds(0, 3)), (0, pl.ds(0, 3)), (pl.ds(0, 3),))):
            ag_copy(m, p, k, 0, where, partner).wait_send()

    def line(p, second, last, h=None):
        return place(p, half_of(h), second, last)

    def ag_one(m, p):
        dst = wb[m][p].at[y, x, z, own_rows, :]
        sem, n = ag_ss.at[(m * 3 + p) * 3], (m * 3 + p) * AG_SEMS + 3 * m
        for d in (2, 1, 3):
            remote(dst, dst, sem, ag_rs.at[n], toward(p, 0, d)).start()
            src = wst.at[m, :, cols_of(p, m)]
            remote(src, dst, sem, ag_rs.at[n], toward(p, 0, d, other)).start()

    def ag_one_in(m, p):
        ag_wait(m, p, 0, (0, 0, pl.ds(0, 3)))

    def ag_own(m, p, k):
        for d in (1, 3, 2):
            where = place(p, turned(p, 0, d), turned(p, 1, 0), turned(p, 2, 0))
            ag_send(m, p, k, 2 * k - 1, where, toward(p, k, 1))
            ag_send(m, p, k, 2 * k - 1, where, toward(p, k, 3))

    def ag_early(m, p):
        for k in (1, 2):
            ag_send(m, p, k, 2 * k - 1, (y, x, z), toward(p, k, 1))
            ag_send(m, p, k, 2 * k - 1, (y, x, z), toward(p, k, 3))

    def ag_two_forward(m, p):
        q3 = turned(p, 2, 0)
        ag_wait(m, p, 1, (0, pl.ds(0, 2)))
        ag_send(m, p, 1, 2, line(p, turned(p, 1, 3), q3, 0), toward(p, 1, 1))
        ag_send(m, p, 1, 2, line(p, turned(p, 1, 1), q3, 1), toward(p, 1, 3))

    def ag_two_last(m, p):
        ag_wait(m, p, 2, line(p, turned(p, 1, 2), turned(p, 2, 0)))

    def ag_three(m, p, l):
        own = line(p, turned(p, 1, l), turned(p, 2, 0))
        ag_send(m, p, 2, 3 + l, own, toward(p, 2, 1))
        ag_send(m, p, 2, 3 + l, own, toward(p, 2, 3))

    def ag_three_forward(m, p, l):
        second = turned(p, 1, l)
        ag_wait(m, p, 3 + l, (0, pl.ds(0, 2)))
        end = ag_end(m, p, l)
        ag_send(m, p, 2, end, line(p, second, turned(p, 2, 3), 0), toward(p, 2, 1))
        ag_send(m, p, 2, end, line(p, second, turned(p, 2, 1), 1), toward(p, 2, 3))

    def ag_three_last(m, p):
        ag_wait(m, p, 7, place(p, FULL, FULL, turned(p, 2, 2)))

    def ag_line_last(m, l):
        ag_wait(m, 2, 7 + l, line(2, turned(2, 1, l), turned(2, 2, 2)))

    def wide(v, w=HALF):
        return jnp.concatenate([v] * (w // 128), axis=1)

    def at_t(t):
        return pl.ds(pl.multiple_of(t * PAIR, PAIR), PAIR)

    def spread_lanes(dst, v):
        for t in range(T):
            dst[pl.ds(t * PAIR, PAIR), :] = jnp.broadcast_to(v[:, t : t + 1], (PAIR, 128))

    r_out = lax.broadcasted_iota(jnp.int32, (ROWS, ROWS), 0)
    r_in = lax.broadcasted_iota(jnp.int32, (ROWS, ROWS), 1)

    def permutation():
        return jnp.where(r_out == (r_in % T) * PAIR + r_in // T, 1.0, 0.0).astype(BF16)

    def permute_next():
        perm = permutation()

        def body(i, _):
            cols = pl.ds(pl.multiple_of(i * 256, 256), 256)
            xp_n[:, cols] = jnp.dot(perm, xr_n[:, cols], preferred_element_type=F32).astype(BF16)
            return 0

        lax.fori_loop(0, D // 256, body, 0)

    def permute_obs(lo, hi):
        perm = permutation()

        def body(i, _):
            cols = pl.ds(pl.multiple_of(i * 256, 256), 256)
            v = jnp.dot(perm, xr_o[:, cols], preferred_element_type=F32)
            xp_o[:, cols] = v.astype(BF16)
            xt[i // 2, pl.ds(2 * (i % 2), 2)] = v.T.astype(BF16).reshape(2, 4, 32, ROWS)
            return 0

        lax.fori_loop(lo, hi, body, 0)

    def project_planes(m, p, planes, fresh):
        xp, v = (xp_n, vt) if m == 0 else (xp_o, vo)
        cols, w = cols_of(p, m), width(m, p)
        axis = 1 if p == 2 else 2
        qs = [turned(p, axis, d) for d in planes]

        def tile(i, _):
            rows = pl.ds(pl.multiple_of(i * PROJECTED, PROJECTED), PROJECTED)
            acc = None if fresh else v[rows, cols]
            for q in qs:
                where = place(p, FULL, q, FULL) if p == 2 else place(p, FULL, FULL, q)
                rhs = wb[m][p][where].reshape(512, w)
                if p == 1:
                    starts = [pl.multiple_of((k * 4 + q) * 128, 128) for k in range(4)]
                    lhs = jnp.concatenate([xp[rows, pl.ds(k, 128)] for k in starts], axis=1)
                else:
                    lhs = xp[rows, pl.ds(pl.multiple_of(q * 512, 512), 512)]
                part = jnp.dot(lhs, rhs, preferred_element_type=F32) * SCALE
                acc = part if acc is None else acc + part
            v[rows, cols] = acc
            return 0

        lax.fori_loop(0, ROWS // PROJECTED, tile, 0)

    def scan(m, v, p, ends):
        cols = cols_of(p, m)

        def body(i, st):
            steps = [at_t(i * 4 + k) for k in range(4)]
            added = [ss[rows, cols] * v[rows, cols] for rows in steps]
            kept = [cc[rows, cols] for rows in steps]
            states = []
            for f, u in zip(kept, added):
                st = f * st + u
                states.append(st)
            for rows, state in zip(steps, states):
                v[rows, cols] = state
            return st

        last = lax.fori_loop(0, T // 4, body, jnp.zeros((PAIR, width(m, p)), F32))
        ends[tm, :, cols] = last.astype(BF16)

    def ends_copy(n, ends, p, slots, dev):
        cols = pl.ds(0, HALF) if p is None else cols_of(p)
        ref = ends.at[slots, :, cols]
        return remote(ref, ref, pre_ss.at[n], pre_rs.at[n], dev)

    def prefix_send(n, ends, p, forward):
        for d in range(TM - 1, 0, -1):
            to = tm + d if forward else tm - d

            @pl.when(to < TM if forward else to >= 0)
            def _(to=to):
                ends_copy(n, ends, p, tm, {"tm": to, "batch": batch}).start()

    def prefix_wait(n, ends, p, count, arrived):
        for k in range(1, TM):

            @pl.when(count == k)
            def _(k=k):
                copies = ends_copy(n, ends, p, pl.ds(0, k), partner)
                copies.wait_recv() if arrived else copies.wait_send()

    def prefix_take(n, ends, p, forward):
        cols, w = (pl.ds(0, HALF), HALF) if p is None else (cols_of(p), WIDTHS[p])
        prefix_wait(n, ends, p, tm if forward else TM - 1 - tm, True)
        decay = dfor if forward else dback
        v = jnp.zeros((PAIR, w), F32)
        for j in range(TM - 1) if forward else range(TM - 1, 0, -1):
            counted = jnp.where(j < tm if forward else j > tm, 1.0, 0.0)
            v = decay[j, :, cols] * v + counted * ends[j, :, cols].astype(F32)
        carry[:, cols] = v

    def prefix_drain(n, ends, p, forward):
        prefix_wait(n, ends, p, TM - 1 - tm if forward else tm, False)

    def quality(m, v, heads, p, fresh, slope):
        cols, w = cols_of(p, m), width(m, p)
        hcols = pl.ds(pl.multiple_of(c * HALF + (OFFSETS_T, OFFSETS)[m][p], 128), w)
        h0 = jnp.broadcast_to(heads[0:1, hcols], (PAIR, w))
        h1 = jnp.broadcast_to(heads[1:2, hcols], (PAIR, w))
        start = carry[:, cols]

        def fold(u):
            out = u[:, :128]
            for i in range(1, w // 128):
                out = out + u[:, i * 128 : (i + 1) * 128]
            return out

        def body(i, _):
            steps = [at_t(i * 8 + k) for k in range(8)]
            states = [v[rows, cols] + pf[rows, cols] * start for rows in steps]
            before = None if fresh else [(qa0[rows, :], qa1[rows, :]) for rows in steps]
            out = []
            for st in states:
                sig = 1.0 / (1.0 + jnp.exp(-st))
                act = st * sig
                out.append((fold(act * h0), fold(act * h1), sig + act * (1.0 - sig)))
            for k, (rows, (f0, f1, rise)) in enumerate(zip(steps, out)):
                qa0[rows, :] = f0 if fresh else before[k][0] + f0
                qa1[rows, :] = f1 if fresh else before[k][1] + f1
                if slope:
                    v[rows, cols] = rise
            return 0

        lax.fori_loop(0, T // 8, body, 0)

    def quality_send(slot):
        def body(i, acc):
            a0, a1 = acc
            for k in range(16):
                rows = at_t(i * 16 + k)
                here = lane8 == i * 16 + k
                a0 = jnp.where(here, jnp.sum(qa0[rows, :], axis=1, keepdims=True), a0)
                a1 = jnp.where(here, jnp.sum(qa1[rows, :], axis=1, keepdims=True), a1)
            return a0, a1

        zero = jnp.zeros((PAIR, 128), F32)
        a0, a1 = lax.fori_loop(0, T // 16, body, (zero, zero))
        q_s[slot, 0] = a0
        q_s[slot, 1] = a1
        send(q_s.at[slot], q_r.at[slot], d2d_ss.at[5 + slot], d2d_rs.at[5 + slot], partner)

    def quality_sum(slot):
        remote(
            q_s.at[slot], q_r.at[slot], d2d_ss.at[5 + slot], d2d_rs.at[5 + slot], partner
        ).wait_recv()
        return [q_s[slot, k] + q_r[slot, k] for k in range(2)]

    for m in range(2):
        for p in range(3):
            ag_one(m, p)
    for m in range(2):
        w_half_in(m)
        for p in range(3):
            ag_early(m, p)
    for p in range(3):
        ag_one_in(0, p)
        ag_own(0, p, 1)
    for p in range(3):
        ag_own(0, p, 2)
    def clear(j, _):
        @pl.when(j > tm)
        def _():
            ends_t[j] = jnp.zeros((PAIR, HALF), BF16)
            ends_o[j] = jnp.zeros((PAIR, HALF), BF16)

        @pl.when(j < tm)
        def _():
            lv[j] = jnp.zeros((PAIR, HALF), BF16)

        return 0

    lax.fori_loop(0, TM, clear, 0)
    remote(pk_m, pk_i, d2d_ss.at[2], d2d_rs.at[2], partner).wait_recv()
    step8 = pk_m[0] + pk_i[0]
    rew8 = pk_m[1] + pk_i[1]
    logp8 = pk_m[2] + pk_i[2]
    rst8 = pk_m[3] + pk_i[3]
    keep8 = 1.0 - rst8
    hor8 = pk_m[4] + pk_i[4]
    burn8 = pk_m[5] + pk_i[5]

    sf[tm, 0] = jnp.broadcast_to(jnp.sum(step8, axis=1, keepdims=True), (PAIR, 128))
    sf[tm, 1] = jnp.broadcast_to(1.0 - jnp.max(rst8, axis=1, keepdims=True), (PAIR, 128))
    for d in range(1, TM):
        dev = {"tm": lax.rem(tm + d, TM), "batch": batch}
        remote(sf.at[tm], sf.at[tm], pre_ss.at[0], pre_rs.at[0], dev).start()

    nb_s[0] = rew8
    nb_s[1] = logp8
    nb_s[2] = keep8
    earlier = lax.rem(tm + TM - 1, TM)
    before = {"tm": earlier, "batch": batch}
    send(nb_s, nb_r, nb_sem.at[0], nb_sem.at[1], before)
    spread_lanes(bc0, step8)
    spread_lanes(bc1, keep8)
    ld8 = jnp.broadcast_to(ld[:, mine], (PAIR, HALF))

    def factors(t, prod):
        e = jnp.exp(wide(bc0[at_t(t), :]) * ld8)
        f = e * wide(bc1[at_t(t), :])
        cc[at_t(t), :] = f
        ss[at_t(t), :] = jnp.sqrt(1.0 - e * e)
        prod = prod * f
        pf[at_t(t), :] = prod
        return prod

    lax.fori_loop(0, T, factors, jnp.ones((PAIR, HALF), F32))
    for p in range(3):
        ag_one_in(1, p)
        ag_own(1, p, 1)
    for p in range(3):
        ag_two_forward(0, p)
        ag_three(0, p, 3)
        ag_three(0, p, 1)
    local[0].wait()
    remote(nxt, xr_n.at[other_half, :], d2d_ss.at[3], d2d_rs.at[3], partner).wait_recv()
    permute_next()
    for p in range(3):
        ag_three_forward(0, p, 0)
    local[1].wait()
    remote(obs, xr_o.at[other_half, :], d2d_ss.at[4], d2d_rs.at[4], partner).wait_recv()
    permute_obs(0, 8)
    for p in range(3):
        ag_two_last(0, p)
        ag_three(0, p, 2)
    for l in (3, 1):
        for p in range(3):
            ag_three_forward(0, p, l)
    for p in range(3):
        ag_two_forward(1, p)
        ag_own(1, p, 2)
    def tails(i, prod):
        t = T - 1 - i
        tp[at_t(t), :] = prod
        return prod * cc[at_t(t), :]

    lax.fori_loop(0, T, tails, jnp.ones((PAIR, HALF), F32))
    for p in range(3):
        ag_three_forward(0, p, 2)
        ag_three(1, p, 3)
        ag_three(1, p, 1)
    for p in (0, 1):
        project_planes(0, p, (0, 1, 3), True)
    for p in range(3):
        ag_two_last(1, p)
        ag_three(1, p, 2)
    sums = remote(
        sf.at[pl.ds(0, TM - 1)], sf.at[pl.ds(0, TM - 1)], pre_ss.at[0], pre_rs.at[0], partner
    )
    sums.wait_recv()

    def block_decay(j, _):
        v = jnp.exp(wide(sf[j, 0]) * ld8) * wide(sf[j, 1])
        dfor[j] = jnp.where(j < tm, v, 1.0)
        dback[j] = jnp.where(j > tm, v, 1.0)
        return 0

    lax.fori_loop(0, TM, block_decay, 0)
    for p in range(3):
        ag_three_forward(1, p, 0)
    for p in (0, 1, 2):
        if p == 2:
            for l in range(4):
                ag_line_last(0, l)
            project_planes(0, p, (0, 1, 3, 2), True)
        else:
            ag_three_last(0, p)
            project_planes(0, p, (2,), False)
        scan(0, vt, p, ends_t)
    prefix_send(1, ends_t, None, True)
    for p in range(3):
        ag_three_forward(1, p, 3)
    for p in range(3):
        ag_three_forward(1, p, 1)
    for p in (0, 1):
        project_planes(1, p, (0,), True)
    for p in range(3):
        ag_three_forward(1, p, 2)
    for p in (0, 1):
        project_planes(1, p, (1, 3), False)
    for p in PARTS:
        if p == 2:
            for l in (0, 3, 1):
                ag_line_last(1, l)
            project_planes(1, p, (0, 1, 3), True)
            ag_line_last(1, 2)
        else:
            ag_three_last(1, p)
        project_planes(1, p, (2,), False)
        scan(1, vo, p, ends_o)
        prefix_send(2 + p, ends_o, p, True)
    prefix_take(1, ends_t, None, True)
    for p in PARTS:
        quality(0, vt, tgh, p, p == PARTS[0], False)
    quality_send(0)
    for core in range(2):
        dev = {"tm": earlier, "batch": z * 2 + core}
        remote(q_s.at[0], q_n.at[c], nb_sem.at[2], nb_sem.at[3], dev).start()
    prefix_take(2 + PARTS[0], ends_o, PARTS[0], True)
    quality(1, vo, onh, PARTS[0], True, True)

    for p in PARTS[1:]:
        prefix_take(2 + p, ends_o, p, True)
        quality(1, vo, onh, p, False, True)
    quality_send(1)
    def value_of(products, log_prob):
        tq = [v * (H ** (-0.5)) for v in products]
        return jnp.minimum(tq[0], tq[1]) - ENTROPY_COEFF * log_prob

    value8 = value_of(quality_sum(0), logp8)
    remote(nb_s, nb_r, nb_sem.at[0], nb_sem.at[1], before).wait_recv()
    later_q = remote(q_n, q_n, nb_sem.at[2], nb_sem.at[3], before)
    later_q.wait_recv()
    later_value = value_of([q_n[0, k] + q_n[1, k] for k in range(2)], nb_r[1])
    inside = (lane8 >= T) & (lane8 < T + NMAX) & (tm < TM - 1)

    def extended(own, later):
        later = jnp.where(inside, pltpu.roll(later, T, 1), 0.0)
        return jnp.where(lane8 < T, own, later)

    ext_r, ext_v = extended(rew8, nb_r[0]), extended(value8, later_value)
    ext_k = extended(keep8, nb_r[2])

    def shifted(v, n):
        return v if n == 0 else pltpu.roll(v, 128 - n, 1)

    total = jnp.zeros((PAIR, 128), F32)
    alive = jnp.ones((PAIR, 128), F32)
    for n in range(NMAX):
        total = total + jnp.where(hor8 > n, DISCOUNT**n * alive * shifted(ext_r, n), 0.0)
        alive = alive * shifted(ext_k, n + 1)
        total = total + jnp.where(
            hor8 == n + 1, DISCOUNT ** (n + 1) * alive * shifted(ext_v, n + 1), 0.0
        )
    ret[...] = jnp.where(c == 0, total[:4, :T], total[4:, :T])
    weight = jnp.where((lane8 + tm * T).astype(F32) >= burn8, 1.0, 0.0)

    oq = quality_sum(1)
    spread_lanes(bc0, weight * (oq[0] * (H ** (-0.5)) - total) * (H ** (-0.5)))
    spread_lanes(bc1, weight * (oq[1] * (H ** (-0.5)) - total) * (H ** (-0.5)))

    h0 = jnp.broadcast_to(onh[0:1, mine], (PAIR, HALF))
    h1 = jnp.broadcast_to(onh[1:2, mine], (PAIR, HALF))

    def back(i, adj):
        for k in range(4):
            rows = at_t(T - 1 - (i * 4 + k))
            dh = wide(bc0[rows, :]) * h0 + wide(bc1[rows, :]) * h1
            adj = dh * vo[rows, :] + adj
            vo[rows, :] = adj
            adj = cc[rows, :] * adj
        return adj

    leaving = lax.fori_loop(0, T // 4, back, jnp.zeros((PAIR, HALF), F32))
    lv[tm] = leaving.astype(BF16)
    prefix_send(5, lv, None, False)

    def finish(p):
        cols = cols_of(p)
        incoming = carry[:, cols]
        both = jnp.concatenate([incoming, incoming], axis=0)

        def body(i, _):
            for k in range(4):
                rows = pl.ds(pl.multiple_of(i * 64 + k * 16, 16), 16)
                adj = vo[rows, cols] + tp[rows, cols] * both
                du[rows, cols] = (ss[rows, cols] * adj).astype(BF16)
            return 0

        lax.fori_loop(0, ROWS // 64, body, 0)

    def gradient(p, l):
        where = place(p, FULL, turned(p, 1, l), FULL)
        lhs = xt[where].reshape(512, ROWS)
        v = jnp.dot(lhs, du[:, cols_of(p)], preferred_element_type=F32)
        gg[p][where] = v.reshape(4, 4, 32, WIDTHS[p])

    def rs_copy(p, k, j, src, dst, dev):
        return remote(src, dst, rs_ss.at[p * 3 + k], rs_rs.at[p * RS_SEMS + j], dev)

    def rs_half(p, s, h, dev):
        return rs_copy(p, 0, s, snd_h[p].at[s, h], rcv_h[p].at[s, h], dev)

    def rs_whole(p, s, h, dev):
        return rs_copy(p, 1, 5 + s, snd_w[p].at[s, h], rcv_w[p].at[s, h], dev)

    def rs_drain(p):
        for k, (src, dst) in enumerate(
            ((snd_h[p], rcv_h[p]), (snd_w[p], rcv_w[p]), (snd_b[p], rcv_b[p]))
        ):
            rs_copy(p, k, 0, src, dst, partner).wait_send()

    def rs_ref(p, s, d, h=None):
        if s < 4:
            return line(p, turned(p, 1, s), turned(p, 2, d), h)
        return line(p, turned(p, 1, d), turned(p, 2, 0), h)

    def rs_axis(s):
        return 2 if s < 4 else 1

    def rs_opposite(p, s):
        for h, d in ((0, 3), (1, 1)):
            snd_h[p][s, h] = gg[p][rs_ref(p, s, 2, h)].astype(BF16)
            rs_half(p, s, h, toward(p, rs_axis(s), d)).start()

    def rs_arrived(p, s):
        rs_copy(p, 0, s, snd_h[p].at[s], rcv_h[p].at[s], partner).wait_recv()

    def rs_neighbour(p, s, h):
        d = (3, 1)[h]
        with_recv = gg[p][rs_ref(p, s, d, h)] + rcv_h[p][s, h].astype(F32)
        snd_w[p][s, h, pl.ds(2 * h, 2)] = with_recv.astype(BF16)
        snd_w[p][s, h, pl.ds(2 - 2 * h, 2)] = gg[p][rs_ref(p, s, d, 1 - h)].astype(BF16)
        rs_whole(p, s, h, toward(p, rs_axis(s), d)).start()

    def rs_neighbours(p, s):
        rs_arrived(p, s)
        rs_neighbour(p, s, 0)
        rs_neighbour(p, s, 1)

    def rs_sum(p, s):
        rs_copy(p, 1, 5 + s, snd_w[p].at[s], rcv_w[p].at[s], partner).wait_recv()
        own = rs_ref(p, s, 0)
        both = rcv_w[p][s, 0].astype(F32) + rcv_w[p][s, 1].astype(F32)
        gg[p][own] = gg[p][own] + both

    def rs_one(p):
        for d in (2, 1, 3):
            where = place(p, turned(p, 0, d), turned(p, 1, 0), turned(p, 2, 0))
            for core in range(2):
                block = gg[p][(*where, pl.ds(16 * core, 16))]
                snd_b[p][core, d - 1] = block.astype(BF16)
                rs_copy(
                    p, 2, 10, snd_b[p].at[core, d - 1], rcv_b[p].at[c, d - 1],
                    toward(p, 0, d, core),
                ).start()
        gx_s[:, cols_of(p)] = gg[p][y, x, z, other_rows, :]

    prefix_take(5, lv, None, False)
    for p in RS_PARTS:
        finish(p)
        gradient(p, LINES[0])
        rs_opposite(p, LINES[0])
    for p in RS_PARTS:
        gradient(p, LINES[1])
        rs_opposite(p, LINES[1])
    for p in RS_PARTS:
        rs_neighbours(p, LINES[0])
        gradient(p, LINES[2])
        rs_opposite(p, LINES[2])
    for p in RS_PARTS:
        rs_neighbours(p, LINES[1])
        gradient(p, LINES[3])
        rs_opposite(p, LINES[3])
    for p in RS_PARTS:
        rs_sum(p, LINES[0])
        rs_opposite(p, 4)
    for p in RS_PARTS:
        rs_neighbours(p, LINES[2])
    for p in RS_PARTS:
        rs_sum(p, LINES[1])
        rs_arrived(p, 4)
        rs_neighbour(p, 4, 0)
    for p in RS_PARTS:
        rs_neighbours(p, LINES[3])
    for p in RS_PARTS:
        rs_sum(p, LINES[2])
        rs_neighbour(p, 4, 1)
    prefix_drain(1, ends_t, None, True)
    for p in range(3):
        prefix_drain(2 + p, ends_o, p, True)
        ag_drain(0, p)
        ag_drain(1, p)
    prefix_drain(5, lv, None, False)
    remote(wst, wst, d2d_ss.at[0], d2d_rs.at[0], partner).wait_send()
    sums.wait_send()
    later_q.wait_send()
    for copy in pending:
        copy.wait_send()
    pending.clear()
    for p in RS_PARTS:
        rs_sum(p, LINES[3])
    for p in RS_PARTS:
        rs_sum(p, 4)
        rs_one(p)
    send(gx_s, gx_r, d2d_ss.at[7], d2d_rs.at[7], partner)
    remote(gx_s, gx_r, d2d_ss.at[7], d2d_rs.at[7], partner).wait_recv()
    for p in range(3):
        rs_copy(p, 2, 10, snd_b[p], rcv_b[p], partner).wait_recv()
        for core, v in (
            (c, gg[p][y, x, z, own_rows, :]), (other, gx_r[:, cols_of(p)]),
        ):
            for d in range(3):
                v = v + rcv_b[p][core, d].astype(F32)
            cols = pl.ds(pl.multiple_of(core * HALF + OFFSETS[p], 128), WIDTHS[p])
            gw[:, cols] = v

    for p in range(3):
        rs_drain(p)
    for copy in pending:
        copy.wait_send()


def update(grad, returns, onw, tgw, grad_w, new_target, returns_out):
    g = grad[...] * SCALE
    grad_w[...] = g
    new_target[...] = (1.0 - POLYAK_RATE) * tgw[...] + POLYAK_RATE * (onw[...] - STEP_SIZE * g)
    returns_out[...] = returns[...]


def shards(
    obs_feats, next_feats, online_w, target_w, log_decay, step_scale, online_heads, target_heads,
    reward, next_action_log_prob, resets, horizon, burn_in,
):
    vmem = pl.BlockSpec(memory_space=pltpu.VMEM)
    smem = pl.BlockSpec(memory_space=pltpu.SMEM)
    hbm = pl.BlockSpec(memory_space=pltpu.HBM)
    small = (
        online_w, target_w, log_decay[None], step_scale, online_heads, target_heads,
        reward, next_action_log_prob, resets,
    )
    weights = [pltpu.VMEM((4, 4, 4, 32, w), BF16) for w in WIDTHS_T + WIDTHS]
    staged = [
        *[pltpu.VMEM((5, 2, 2, 32, w), BF16) for w in WIDTHS],
        *[pltpu.VMEM((5, 2, 4, 32, w), BF16) for w in WIDTHS],
        *[pltpu.VMEM((2, 3, 16, w), BF16) for w in WIDTHS],
    ]
    big = pltpu.VMEM((ROWS, HALF), F32)
    table = pltpu.VMEM((TM, PAIR, HALF), F32)
    ends = pltpu.VMEM((TM, PAIR, HALF), BF16)
    narrow = pltpu.VMEM((ROWS, 128), F32)
    scratch = [
        *[pltpu.VMEM(a.shape, a.dtype) for a in small],
        pltpu.VMEM((ROWS, D), BF16), pltpu.VMEM((ROWS, D), BF16),
        pltpu.VMEM((ROWS, D), BF16), pltpu.VMEM((ROWS, D), BF16),
        pltpu.VMEM((4, 4, 4, 32, ROWS), BF16), pltpu.VMEM((2, 16, HALF), BF16),
        *weights,
        pltpu.VMEM((6, PAIR, 128), F32), pltpu.VMEM((6, PAIR, 128), F32),
        narrow, narrow, narrow, narrow,
        big, big, big, big, big, big,
        pltpu.VMEM((TM, 2, PAIR, 128), F32), table, table, ends, ends, ends,
        pltpu.VMEM((PAIR, HALF), F32),
        pltpu.VMEM((2, 2, PAIR, 128), F32), pltpu.VMEM((2, 2, PAIR, 128), F32),
        pltpu.VMEM((2, 2, PAIR, 128), F32),
        pltpu.VMEM((3, PAIR, 128), F32), pltpu.VMEM((3, PAIR, 128), F32),
        pltpu.VMEM((ROWS, HALF), BF16),
        *[pltpu.VMEM((4, 4, 4, 32, w), F32) for w in WIDTHS],
        *staged, *staged,
        pltpu.VMEM((16, HALF), F32), pltpu.VMEM((16, HALF), F32),
        pltpu.SemaphoreType.DMA((18,)), pltpu.SemaphoreType.DMA((6 * AG_SEMS + 6,)),
        pltpu.SemaphoreType.DMA((9,)), pltpu.SemaphoreType.DMA((3 * RS_SEMS,)),
        pltpu.SemaphoreType.DMA((6,)), pltpu.SemaphoreType.DMA((6,)),
        pltpu.SemaphoreType.DMA((2,)), pltpu.SemaphoreType.DMA((9,)),
        pltpu.SemaphoreType.DMA((8,)), pltpu.SemaphoreType.DMA((8,)),
        pltpu.SemaphoreType.DMA((4,)),
    ]
    rows_b, span, width = obs_feats.shape
    grad, returns = pl.pallas_call(
        kernel,
        name="critic_step",
        out_shape=(
            jax.ShapeDtypeStruct(online_w.shape, F32),
            jax.ShapeDtypeStruct(reward.shape, F32),
        ),
        in_specs=[hbm] * 11 + [smem] * 2,
        out_specs=(vmem, vmem),
        scratch_shapes=scratch,
        compiler_params=pltpu.CompilerParams(
            collective_id=0, has_side_effects=True, vmem_limit_bytes=VMEM_LIMIT * 1024 * 1024
        ),
    )(
        obs_feats.reshape(rows_b * span, width), next_feats.reshape(rows_b * span, width),
        *small, horizon, burn_in,
    )
    return pl.pallas_call(
        update,
        name="target_update",
        out_shape=(
            jax.ShapeDtypeStruct(online_w.shape, F32),
            jax.ShapeDtypeStruct(target_w.shape, F32),
            jax.ShapeDtypeStruct(reward.shape, F32),
        ),
        in_specs=[vmem] * 4,
        out_specs=(vmem, vmem, vmem),
    )(grad, returns, online_w, target_w)


def solution(mesh):
    return jax.shard_map(
        shards,
        mesh=mesh,
        in_specs=(
            P("batch", "tm", None), P("batch", "tm", None),
            P(("tm", "batch"), None), P(("tm", "batch"), None),
            P(), P("batch", "tm"), P(), P(),
            P("batch", "tm"), P("batch", "tm"), P("batch", "tm"), P("batch"), P("batch"),
        ),
        out_specs=(P(("tm", "batch"), None), P(("tm", "batch"), None), P("batch", "tm")),
        check_vma=False,
    )
```
